256 devices in a mesh: obs: 8 (over x, core), ord: 32 (over y, z).
Axes of the slice: x: 4, y: 4, z: 8, core: 2. Of those that a mesh axis runs over, the one named last changes fastest.
Arguments:
- longitude: float32 [8, 32768], P('obs'), may hold values from -3.140625 to 3.140625
- cycle_of: int32 [8, 32768], P('obs'), may hold values from 0 to 255, never falling along the last dimension, each value on 1 to 256 neighbouring positions
- obs_count: int32 [8], P('obs'), may hold values from 16384 to 32768
- observed: float32 [8, 32768], P('obs'), may hold values from -1792 to 1792
- obs_weight: float32 [8, 32768], P('obs'), may hold values from 0.3 to 3
- legendre: float32 [8, 288, 288, 256], P('obs', 'ord'), as said below
- precond_inv: float32 [288, 288, 288], P('ord'), as said below
- order_of_slot: int32 [288], P('ord'), may hold values from 0 to 287, each once
Outputs:
- solution: float32 [288, 2, 288], P('ord')
- residual: float32 [288, 2, 288], P('ord')
The draws below stay inside these ranges and needn't reach their ends.
Inputs may be any that keep to these rules, and one draw needn't show every extreme that they name: `cycle_of`: cycle numbers never fall along a slab; each cycle holds at least one observation slot. `obs_count`: observation slots at or beyond a slab's count carry no weight. legendre[b, m, n, j] is the fully normalized associated Legendre function of degree n and order m at the colatitude of cycle j of slab b, and 0 for n < m. `precond_inv`: every block is symmetric positive definite. order_of_slot names each order once; slot s lies on ord index s // 9.
All inputs are finite; a program needn't handle non-finite values.
Results may differ from the reference program's by a relative error of at most 0.0003.
Values sent between devices are 32-bit elements; how exact they have to be, the bound alone decides.
A program may use at most 128 MiB of HBM per device.

```python
import math
import jax
import jax.numpy as jnp
import numpy as np
from jax import lax

NB = 288
CYCLE_DEV = 256
OBS_DEV = 32768
ITERS = 2
ORDERS = 288
N_OBS = 8


def draw_legendre(key, part):
    colatitude = jax.random.uniform(jax.random.fold_in(key, 11), (N_OBS, CYCLE_DEV), jnp.float32, 0.25, 2.89)
    cosine_col = jnp.cos(colatitude)[:, :, None]
    sine_col = jnp.sin(colatitude)[:, :, None]
    orders = jnp.arange(ORDERS, dtype=jnp.int32).astype(jnp.float32)
    gamma_log = jax.scipy.special.gammaln
    log_start = 0.5 * (gamma_log(2.0 * orders + 2.0) - orders * jnp.log(4.0) - 2.0 * gamma_log(orders + 1.0))
    log_start = log_start + 0.5 * jnp.log(jnp.where(orders > 0, 2.0, 1.0))
    sectoral = jnp.exp(orders[None, None, :] * jnp.log(sine_col) + log_start[None, None, :])
    zeros = jnp.zeros((N_OBS, CYCLE_DEV, ORDERS), jnp.float32)

    def degree_step(state_pair, degree):
        previous, before_previous = state_pair
        degree_f = degree.astype(jnp.float32)
        minus_order = jnp.maximum(degree_f - orders, 1.0)
        plus_order = jnp.maximum(degree_f + orders, 1.0)
        rise_factor = jnp.sqrt(jnp.maximum((2.0 * degree_f - 1.0) * (2.0 * degree_f + 1.0), 0.0) / (minus_order * plus_order))
        fall_top = jnp.maximum((2.0 * degree_f + 1.0) * (degree_f + orders - 1.0) * (degree_f - orders - 1.0), 0.0)
        fall_factor = jnp.sqrt(fall_top / (minus_order * plus_order * jnp.maximum(2.0 * degree_f - 3.0, 1.0)))
        recurred = rise_factor * cosine_col * previous - fall_factor * before_previous
        current = jnp.where(degree_f < orders, 0.0, jnp.where(degree_f == orders, sectoral, recurred))
        return ((current, previous), current)
    unused, values = lax.scan(degree_step, (zeros, zeros), jnp.arange(NB, dtype=jnp.int32))
    return jnp.transpose(values, (1, 3, 0, 2))


def draw_precond_inv(key, part):
    diag_key, noise_key = jax.random.split(jax.random.fold_in(key, 23))
    diagonal = jnp.exp(jax.random.uniform(diag_key, (ORDERS, NB), jnp.float32, 0.0, jnp.log(4.0)))
    random_part = jax.random.normal(noise_key, (ORDERS, NB, NB), jnp.float32) * (0.18 / NB ** 0.5)
    symmetric = (random_part + jnp.transpose(random_part, (0, 2, 1))) / jnp.sqrt(2.0)
    root_diag = jnp.sqrt(diagonal)
    unit = jnp.eye(NB, dtype=jnp.float32)
    return (unit[None, :, :] + symmetric) * root_diag[:, :, None] * root_diag[:, None, :]


def with_ends(drawn, key, least, largest):
    longest = drawn.shape.index(max(drawn.shape))
    spots = []
    for shift in (0, 1):
        where = [jax.random.randint(jax.random.fold_in(key, axis), (), 0, length) for axis, length in enumerate(drawn.shape)]
        where[longest] = (where[longest] + shift) % drawn.shape[longest]
        spots.append(tuple(where))
    return drawn.at[spots[0]].set(least).at[spots[1]].set(largest)


def shard_levels(key, shape, cuts, smallest, top_value):
    factor_of = 1.0
    for position, blocks in cuts:
        steps = jax.random.uniform(jax.random.fold_in(jax.random.fold_in(key, 6), position), (blocks,), jnp.float32, smallest / len(cuts), top_value / len(cuts))
        factor_of = factor_of * jnp.repeat(jnp.exp(steps), shape[position] // blocks).reshape((-1,) + (1,) * (len(shape) - 1 - position))
    return factor_of


def profile(number_of, total, bound, lean):
    loads = [(1 << 20) // math.isqrt(rank ** lean) + 1 for rank in range(2, number_of + 1)]
    rest, given = total - bound - (number_of - 1), [1] * (number_of - 1)
    while rest > 0:
        candidates = [i for i in range(number_of - 1) if given[i] < bound]
        mass, left = sum([loads[i] for i in candidates]), rest
        for i in candidates:
            more = min(bound - given[i], max(1, left * loads[i] // mass), rest)
            given[i] = given[i] + more
            rest = rest - more
    return np.array([bound] + given)


def ragged(key, count, total, limit, lean):
    if count == 2:
        one = jax.random.randint(key, (), max(1, total - limit), min(limit, total - 1) + 1)
        return jnp.stack([one, total - one])
    lengths = jnp.asarray(profile(count, total, limit, lean), jnp.int32)
    couples = (count - 1) // 2
    source_of, sink = lengths[1:1 + 2 * couples:2], lengths[2:2 + 2 * couples:2]
    slack = jnp.minimum(source_of - 1, limit - sink)
    moved = jax.random.randint(jax.random.fold_in(key, 1), (couples,), 0, 1 << 20) % (slack + 1)
    lengths = lengths.at[1:1 + 2 * couples:2].set(source_of - moved).at[2:2 + 2 * couples:2].set(sink + moved)
    return lengths[jax.random.permutation(jax.random.fold_in(key, 2), count)]


def scatter_about(rng, shape, width, limit, cuts=(), held_as=jnp.bfloat16):
    loudness = shard_levels(rng, shape, cuts, -0.22, 0.18) if cuts else 1.0
    drawn = jax.random.normal(rng, shape, jnp.float32) * width * loudness
    return jnp.minimum(jnp.maximum(drawn, -limit), limit).astype(held_as)


def setup_inputs(seed: int = 0) -> dict:
    key_of = jax.random.split(jax.random.key(seed), 9)
    longitude = jnp.clip(jax.random.uniform(key_of[0], (N_OBS, OBS_DEV), jnp.float32, -3.140625, 3.140625), -3.140625, 3.140625)
    cycle_of = jax.vmap(lambda own: jnp.searchsorted(jnp.cumsum(ragged(own, CYCLE_DEV, OBS_DEV, 2 * OBS_DEV // CYCLE_DEV, 1)), jnp.arange(OBS_DEV), side="right"))(jax.random.split(key_of[1], N_OBS)).reshape((N_OBS, OBS_DEV)).astype(jnp.int32)
    obs_count = with_ends(jax.random.randint(key_of[2], (N_OBS,), OBS_DEV // 2, OBS_DEV + 1), jax.random.fold_in(key_of[2], 1), OBS_DEV // 2, OBS_DEV).astype(jnp.int32)
    observed = scatter_about(key_of[3], (N_OBS, OBS_DEV), ((ORDERS * NB) ** 0.5), 1792.0, ((0, 8),), jnp.float32)
    obs_weight = jnp.clip(jnp.exp(math.log(3.0) - 2.3025851 * jax.random.uniform(key_of[4], (N_OBS, OBS_DEV), jnp.float32) ** shard_levels(key_of[4], (N_OBS, OBS_DEV), ((0, 8),), -0.2, 0.2)), 0.3, 3.0)
    legendre = draw_legendre(jax.random.fold_in(key_of[8], 71), 0)
    precond_inv = draw_precond_inv(jax.random.fold_in(key_of[8], 71), 0)
    order_of_slot = jax.random.permutation(key_of[7], ORDERS).astype(jnp.int32)
    return {"longitude": longitude, "cycle_of": cycle_of, "obs_count": obs_count, "observed": observed, "obs_weight": obs_weight, "legendre": legendre, "precond_inv": precond_inv, "order_of_slot": order_of_slot}


PRECISE = lax.Precision.HIGHEST


def harmonic_table(orders, longitudes):
    angles = orders.astype(jnp.float32)[:, None] * longitudes[None, :]
    return jnp.stack([jnp.cos(angles), jnp.sin(angles)], axis=1)


def synthesize(coefficients, legendre_here, harmonic, cycle_ids):
    cycle_values = jnp.einsum("okn,onr->okr", coefficients, legendre_here, precision=PRECISE)
    at_points = jnp.take(cycle_values, cycle_ids, axis=2)
    return jnp.sum(at_points * harmonic, axis=(0, 1))


def adjoint(values, legendre_here, harmonic, cycle_ids):
    weighted = harmonic * values[None, None, :]
    per_cycle = jax.ops.segment_sum(jnp.moveaxis(weighted, 2, 0), cycle_ids, num_segments=legendre_here.shape[2], indices_are_sorted=True)
    return jnp.einsum("rok,onr->okn", per_cycle, legendre_here, precision=PRECISE)


def reference(longitude, cycle_of, obs_count, observed, obs_weight, legendre, precond_inv, order_of_slot):
    orders = jnp.arange(ORDERS, dtype=jnp.int32)
    slot_of_order = jnp.sum(jnp.where(order_of_slot[None, :] == orders[:, None], orders[None, :], 0), axis=1).astype(jnp.int32)
    live_mask = (jnp.arange(NB, dtype=jnp.int32)[None, None, :] >= order_of_slot[:, None, None]).astype(jnp.float32)
    positions = jnp.arange(OBS_DEV, dtype=jnp.int32)
    obs_scale = obs_weight * (positions[None, :] < obs_count[:, None]).astype(jnp.float32) / (N_OBS * OBS_DEV)

    def owner_adjoint(values):
        def slab_step(accumulated, slab_data):
            east, cycle_ids, slab_values, legendre_here = slab_data
            harmonic = harmonic_table(orders, east)
            return accumulated + adjoint(slab_values, legendre_here, harmonic, cycle_ids), None

        accumulated, unused = lax.scan(slab_step, jnp.zeros((ORDERS, 2, NB), jnp.float32), (longitude, cycle_of, values, legendre))
        return jnp.take(accumulated, order_of_slot, axis=0)

    def normal_image(direction):
        coefficients = jnp.take(direction, slot_of_order, axis=0)

        def slab_step(accumulated, slab_data):
            east, cycle_ids, slab_scale, legendre_here = slab_data
            harmonic = harmonic_table(orders, east)
            gradient = synthesize(coefficients, legendre_here, harmonic, cycle_ids)
            return accumulated + adjoint(slab_scale * gradient, legendre_here, harmonic, cycle_ids), None

        accumulated, unused = lax.scan(slab_step, jnp.zeros((ORDERS, 2, NB), jnp.float32), (longitude, cycle_of, obs_scale, legendre))
        return jnp.take(accumulated, order_of_slot, axis=0)

    def precondition(values):
        return live_mask * jnp.einsum("snj,skj->skn", precond_inv, values, precision=PRECISE)

    residual = owner_adjoint(obs_scale * observed)
    solution = jnp.zeros_like(residual)
    precond = precondition(residual)
    direction = precond
    energy_now = jnp.sum(residual * precond)
    for iteration in range(ITERS):
        image = normal_image(direction)
        step_size = energy_now / jnp.sum(direction * image)
        solution = solution + step_size * direction
        residual = residual - step_size * image
        if iteration + 1 < ITERS:
            precond = precondition(residual)
            energy_next = jnp.sum(residual * precond)
            direction = precond + (energy_next / energy_now) * direction
            energy_now = energy_next
    return solution, residual
```

```python
import functools

import jax
import jax.numpy as jnp
from jax import lax
from jax.experimental import pallas as pl
from jax.experimental.pallas import tpu as pltpu
from jax.sharding import PartitionSpec as P

ITERS = 2
MESH = pl.DeviceIdType.MESH
LANES = 128
SLOTS = 256
CYCLES_HERE = 8
GROUP = 20
GROUPS = 5
SHARE = 8 * GROUPS
SCALAR_LANE = 127
CURVE_COLUMN = 18
TWO_OVER_PI = 0.6366197723675814
PI_2_A = 1.5703125
PI_2_B = 0.00048351287841796875
PI_2_C = 3.13855707645416259765625e-07
PI_2_D = 6.077100628276710e-11


def sine_cosine(angle):
    turns = jnp.floor(angle * TWO_OVER_PI + 0.5)
    rest = angle - turns * PI_2_A
    rest = rest - turns * PI_2_B
    rest = rest - turns * PI_2_C
    rest = rest - turns * PI_2_D
    square = rest * rest
    sine = rest + rest * square * (-1.6666654611e-1 + square * (8.3321608736e-3 + square * -1.9515295891e-4))
    cosine = 1.0 - 0.5 * square + square * square * (
        4.166664568298827e-2 + square * (-1.388731625493765e-3 + square * 2.443315711809948e-5)
    )
    quadrant = turns.astype(jnp.int32)
    swap = (quadrant & 1) == 1
    sine_out = jnp.where(swap, cosine, sine)
    cosine_out = jnp.where(swap, sine, cosine)
    sine_out = jnp.where((quadrant & 2) == 2, -sine_out, sine_out)
    cosine_out = jnp.where(((quadrant + 1) & 2) == 2, -cosine_out, cosine_out)
    return sine_out, cosine_out


def prologue_kernel(total_obs, count_ref, cycle_ref, lon_ref, obs_ref, weight_ref, lon_out, scale_out, first_out):
    first_cycle = lax.axis_index("ord") * CYCLES_HERE
    rows = cycle_ref.shape[0]
    ids = cycle_ref[...]
    starts = []
    for step in range(CYCLES_HERE + 1):
        below = jnp.where(ids < first_cycle + step, 1.0, 0.0)
        starts.append(jnp.sum(below).astype(jnp.int32))
    lane = lax.broadcasted_iota(jnp.int32, (1, LANES), 1)
    used = count_ref[0]
    for step in range(CYCLES_HERE):
        start = starts[step]
        count = starts[step + 1] - start
        row = start // LANES
        shift = start - row * LANES
        turn = lax.rem(LANES - shift, LANES)
        lines = [jnp.minimum(row + part, rows - 1) for part in range(3)]
        head = lane < LANES - shift
        windows = []
        for ref in (lon_ref, obs_ref, weight_ref):
            turned = [pltpu.roll(ref[pl.ds(line, 1), :], turn, 1) for line in lines]
            windows.append([jnp.where(head, turned[part], turned[part + 1]) for part in range(2)])
        for part in range(2):
            slot = lane + part * LANES
            valid = jnp.logical_and(slot < count, start + slot < used)
            scale = jnp.where(valid, windows[2][part] / total_obs, 0.0)
            cut = pl.ds(part * LANES, LANES)
            lon_out[pl.ds(step, 1), cut] = windows[0][part]
            scale_out[pl.ds(step, 1), cut] = scale
            first_out[pl.ds(step, 1), cut] = scale * windows[1][part]


def offset(index):
    return ((index + 1) // 2) * (1 - 2 * (index % 2))


def main_kernel(
    dims, own_ref, lon_ref, scale_ref, first_ref, leg_hbm, inv_hbm, solution_ref, residual_ref,
    harm, leg, inv, column, rows_ref, tile_send, tile_recv, part_send, part_recv, share_send, share_recv,
    all_send, all_recv, ids_send, ids_recv, ids_smem, slot_smem, local_sem, send_sem, recv_sem,
):
    block, degrees, cycles, ord_y, ord_z, obs_x = dims
    ords = ord_y * ord_z
    obss = obs_x * 2
    columns = 2 * block
    ord_here = lax.axis_index("ord")
    obs_here = lax.axis_index("obs")

    for slot in range(block):
        inv[slot, pl.ds(degrees, SHARE * obss - degrees), :] = jnp.zeros((SHARE * obss - degrees, degrees), jnp.float32)
    leg_copy = pltpu.make_async_copy(leg_hbm, leg, local_sem.at[0])
    inv_copy = pltpu.make_async_copy(inv_hbm, inv.at[:, pl.ds(0, degrees), :], local_sem.at[1])
    leg_copy.start()
    inv_copy.start()

    def ord_peer(index):
        step_y = ord_y // 2 + offset(index // ord_z)
        step_z = ord_z // 2 + offset(index % ord_z)
        here_y = ord_here // ord_z
        here_z = ord_here % ord_z
        return ((here_y + step_y) % ord_y) * ord_z + (here_z + step_z) % ord_z

    def obs_peer(index):
        step_x = obs_x // 2 + offset(index // 2)
        step_core = 1 - index % 2
        return ((obs_here // 2 + step_x) % obs_x) * 2 + (obs_here % 2 + step_core) % 2

    barrier = pltpu.get_barrier_semaphore()

    def greet_ord(index, carry):
        pl.semaphore_signal(barrier, inc=1, device_id={"ord": ord_peer(index)}, device_id_type=MESH)
        return carry

    def greet_obs(index, carry):
        pl.semaphore_signal(barrier, inc=1, device_id={"obs": obs_peer(index)}, device_id_type=MESH)
        return carry

    lax.fori_loop(0, ords - 1, greet_ord, 0)
    lax.fori_loop(0, obss - 1, greet_obs, 0)

    lane = lax.broadcasted_iota(jnp.int32, (8, LANES), 1)
    sublane = lax.broadcasted_iota(jnp.int32, (8, LANES), 0)
    group = lane // GROUP
    inner = lane % GROUP
    slot_lane = inner // 2
    degree_here = obs_here * SHARE + group * 8 + sublane
    inside = jnp.logical_and(jnp.logical_and(group < GROUPS, inner < columns), degree_here < degrees)
    order_lane = jnp.zeros((8, LANES), jnp.int32)
    for slot in range(block):
        order_lane = jnp.where(slot_lane == slot, own_ref[slot], order_lane)
    live = jnp.logical_and(inside, degree_here >= order_lane)

    ids_row = jnp.zeros((1, LANES), jnp.int32)
    lane_row = lax.broadcasted_iota(jnp.int32, (1, LANES), 1)
    for slot in range(block):
        ids_row = jnp.where(lane_row == slot, own_ref[slot], ids_row)
    ids_send[...] = ids_row
    ids_recv[ord_here] = ids_row
    for which in range(len(rows_ref)):
        rows_ref[which][...] = jnp.zeros((32, cycles), jnp.float32)
    column[...] = jnp.zeros(column.shape, jnp.float32)

    longitude = lon_ref[...]

    def harmonic_block(index, carry):
        for order in range(block):
            number = (index * block + order).astype(jnp.float32)
            sine, cosine = sine_cosine(number * longitude)
            harm[index, 2 * order] = cosine
            harm[index, 2 * order + 1] = sine
        return carry

    lax.fori_loop(0, ords, harmonic_block, 0)
    pl.semaphore_wait(barrier, ords - 1 + obss - 1)

    rounds = [0]
    waits = []

    def next_round():
        rounds[0] += 1
        return rounds[0] - 1

    def ord_copy(source, target, sems, peer):
        return pltpu.make_async_remote_copy(
            src_ref=source, dst_ref=target, send_sem=send_sem.at[sems], recv_sem=recv_sem.at[sems],
            device_id={"ord": peer}, device_id_type=MESH,
        )

    def obs_copy(source, target, sems, peer):
        return pltpu.make_async_remote_copy(
            src_ref=source, dst_ref=target, send_sem=send_sem.at[sems], recv_sem=recv_sem.at[sems],
            device_id={"obs": peer}, device_id_type=MESH,
        )

    def whole(make, buffer, sems, peers, peer):
        cut = buffer.at[pl.ds(0, peers)]
        return make(cut, cut, sems, peer)

    def gather_ord(source, buffer):
        sems = next_round()

        def send(index, carry):
            ord_copy(source, buffer.at[ord_here], sems, ord_peer(index)).start()
            return carry

        lax.fori_loop(0, ords - 1, send, 0)
        done = whole(ord_copy, buffer, sems, ords - 1, ord_peer(0))
        waits.append(done)
        return done

    def gather_obs(source, buffer):
        sems = next_round()

        def send(index, carry):
            obs_copy(source, buffer.at[obs_here], sems, obs_peer(index)).start()
            return carry

        lax.fori_loop(0, obss - 1, send, 0)
        done = whole(obs_copy, buffer, sems, obss - 1, obs_peer(0))
        waits.append(done)
        return done

    ids_done = gather_ord(ids_send, ids_recv)

    tiles = [0]
    parts = [0]
    shares = [0]
    alls = [0]

    def per_cycle(weighted, curve):
        which = tiles[0]
        tiles[0] += 1
        sems = next_round()
        send_buf, recv_buf = tile_send[which], tile_recv[which]
        corner = jnp.logical_and(lane == CURVE_COLUMN, sublane == 0)
        empty = jnp.where(corner, curve, 0.0)

        def step(outer, carry):
            for inner_step in range(4):
                index = outer * 4 + inner_step
                peer = ord_peer(index)
                tile = empty
                for col in range(columns):
                    total = jnp.sum(harm[peer, col] * weighted, axis=1, keepdims=True)
                    tile = jnp.where(lane == col, total, tile)
                send_buf[peer] = tile
                if inner_step < 3:
                    ord_copy(send_buf.at[peer], recv_buf.at[ord_here], sems, peer).start()
                else:
                    @pl.when(index < ords - 1)
                    def _():
                        ord_copy(send_buf.at[peer], recv_buf.at[ord_here], sems, peer).start()

                    @pl.when(index == ords - 1)
                    def _():
                        recv_buf[ord_here] = tile
            return carry

        lax.fori_loop(0, ords // 4, step, 0)
        done = whole(ord_copy, recv_buf, sems, ords - 1, ord_peer(0))
        waits.append(done)
        return done, recv_buf

    def adjoint(recv_buf, rows):
        per_order = jnp.transpose(recv_buf[...].reshape(cycles, LANES)[:, :32])
        rows[...] = per_order
        curve = jnp.sum(rows[pl.ds(CURVE_COLUMN, 1), :], axis=1, keepdims=True)
        lane_all = lax.broadcasted_iota(jnp.int32, (degrees, LANES), 1)
        total = jnp.zeros((degrees, LANES), jnp.float32)
        for order in range(block):
            table = leg[order]
            for part in range(2):
                col = 2 * order + part
                value = jnp.sum(table * rows[pl.ds(col, 1), :], axis=1, keepdims=True)
                total = jnp.where(lane_all == col, value, total)
        column[pl.ds(0, degrees), :] = total
        which = parts[0]
        parts[0] += 1
        send_buf, recv_obs = part_send[which], part_recv[which]
        for owner in range(obss):
            packed = jnp.where(lane == SCALAR_LANE, curve, 0.0)
            for piece in range(GROUPS):
                start = owner * SHARE + piece * 8
                if start < degrees:
                    lines = column[pl.ds(start, 8), :]
                    packed = packed + (pltpu.roll(lines, GROUP * piece, 1) if piece else lines)
            send_buf[owner] = packed
        sems = next_round()

        def send(index, carry):
            peer = obs_peer(index)
            obs_copy(send_buf.at[peer], recv_obs.at[obs_here], sems, peer).start()
            return carry

        lax.fori_loop(0, obss - 1, send, 0)
        recv_obs[obs_here] = send_buf[obs_here]
        done = whole(obs_copy, recv_obs, sems, obss - 1, obs_peer(0))
        waits.append(done)
        done.wait_recv()
        summed = jnp.sum(recv_obs[...], axis=0)
        return summed, summed[0:1, SCALAR_LANE : SCALAR_LANE + 1]

    def exchange_ord(packed, index_ref):
        which = shares[0]
        shares[0] += 1
        send_buf, recv_buf = share_send[which], share_recv[which]
        send_buf[...] = packed
        recv_buf[ord_here] = packed
        gather_ord(send_buf, recv_buf).wait_recv()
        everyone = jnp.sum(recv_buf[...], axis=0)
        chosen = jnp.where(lane == SCALAR_LANE, everyone, 0.0)
        for slot in range(block):
            number = index_ref[slot]
            source = number // block
            place = number - source * block
            turn = lax.rem(2 * slot - 2 * place + LANES, LANES)
            lines = pltpu.roll(recv_buf[source], turn, 1)
            chosen = jnp.where(jnp.logical_and(inside, slot_lane == slot), lines, chosen)
        return chosen

    def exchange_obs(packed):
        which = alls[0]
        alls[0] += 1
        send_buf, recv_buf = all_send[which], all_recv[which]
        send_buf[...] = packed
        recv_buf[obs_here] = packed
        gather_obs(send_buf, recv_buf).wait_recv()
        total = jnp.sum(recv_buf[...], axis=0)[0:1, SCALAR_LANE : SCALAR_LANE + 1]
        pieces = []
        for owner in range(obss):
            for piece in range(GROUPS):
                if owner * SHARE + piece * 8 < degrees:
                    lines = recv_buf[owner]
                    pieces.append(pltpu.roll(lines, LANES - GROUP * piece, 1) if piece else lines)
        return jnp.concatenate(pieces, axis=0), total

    def precondition(packed):
        lines, unused = exchange_obs(packed)
        column[pl.ds(0, degrees), :] = lines
        by_slot = jnp.transpose(column[...])
        start = pl.multiple_of(obs_here * SHARE, 8)
        result = jnp.zeros((8, LANES), jnp.float32)
        for slot in range(block):
            table = inv[slot, pl.ds(start, SHARE), :]
            for part in range(2):
                col = 2 * slot + part
                value = jnp.sum(table * by_slot[col : col + 1, :degrees], axis=1, keepdims=True)
                for piece in range(GROUPS):
                    result = jnp.where(lane == GROUP * piece + col, value[8 * piece : 8 * piece + 8], result)
        return jnp.where(live, result, 0.0)

    def with_energy(residual, precond):
        product = jnp.where(inside, residual * precond, 0.0)
        share = jnp.sum(jnp.sum(product, axis=1, keepdims=True), axis=0, keepdims=True)
        return jnp.where(lane == SCALAR_LANE, share, precond)

    def synthesize(coefficients, rows):
        which = tiles[0]
        tiles[0] += 1
        sems = next_round()
        send_buf, recv_buf = tile_send[which], tile_recv[which]
        for order in range(block):
            table = leg[order]
            for part in range(2):
                col = 2 * order + part
                rows[pl.ds(col, 1), :] = jnp.sum(table * coefficients[:, col : col + 1], axis=0, keepdims=True)
        turned = jnp.transpose(rows[...]).reshape(ords, CYCLES_HERE, 32)
        send_buf[:, :, pl.ds(0, 32)] = turned
        recv_buf[ord_here] = send_buf[ord_here]

        def send(index, carry):
            peer = ord_peer(index)
            ord_copy(send_buf.at[peer], recv_buf.at[ord_here], sems, peer).start()
            return carry

        lax.fori_loop(0, ords - 1, send, 0)
        done = whole(ord_copy, recv_buf, sems, ords - 1, ord_peer(0))
        waits.append(done)
        done.wait_recv()

        def step(outer, sums):
            sums = list(sums)
            for inner_step in range(4):
                index = outer * 4 + inner_step
                tile = recv_buf[index]
                for col in range(columns):
                    sums[col % 2] = sums[col % 2] + harm[index, col] * tile[:, col : col + 1]
            return tuple(sums)

        zero = jnp.zeros((CYCLES_HERE, SLOTS), jnp.float32)
        sums = lax.fori_loop(0, ords // 4, step, (zero, zero))
        return sums[0] + sums[1]

    leg_copy.wait()
    done, recv_buf = per_cycle(first_ref[...], jnp.zeros((1, 1), jnp.float32))

    ids_done.wait_recv()
    ids_copy = pltpu.make_async_copy(ids_recv, ids_smem, local_sem.at[2])
    ids_copy.start()
    ids_copy.wait()
    first_order = ord_here * block

    def find(owner, found):
        found = list(found)
        for slot in range(block):
            number = ids_smem[owner, 0, slot]
            for order in range(block):
                found[order] = jnp.where(number == first_order + order, owner * block + slot, found[order])
        return tuple(found)

    found = lax.fori_loop(0, ords, find, tuple(jnp.int32(0) for unused in range(block)))
    for order in range(block):
        slot_smem[order] = found[order]
    inv_copy.wait()

    done.wait_recv()
    summed, unused = adjoint(recv_buf, rows_ref[0])
    residual = exchange_ord(summed, own_ref)
    residual = jnp.where(inside, residual, 0.0)
    precond = precondition(residual)
    solution = jnp.zeros((8, LANES), jnp.float32)
    direction = None
    coefficients = None
    energy_now = None
    for iteration in range(ITERS):
        chosen = exchange_ord(with_energy(residual, precond), slot_smem)
        lines, energy = exchange_obs(chosen)
        if iteration == 0:
            direction, coefficients = precond, lines
        else:
            ratio = energy / energy_now
            direction = precond + ratio * direction
            coefficients = lines + ratio * coefficients
        energy_now = energy
        gradient = synthesize(coefficients, rows_ref[1])
        weighted = scale_ref[...] * gradient
        curve = jnp.sum(jnp.sum(weighted * gradient, axis=1, keepdims=True), axis=0, keepdims=True)
        done, recv_buf = per_cycle(weighted, curve)
        done.wait_recv()
        summed, curvature = adjoint(recv_buf, rows_ref[0])
        image = jnp.where(inside, exchange_ord(summed, own_ref), 0.0)
        step_size = energy_now / curvature
        solution = solution + step_size * direction
        residual = residual - step_size * image
        if iteration + 1 < ITERS:
            precond = precondition(residual)

    for value, out in ((solution, solution_ref), (residual, residual_ref)):
        lines, unused = exchange_obs(value)
        column[pl.ds(0, degrees), :] = lines
        by_slot = jnp.transpose(column[...])
        for slot in range(block):
            out[slot] = by_slot[2 * slot : 2 * slot + 2, :degrees]
    for done in waits:
        done.wait_send()


def buffers(rounds, *shape):
    return [pltpu.VMEM(shape, jnp.float32) for unused in range(rounds)]


def body(ord_y, ord_z, obs_x, longitude, cycle_of, obs_count, observed, obs_weight, legendre, precond_inv, order_of_slot):
    block, degrees, cycles = legendre.shape[1:]
    slab = longitude.shape[1]
    ords, obss = ord_y * ord_z, obs_x * 2
    vmem = pl.BlockSpec(memory_space=pltpu.VMEM)
    smem = pl.BlockSpec(memory_space=pltpu.SMEM)
    hbm = pl.BlockSpec(memory_space=pl.ANY)
    window = jax.ShapeDtypeStruct((CYCLES_HERE, SLOTS), jnp.float32)
    lines = (slab // LANES, LANES)
    east, scale, first = pl.pallas_call(
        functools.partial(prologue_kernel, float(slab * obss)),
        out_shape=(window, window, window),
        in_specs=[smem, vmem, vmem, vmem, vmem],
        out_specs=(vmem, vmem, vmem),
        name="windows",
    )(obs_count, cycle_of.reshape(lines), longitude.reshape(lines), observed.reshape(lines), obs_weight.reshape(lines))
    result = jax.ShapeDtypeStruct((block, 2, degrees), jnp.float32)
    dims = (block, degrees, cycles, ord_y, ord_z, obs_x)
    column_rows = -(-max(degrees, 1) // LANES) * LANES
    tile_rounds = 1 + 2 * ITERS
    share_rounds = 1 + 2 * ITERS
    all_rounds = 2 * ITERS + 2
    total_rounds = 1 + tile_rounds + (1 + ITERS) + share_rounds + all_rounds
    scratch = [
        pltpu.VMEM((ords, 2 * block, CYCLES_HERE, SLOTS), jnp.float32),
        pltpu.VMEM((block, degrees, cycles), jnp.float32),
        pltpu.VMEM((block, SHARE * obss, degrees), jnp.float32),
        pltpu.VMEM((column_rows, LANES), jnp.float32),
        [pltpu.VMEM((32, cycles), jnp.float32), pltpu.VMEM((32, cycles), jnp.float32)],
        buffers(tile_rounds, ords, CYCLES_HERE, LANES),
        buffers(tile_rounds, ords, CYCLES_HERE, LANES),
        buffers(1 + ITERS, obss, 8, LANES),
        buffers(1 + ITERS, obss, 8, LANES),
        buffers(share_rounds, 8, LANES),
        buffers(share_rounds, ords, 8, LANES),
        buffers(all_rounds, 8, LANES),
        buffers(all_rounds, obss, 8, LANES),
        pltpu.VMEM((1, LANES), jnp.int32),
        pltpu.VMEM((ords, 1, LANES), jnp.int32),
        pltpu.SMEM((ords, 1, LANES), jnp.int32),
        pltpu.SMEM((block,), jnp.int32),
        pltpu.SemaphoreType.DMA((3,)),
        pltpu.SemaphoreType.DMA((total_rounds,)),
        pltpu.SemaphoreType.DMA((total_rounds,)),
    ]
    return pl.pallas_call(
        functools.partial(main_kernel, dims),
        out_shape=(result, result),
        in_specs=[smem, vmem, vmem, vmem, hbm, hbm],
        out_specs=(vmem, vmem),
        scratch_shapes=scratch,
        compiler_params=pltpu.CompilerParams(
            collective_id=0, has_side_effects=True, vmem_limit_bytes=48 * 1024 * 1024
        ),
        name="solve",
    )(order_of_slot, east, scale, first, legendre[0], precond_inv)


def solution(mesh):
    placed = (
        P("obs", None),
        P("obs", None),
        P("obs"),
        P("obs", None),
        P("obs", None),
        P("obs", "ord", None, None),
        P("ord", None, None),
        P("ord"),
    )
    ords = mesh.shape["ord"]
    ord_y = 4 if ords == 32 else 2
    run = functools.partial(body, ord_y, ords // ord_y, mesh.shape["obs"] // 2)
    return jax.shard_map(
        run,
        mesh=mesh,
        in_specs=placed,
        out_specs=(P("ord", None, None), P("ord", None, None)),
        check_vma=False,
    )
```

```python
import functools

import jax
import jax.numpy as jnp
from jax import lax
from jax.experimental import pallas as pl
from jax.experimental.pallas import tpu as pltpu
from jax.sharding import PartitionSpec as P

ITERS = 2
MESH = pl.DeviceIdType.MESH
LANES = 128
SLOTS = 256
CYCLES_HERE = 8
GROUP = 20
GROUPS = 5
SHARE = 8 * GROUPS
SCALAR_LANE = 127
CURVE_COLUMN = 18
TWO_OVER_PI = 0.6366197723675814
PI_2_A = 1.5703125
PI_2_B = 0.00048351287841796875
PI_2_C = 3.13855707645416259765625e-07
PI_2_D = 6.077100628276710e-11


def sine_cosine(angle):
    turns = jnp.floor(angle * TWO_OVER_PI + 0.5)
    rest = angle - turns * PI_2_A
    rest = rest - turns * PI_2_B
    rest = rest - turns * PI_2_C
    rest = rest - turns * PI_2_D
    square = rest * rest
    sine = rest + rest * square * (-1.6666654611e-1 + square * (8.3321608736e-3 + square * -1.9515295891e-4))
    cosine = 1.0 - 0.5 * square + square * square * (
        4.166664568298827e-2 + square * (-1.388731625493765e-3 + square * 2.443315711809948e-5)
    )
    quadrant = turns.astype(jnp.int32)
    swap = (quadrant & 1) == 1
    sine_out = jnp.where(swap, cosine, sine)
    cosine_out = jnp.where(swap, sine, cosine)
    sine_out = jnp.where((quadrant & 2) == 2, -sine_out, sine_out)
    cosine_out = jnp.where(((quadrant + 1) & 2) == 2, -cosine_out, cosine_out)
    return sine_out, cosine_out


def prologue_kernel(total_obs, count_ref, cycle_ref, lon_ref, obs_ref, weight_ref, out_ref):
    first_cycle = lax.axis_index("ord") * CYCLES_HERE
    rows = cycle_ref.shape[0]
    ids = cycle_ref[...]
    starts = []
    for step in range(CYCLES_HERE + 1):
        below = jnp.where(ids < first_cycle + step, 1.0, 0.0)
        starts.append(jnp.sum(below).astype(jnp.int32))
    lane = lax.broadcasted_iota(jnp.int32, (1, LANES), 1)
    used = count_ref[0]
    for step in range(CYCLES_HERE):
        start = starts[step]
        count = starts[step + 1] - start
        row = start // LANES
        shift = start - row * LANES
        turn = lax.rem(LANES - shift, LANES)
        lines = [jnp.minimum(row + part, rows - 1) for part in range(3)]
        head = lane < LANES - shift
        windows = []
        for ref in (lon_ref, obs_ref, weight_ref):
            turned = [pltpu.roll(ref[pl.ds(line, 1), :], turn, 1) for line in lines]
            windows.append([jnp.where(head, turned[part], turned[part + 1]) for part in range(2)])
        for part in range(2):
            slot = lane + part * LANES
            valid = jnp.logical_and(slot < count, start + slot < used)
            scale = jnp.where(valid, windows[2][part] / total_obs, 0.0)
            cut = pl.ds(part * LANES, LANES)
            for which, value in enumerate((windows[0][part], scale, scale * windows[1][part])):
                out_ref[pl.ds(which * CYCLES_HERE + step, 1), cut] = value


def offset(index):
    return ((index + 1) // 2) * (1 - 2 * (index % 2))


def main_kernel(
    dims, own_ref, windows_ref, leg_hbm, inv_hbm, solution_ref, residual_ref,
    harm, leg, inv, column, rows_ref, tile_send, tile_recv, part_send, part_recv, share_send, share_recv,
    all_send, all_recv, ids_send, ids_recv, ids_smem, slot_smem, local_sem, send_sem, recv_sem,
):
    block, degrees, cycles, ord_y, ord_z, obs_x = dims
    ords = ord_y * ord_z
    obss = obs_x * 2
    columns = 2 * block
    unroll = 2 * ord_y
    ord_here = lax.axis_index("ord")
    obs_here = lax.axis_index("obs")

    for slot in range(block):
        inv[slot, pl.ds(degrees, SHARE * obss - degrees), :] = jnp.zeros((SHARE * obss - degrees, degrees), jnp.float32)
    leg_copy = pltpu.make_async_copy(leg_hbm, leg, local_sem.at[0])
    inv_copy = pltpu.make_async_copy(inv_hbm, inv.at[:, pl.ds(0, degrees), :], local_sem.at[1])
    leg_copy.start()
    inv_copy.start()

    here_y, here_z = lax.div(ord_here, ord_z), lax.rem(ord_here, ord_z)
    here_x, here_core = lax.div(obs_here, 2), lax.rem(obs_here, 2)

    def ord_at(step_y, step_z):
        return lax.rem(here_y + step_y, ord_y) * ord_z + lax.rem(here_z + step_z, ord_z)

    def ord_peer(index):
        return ord_at(ord_y // 2 + offset(index % ord_y), ord_z // 2 + offset(index // ord_y))

    def obs_peer(index):
        step_x = obs_x // 2 + offset(index // 2)
        step_core = 1 - index % 2
        return lax.rem(here_x + step_x, obs_x) * 2 + lax.rem(here_core + step_core, 2)

    barrier = pltpu.get_barrier_semaphore()

    for index in range(ords - 1):
        pl.semaphore_signal(barrier, inc=1, device_id={"ord": ord_peer(index)}, device_id_type=MESH)
    for index in range(obss - 1):
        pl.semaphore_signal(barrier, inc=1, device_id={"obs": obs_peer(index)}, device_id_type=MESH)

    lane = lax.broadcasted_iota(jnp.int32, (8, LANES), 1)
    sublane = lax.broadcasted_iota(jnp.int32, (8, LANES), 0)
    group = lane // GROUP
    inner = lane % GROUP
    slot_lane = inner // 2
    degree_here = obs_here * SHARE + group * 8 + sublane
    inside = jnp.logical_and(jnp.logical_and(group < GROUPS, inner < columns), degree_here < degrees)
    order_lane = jnp.zeros((8, LANES), jnp.int32)
    for slot in range(block):
        order_lane = jnp.where(slot_lane == slot, own_ref[slot], order_lane)
    live = jnp.logical_and(inside, degree_here >= order_lane)

    ids_row = jnp.zeros((1, LANES), jnp.int32)
    lane_row = lax.broadcasted_iota(jnp.int32, (1, LANES), 1)
    for slot in range(block):
        ids_row = jnp.where(lane_row == slot, own_ref[slot], ids_row)
    ids_send[...] = ids_row
    ids_recv[ord_here] = ids_row
    for which in range(len(rows_ref)):
        rows_ref[which][...] = jnp.zeros((32, cycles), jnp.float32)
    column[...] = jnp.zeros(column.shape, jnp.float32)

    longitude = windows_ref[pl.ds(0, CYCLES_HERE), :]

    def harmonic_block(index, carry):
        for order in range(block):
            number = (index * block + order).astype(jnp.float32)
            sine, cosine = sine_cosine(number * longitude)
            harm[index, 2 * order] = cosine
            harm[index, 2 * order + 1] = sine
        return carry

    lax.fori_loop(0, ords, harmonic_block, 0)
    pl.semaphore_wait(barrier, ords - 1 + obss - 1)

    rounds = [0]
    waits = []

    def next_round():
        rounds[0] += 1
        return rounds[0] - 1

    def ord_copy(source, target, sems, peer):
        return pltpu.make_async_remote_copy(
            src_ref=source, dst_ref=target, send_sem=send_sem.at[sems], recv_sem=recv_sem.at[sems],
            device_id={"ord": peer}, device_id_type=MESH,
        )

    def obs_copy(source, target, sems, peer):
        return pltpu.make_async_remote_copy(
            src_ref=source, dst_ref=target, send_sem=send_sem.at[sems], recv_sem=recv_sem.at[sems],
            device_id={"obs": peer}, device_id_type=MESH,
        )

    def whole(make, buffer, sems, peers, peer):
        cut = buffer.at[pl.ds(0, peers)]
        return make(cut, cut, sems, peer)

    def gather_ord(source, buffer):
        sems = next_round()

        def send(index, carry):
            ord_copy(source, buffer.at[ord_here], sems, ord_peer(index)).start()
            return carry

        lax.fori_loop(0, ords - 1, send, 0)
        done = whole(ord_copy, buffer, sems, ords - 1, ord_peer(0))
        waits.append(done)
        return done

    def gather_obs(source, buffer):
        sems = next_round()

        def send(index, carry):
            obs_copy(source, buffer.at[obs_here], sems, obs_peer(index)).start()
            return carry

        lax.fori_loop(0, obss - 1, send, 0)
        done = whole(obs_copy, buffer, sems, obss - 1, obs_peer(0))
        waits.append(done)
        return done

    tiles = [0]
    parts = [0]
    shares = [0]
    alls = [0]

    def per_cycle(weighted, curve):
        which = tiles[0]
        tiles[0] += 1
        sems = next_round()
        send_buf, recv_buf = tile_send[which], tile_recv[which]
        corner = jnp.logical_and(lane == CURVE_COLUMN, sublane == 0)
        empty = jnp.where(corner, curve, 0.0)

        def step(outer, carry):
            for inner_step in range(unroll):
                index = outer * unroll + inner_step
                peer = ord_at(
                    ord_y // 2 + offset(inner_step % ord_y), ord_z // 2 + offset(outer * (unroll // ord_y) + inner_step // ord_y)
                )
                tile = empty
                for col in range(columns):
                    total = jnp.sum(harm[peer, col] * weighted, axis=1, keepdims=True)
                    tile = jnp.where(lane == col, total, tile)
                send_buf[peer] = tile
                if inner_step < unroll - 1:
                    ord_copy(send_buf.at[peer], recv_buf.at[ord_here], sems, peer).start()
                else:
                    @pl.when(index < ords - 1)
                    def _():
                        ord_copy(send_buf.at[peer], recv_buf.at[ord_here], sems, peer).start()

                    @pl.when(index == ords - 1)
                    def _():
                        recv_buf[ord_here] = tile
            return carry

        lax.fori_loop(0, ords // unroll, step, 0)
        done = whole(ord_copy, recv_buf, sems, ords - 1, ord_peer(0))
        waits.append(done)
        return done, recv_buf

    def adjoint(recv_buf, rows):
        per_order = jnp.transpose(recv_buf[...].reshape(cycles, LANES)[:, :32])
        rows[...] = per_order
        curve = jnp.sum(rows[pl.ds(CURVE_COLUMN, 1), :], axis=1, keepdims=True)
        lane_all = lax.broadcasted_iota(jnp.int32, (degrees, LANES), 1)
        total = jnp.zeros((degrees, LANES), jnp.float32)
        for order in range(block):
            table = leg[order]
            for part in range(2):
                col = 2 * order + part
                value = jnp.sum(table * rows[pl.ds(col, 1), :], axis=1, keepdims=True)
                total = jnp.where(lane_all == col, value, total)
        column[pl.ds(0, degrees), :] = total
        which = parts[0]
        parts[0] += 1
        send_buf, recv_obs = part_send[which], part_recv[which]
        for owner in range(obss):
            packed = jnp.where(lane == SCALAR_LANE, curve, 0.0)
            for piece in range(GROUPS):
                start = owner * SHARE + piece * 8
                if start < degrees:
                    lines = column[pl.ds(start, 8), :]
                    packed = packed + (pltpu.roll(lines, GROUP * piece, 1) if piece else lines)
            send_buf[owner] = packed
        sems = next_round()

        def send(index, carry):
            peer = obs_peer(index)
            obs_copy(send_buf.at[peer], recv_obs.at[obs_here], sems, peer).start()
            return carry

        lax.fori_loop(0, obss - 1, send, 0)
        recv_obs[obs_here] = send_buf[obs_here]
        done = whole(obs_copy, recv_obs, sems, obss - 1, obs_peer(0))
        waits.append(done)
        done.wait_recv()
        summed = jnp.sum(recv_obs[...], axis=0)
        return summed, summed[0:1, SCALAR_LANE : SCALAR_LANE + 1]

    def exchange_ord(packed, index_ref):
        which = shares[0]
        shares[0] += 1
        send_buf, recv_buf = share_send[which], share_recv[which]
        send_buf[...] = packed
        recv_buf[ord_here] = packed
        gather_ord(send_buf, recv_buf).wait_recv()
        everyone = jnp.sum(recv_buf[...], axis=0)
        chosen = jnp.where(lane == SCALAR_LANE, everyone, 0.0)
        for slot in range(block):
            number = index_ref[slot]
            source = number // block
            place = number - source * block
            turn = lax.rem(2 * slot - 2 * place + LANES, LANES)
            lines = pltpu.roll(recv_buf[source], turn, 1)
            chosen = jnp.where(jnp.logical_and(inside, slot_lane == slot), lines, chosen)
        return chosen

    def send_obs(packed):
        which = alls[0]
        alls[0] += 1
        send_buf, recv_buf = all_send[which], all_recv[which]
        send_buf[...] = packed
        recv_buf[obs_here] = packed
        return gather_obs(send_buf, recv_buf), recv_buf

    def take_obs(sent):
        done, recv_buf = sent
        done.wait_recv()
        total = jnp.sum(recv_buf[...], axis=0)[0:1, SCALAR_LANE : SCALAR_LANE + 1]
        pieces = []
        for owner in range(obss):
            for piece in range(GROUPS):
                if owner * SHARE + piece * 8 < degrees:
                    lines = recv_buf[owner]
                    pieces.append(pltpu.roll(lines, LANES - GROUP * piece, 1) if piece else lines)
        return jnp.concatenate(pieces, axis=0), total

    def exchange_obs(packed):
        return take_obs(send_obs(packed))

    def precondition(packed):
        lines, unused = exchange_obs(packed)
        column[pl.ds(0, degrees), :] = lines
        by_slot = jnp.transpose(column[...])
        start = pl.multiple_of(obs_here * SHARE, 8)
        result = jnp.zeros((8, LANES), jnp.float32)
        for slot in range(block):
            table = inv[slot, pl.ds(start, SHARE), :]
            for part in range(2):
                col = 2 * slot + part
                value = jnp.sum(table * by_slot[col : col + 1, :degrees], axis=1, keepdims=True)
                for piece in range(GROUPS):
                    result = jnp.where(lane == GROUP * piece + col, value[8 * piece : 8 * piece + 8], result)
        return jnp.where(live, result, 0.0)

    def with_energy(residual, precond):
        product = jnp.where(inside, residual * precond, 0.0)
        share = jnp.sum(jnp.sum(product, axis=1, keepdims=True), axis=0, keepdims=True)
        return jnp.where(lane == SCALAR_LANE, share, precond)

    def synthesize(coefficients, rows):
        which = tiles[0]
        tiles[0] += 1
        sems = next_round()
        send_buf, recv_buf = tile_send[which], tile_recv[which]
        for order in range(block):
            table = leg[order]
            for part in range(2):
                col = 2 * order + part
                rows[pl.ds(col, 1), :] = jnp.sum(table * coefficients[:, col : col + 1], axis=0, keepdims=True)
        turned = jnp.transpose(rows[...]).reshape(ords, CYCLES_HERE, 32)
        send_buf[:, :, pl.ds(0, 32)] = turned
        recv_buf[ord_here] = send_buf[ord_here]

        half = ord_z // 2
        sems = [sems] + [next_round() for unused in range(half)]

        def send_line(peer, sem):
            ord_copy(send_buf.at[peer], recv_buf.at[ord_here], sem, peer).start()

        for far in range(half, -1, -1):
            for step_z in ([far] if far in (0, half) else [far, ord_z - far]):
                for step_y in range(ord_y - 1, -1, -1):
                    if step_z or step_y:
                        send_line(ord_at(step_y, step_z), sems[far])

        sums = [jnp.zeros((CYCLES_HERE, SLOTS), jnp.float32) for unused in range(4)]
        for far in range(half + 1):
            steps = [far] if far in (0, half) else [far, ord_z - far]
            peers = len(steps) * ord_y - (far == 0)
            done = whole(ord_copy, recv_buf, sems[far], peers, ord_at(0, half))
            waits.append(done)
            done.wait_recv()
            for step_z in steps:
                for step_y in range(ord_y):
                    index = ord_at(step_y, step_z)
                    tile = recv_buf[index]
                    for col in range(columns):
                        sums[col % 4] = sums[col % 4] + harm[index, col] * tile[:, col : col + 1]
        return (sums[0] + sums[1]) + (sums[2] + sums[3])

    leg_copy.wait()
    done, recv_buf = per_cycle(windows_ref[pl.ds(2 * CYCLES_HERE, CYCLES_HERE), :], jnp.zeros((1, 1), jnp.float32))

    ids_done = gather_ord(ids_send, ids_recv)
    ids_done.wait_recv()
    ids_copy = pltpu.make_async_copy(ids_recv, ids_smem, local_sem.at[2])
    ids_copy.start()
    ids_copy.wait()
    first_order = ord_here * block

    def find(owner, found):
        found = list(found)
        for slot in range(block):
            number = ids_smem[owner, 0, slot]
            for order in range(block):
                found[order] = jnp.where(number == first_order + order, owner * block + slot, found[order])
        return tuple(found)

    found = lax.fori_loop(0, ords, find, tuple(jnp.int32(0) for unused in range(block)))
    for order in range(block):
        slot_smem[order] = found[order]
    inv_copy.wait()

    done.wait_recv()
    summed, unused = adjoint(recv_buf, rows_ref[0])
    residual = exchange_ord(summed, own_ref)
    residual = jnp.where(inside, residual, 0.0)
    precond = precondition(residual)
    solution = jnp.zeros((8, LANES), jnp.float32)
    direction = None
    coefficients = None
    energy_now = None
    for iteration in range(ITERS):
        chosen = exchange_ord(with_energy(residual, precond), slot_smem)
        lines, energy = exchange_obs(chosen)
        if iteration == 0:
            direction, coefficients = precond, lines
        else:
            ratio = energy / energy_now
            direction = precond + ratio * direction
            coefficients = lines + ratio * coefficients
        energy_now = energy
        gradient = synthesize(coefficients, rows_ref[1])
        weighted = windows_ref[pl.ds(CYCLES_HERE, CYCLES_HERE), :] * gradient
        curve = jnp.sum(jnp.sum(weighted * gradient, axis=1, keepdims=True), axis=0, keepdims=True)
        done, recv_buf = per_cycle(weighted, curve)
        done.wait_recv()
        summed, curvature = adjoint(recv_buf, rows_ref[0])
        step_size = energy_now / curvature
        solution = solution + step_size * direction
        if iteration + 1 == ITERS:
            sent_solution = send_obs(solution)
        image = jnp.where(inside, exchange_ord(summed, own_ref), 0.0)
        residual = residual - step_size * image
        if iteration + 1 < ITERS:
            precond = precondition(residual)

    sent = [(sent_solution, solution_ref), (send_obs(residual), residual_ref)]
    for exchange, out in sent:
        lines, unused = take_obs(exchange)
        column[pl.ds(0, degrees), :] = lines
        by_slot = jnp.transpose(column[...])
        for slot in range(block):
            out[slot] = by_slot[2 * slot : 2 * slot + 2, :degrees]
    for done in waits:
        done.wait_send()


def buffers(rounds, *shape):
    return [pltpu.VMEM(shape, jnp.float32) for unused in range(rounds)]


def body(ord_y, ord_z, obs_x, longitude, cycle_of, obs_count, observed, obs_weight, legendre, precond_inv, order_of_slot):
    block, degrees, cycles = legendre.shape[1:]
    slab = longitude.shape[1]
    ords, obss = ord_y * ord_z, obs_x * 2
    vmem = pl.BlockSpec(memory_space=pltpu.VMEM)
    smem = pl.BlockSpec(memory_space=pltpu.SMEM)
    hbm = pl.BlockSpec(memory_space=pltpu.HBM)
    window = jax.ShapeDtypeStruct((3 * CYCLES_HERE, SLOTS), jnp.float32)
    lines = (slab // LANES, LANES)
    windows = pl.pallas_call(
        functools.partial(prologue_kernel, float(slab * obss)),
        out_shape=window,
        in_specs=[smem, vmem, vmem, vmem, vmem],
        out_specs=vmem,
        name="windows",
    )(obs_count, cycle_of.reshape(lines), longitude.reshape(lines), observed.reshape(lines), obs_weight.reshape(lines))
    result = jax.ShapeDtypeStruct((block, 2, degrees), jnp.float32)
    dims = (block, degrees, cycles, ord_y, ord_z, obs_x)
    column_rows = -(-max(degrees, 1) // LANES) * LANES
    tile_rounds = 1 + 2 * ITERS
    share_rounds = 1 + 2 * ITERS
    all_rounds = 2 * ITERS + 2
    total_rounds = 1 + tile_rounds + (1 + ITERS) + share_rounds + all_rounds + ITERS * (ord_z // 2)
    scratch = [
        pltpu.VMEM((ords, 2 * block, CYCLES_HERE, SLOTS), jnp.float32),
        pltpu.VMEM((block, degrees, cycles), jnp.float32),
        pltpu.VMEM((block, SHARE * obss, degrees), jnp.float32),
        pltpu.VMEM((column_rows, LANES), jnp.float32),
        [pltpu.VMEM((32, cycles), jnp.float32), pltpu.VMEM((32, cycles), jnp.float32)],
        buffers(tile_rounds, ords, CYCLES_HERE, LANES),
        buffers(tile_rounds, ords, CYCLES_HERE, LANES),
        buffers(1 + ITERS, obss, 8, LANES),
        buffers(1 + ITERS, obss, 8, LANES),
        buffers(share_rounds, 8, LANES),
        buffers(share_rounds, ords, 8, LANES),
        buffers(all_rounds, 8, LANES),
        buffers(all_rounds, obss, 8, LANES),
        pltpu.VMEM((1, LANES), jnp.int32),
        pltpu.VMEM((ords, 1, LANES), jnp.int32),
        pltpu.SMEM((ords, 1, LANES), jnp.int32),
        pltpu.SMEM((block,), jnp.int32),
        pltpu.SemaphoreType.DMA((3,)),
        pltpu.SemaphoreType.DMA((total_rounds,)),
        pltpu.SemaphoreType.DMA((total_rounds,)),
    ]
    return pl.pallas_call(
        functools.partial(main_kernel, dims),
        out_shape=(result, result),
        in_specs=[smem, vmem, hbm, hbm],
        out_specs=(vmem, vmem),
        scratch_shapes=scratch,
        compiler_params=pltpu.CompilerParams(
            collective_id=0, has_side_effects=True
        ),
        name="solve",
    )(order_of_slot, windows, legendre[0], precond_inv)


def solution(mesh):
    placed = (
        P("obs", None),
        P("obs", None),
        P("obs"),
        P("obs", None),
        P("obs", None),
        P("obs", "ord", None, None),
        P("ord", None, None),
        P("ord"),
    )
    ords = mesh.shape["ord"]
    ord_y = 4 if ords == 32 else 2
    run = functools.partial(body, ord_y, ords // ord_y, mesh.shape["obs"] // 2)
    return jax.shard_map(
        run,
        mesh=mesh,
        in_specs=placed,
        out_specs=(P("ord", None, None), P("ord", None, None)),
        check_vma=False,
    )
```

```python
import functools

import jax
import jax.numpy as jnp
from jax import lax
from jax.experimental import pallas as pl
from jax.experimental.pallas import tpu as pltpu
from jax.sharding import PartitionSpec as P

ITERS = 2
MESH = pl.DeviceIdType.MESH
LANES = 128
SLOTS = 256
CYCLES_HERE = 8
GROUP = 20
GROUPS = 5
SHARE = 8 * GROUPS
SCALAR_LANE = 127
CURVE_COLUMN = 18
TWO_OVER_PI = 0.6366197723675814
PI_2_A = 1.5703125
PI_2_B = 0.00048351287841796875
PI_2_C = 3.13855707645416259765625e-07
PI_2_D = 6.077100628276710e-11


def sine_cosine(angle):
    turns = jnp.floor(angle * TWO_OVER_PI + 0.5)
    rest = angle - turns * PI_2_A
    rest = rest - turns * PI_2_B
    rest = rest - turns * PI_2_C
    rest = rest - turns * PI_2_D
    square = rest * rest
    sine = rest + rest * square * (-1.6666654611e-1 + square * (8.3321608736e-3 + square * -1.9515295891e-4))
    cosine = 1.0 - 0.5 * square + square * square * (
        4.166664568298827e-2 + square * (-1.388731625493765e-3 + square * 2.443315711809948e-5)
    )
    quadrant = turns.astype(jnp.int32)
    swap = (quadrant & 1) == 1
    sine_out = jnp.where(swap, cosine, sine)
    cosine_out = jnp.where(swap, sine, cosine)
    sine_out = jnp.where((quadrant & 2) == 2, -sine_out, sine_out)
    cosine_out = jnp.where(((quadrant + 1) & 2) == 2, -cosine_out, cosine_out)
    return sine_out, cosine_out


def prologue_kernel(total_obs, count_ref, cycle_ref, lon_ref, obs_ref, weight_ref, out_ref):
    first_cycle = lax.axis_index("ord") * CYCLES_HERE
    rows = cycle_ref.shape[0]
    ids = cycle_ref[...]
    starts = []
    for step in range(CYCLES_HERE + 1):
        below = jnp.where(ids < first_cycle + step, 1.0, 0.0)
        starts.append(jnp.sum(below).astype(jnp.int32))
    lane = lax.broadcasted_iota(jnp.int32, (1, LANES), 1)
    used = count_ref[0]
    for step in range(CYCLES_HERE):
        start = starts[step]
        count = starts[step + 1] - start
        row = start // LANES
        shift = start - row * LANES
        turn = lax.rem(LANES - shift, LANES)
        lines = [jnp.minimum(row + part, rows - 1) for part in range(3)]
        head = lane < LANES - shift
        windows = []
        for ref in (lon_ref, obs_ref, weight_ref):
            turned = [pltpu.roll(ref[pl.ds(line, 1), :], turn, 1) for line in lines]
            windows.append([jnp.where(head, turned[part], turned[part + 1]) for part in range(2)])
        for part in range(2):
            slot = lane + part * LANES
            valid = jnp.logical_and(slot < count, start + slot < used)
            scale = jnp.where(valid, windows[2][part] / total_obs, 0.0)
            cut = pl.ds(part * LANES, LANES)
            for which, value in enumerate((windows[0][part], scale, scale * windows[1][part])):
                out_ref[pl.ds(which * CYCLES_HERE + step, 1), cut] = value


def offset(index):
    return ((index + 1) // 2) * (1 - 2 * (index % 2))


def main_kernel(
    dims, own_ref, windows_ref, leg_hbm, inv_hbm, solution_ref, residual_ref,
    harm, leg, inv, column, rows_ref, tile_send, tile_recv, part_send, part_recv, share_send, share_recv,
    all_send, all_recv, ids_send, ids_recv, ids_smem, slot_vmem, slot_all, slot_smem, spread_send, spread_recv,
    inv_send, inv_recv, inv_block, local_sem, send_sem, recv_sem,
):
    block, degrees, cycles, ord_y, ord_z, obs_x = dims
    ords = ord_y * ord_z
    obss = obs_x * 2
    columns = 2 * block
    unroll = 2 * ord_y
    ord_here = lax.axis_index("ord")
    obs_here = lax.axis_index("obs")

    for slot in range(block):
        inv[slot, pl.ds(degrees, SHARE * obss - degrees), :] = jnp.zeros((SHARE * obss - degrees, degrees), jnp.float32)
    leg_copy = pltpu.make_async_copy(leg_hbm, leg, local_sem.at[0])
    inv_copy = pltpu.make_async_copy(inv_hbm, inv.at[:, pl.ds(0, degrees), :], local_sem.at[1])
    leg_copy.start()
    inv_copy.start()

    here_y, here_z = lax.div(ord_here, ord_z), lax.rem(ord_here, ord_z)
    here_x, here_core = lax.div(obs_here, 2), lax.rem(obs_here, 2)

    def ord_at(step_y, step_z):
        return lax.rem(here_y + step_y, ord_y) * ord_z + lax.rem(here_z + step_z, ord_z)

    def ord_peer(index):
        return ord_at(ord_y // 2 + offset(index % ord_y), ord_z // 2 + offset(index // ord_y))

    def obs_peer(index):
        step_x = obs_x // 2 + offset(index // 2)
        step_core = 1 - index % 2
        return lax.rem(here_x + step_x, obs_x) * 2 + lax.rem(here_core + step_core, 2)

    barrier = pltpu.get_barrier_semaphore()

    for index in range(ords - 1):
        pl.semaphore_signal(barrier, inc=1, device_id={"ord": ord_peer(index)}, device_id_type=MESH)
    for index in range(obss - 1):
        pl.semaphore_signal(barrier, inc=1, device_id={"obs": obs_peer(index)}, device_id_type=MESH)

    lane = lax.broadcasted_iota(jnp.int32, (8, LANES), 1)
    sublane = lax.broadcasted_iota(jnp.int32, (8, LANES), 0)
    group = lane // GROUP
    inner = lane % GROUP
    slot_lane = inner // 2
    degree_here = obs_here * SHARE + group * 8 + sublane
    inside = jnp.logical_and(jnp.logical_and(group < GROUPS, inner < columns), degree_here < degrees)
    order_lane = jnp.zeros((8, LANES), jnp.int32)
    for slot in range(block):
        order_lane = jnp.where(slot_lane == slot, own_ref[slot], order_lane)
    live = jnp.logical_and(inside, degree_here >= order_lane)
    live_block = jnp.logical_and(inside, degree_here >= ord_here * block + slot_lane)

    ids_row = jnp.zeros((1, LANES), jnp.int32)
    lane_row = lax.broadcasted_iota(jnp.int32, (1, LANES), 1)
    for slot in range(block):
        ids_row = jnp.where(lane_row == slot, own_ref[slot], ids_row)
    ids_send[...] = ids_row
    ids_recv[ord_here] = ids_row
    for which in range(len(rows_ref)):
        rows_ref[which][...] = jnp.zeros((32, cycles), jnp.float32)
    column[...] = jnp.zeros(column.shape, jnp.float32)

    longitude = windows_ref[pl.ds(0, CYCLES_HERE), :]

    def harmonic_block(index, carry):
        for order in range(block):
            number = (index * block + order).astype(jnp.float32)
            sine, cosine = sine_cosine(number * longitude)
            harm[index, 2 * order] = cosine
            harm[index, 2 * order + 1] = sine
        return carry

    lax.fori_loop(0, ords, harmonic_block, 0)
    pl.semaphore_wait(barrier, ords - 1 + obss - 1)

    rounds = [0]
    waits = []

    def next_round():
        rounds[0] += 1
        return rounds[0] - 1

    def ord_copy(source, target, sems, peer):
        return pltpu.make_async_remote_copy(
            src_ref=source, dst_ref=target, send_sem=send_sem.at[sems], recv_sem=recv_sem.at[sems],
            device_id={"ord": peer}, device_id_type=MESH,
        )

    def obs_copy(source, target, sems, peer):
        return pltpu.make_async_remote_copy(
            src_ref=source, dst_ref=target, send_sem=send_sem.at[sems], recv_sem=recv_sem.at[sems],
            device_id={"obs": peer}, device_id_type=MESH,
        )

    def whole(make, buffer, sems, peers, peer):
        cut = buffer.at[pl.ds(0, peers)]
        return make(cut, cut, sems, peer)

    def gather_ord(source, buffer):
        sems = next_round()

        def send(index, carry):
            ord_copy(source, buffer.at[ord_here], sems, ord_peer(index)).start()
            return carry

        lax.fori_loop(0, ords - 1, send, 0)
        done = whole(ord_copy, buffer, sems, ords - 1, ord_peer(0))
        waits.append(done)
        return done

    def gather_obs(source, buffer):
        sems = next_round()

        def send(index, carry):
            obs_copy(source, buffer.at[obs_here], sems, obs_peer(index)).start()
            return carry

        lax.fori_loop(0, obss - 1, send, 0)
        done = whole(obs_copy, buffer, sems, obss - 1, obs_peer(0))
        waits.append(done)
        return done

    tiles = [0]
    parts = [0]
    shares = [0]
    alls = [0]

    def per_cycle(weighted, curve):
        which = tiles[0]
        tiles[0] += 1
        sems = next_round()
        send_buf, recv_buf = tile_send[which], tile_recv[which]
        corner = jnp.logical_and(lane == CURVE_COLUMN, sublane == 0)
        empty = jnp.where(corner, curve, 0.0)

        def step(outer, carry):
            for inner_step in range(unroll):
                index = outer * unroll + inner_step
                peer = ord_at(
                    ord_y // 2 + offset(inner_step % ord_y), ord_z // 2 + offset(outer * (unroll // ord_y) + inner_step // ord_y)
                )
                tile = empty
                for col in range(columns):
                    total = jnp.sum(harm[peer, col] * weighted, axis=1, keepdims=True)
                    tile = jnp.where(lane == col, total, tile)
                send_buf[peer] = tile
                if inner_step < unroll - 1:
                    ord_copy(send_buf.at[peer], recv_buf.at[ord_here], sems, peer).start()
                else:
                    @pl.when(index < ords - 1)
                    def _():
                        ord_copy(send_buf.at[peer], recv_buf.at[ord_here], sems, peer).start()

                    @pl.when(index == ords - 1)
                    def _():
                        recv_buf[ord_here] = tile
            return carry

        lax.fori_loop(0, ords // unroll, step, 0)
        done = whole(ord_copy, recv_buf, sems, ords - 1, ord_peer(0))
        waits.append(done)
        return done, recv_buf

    def adjoint(recv_buf, rows):
        per_order = jnp.transpose(recv_buf[...].reshape(cycles, LANES)[:, :32])
        rows[...] = per_order
        curve = jnp.sum(rows[pl.ds(CURVE_COLUMN, 1), :], axis=1, keepdims=True)
        lane_all = lax.broadcasted_iota(jnp.int32, (degrees, LANES), 1)
        total = jnp.zeros((degrees, LANES), jnp.float32)
        for order in range(block):
            table = leg[order]
            for part in range(2):
                col = 2 * order + part
                value = jnp.sum(table * rows[pl.ds(col, 1), :], axis=1, keepdims=True)
                total = jnp.where(lane_all == col, value, total)
        column[pl.ds(0, degrees), :] = total
        which = parts[0]
        parts[0] += 1
        send_buf, recv_obs = part_send[which], part_recv[which]
        for owner in range(obss):
            packed = jnp.where(lane == SCALAR_LANE, curve, 0.0)
            for piece in range(GROUPS):
                start = owner * SHARE + piece * 8
                if start < degrees:
                    lines = column[pl.ds(start, 8), :]
                    packed = packed + (pltpu.roll(lines, GROUP * piece, 1) if piece else lines)
            send_buf[owner] = packed
        sems = next_round()

        def send(index, carry):
            peer = obs_peer(index)
            obs_copy(send_buf.at[peer], recv_obs.at[obs_here], sems, peer).start()
            return carry

        lax.fori_loop(0, obss - 1, send, 0)
        recv_obs[obs_here] = send_buf[obs_here]
        done = whole(obs_copy, recv_obs, sems, obss - 1, obs_peer(0))
        waits.append(done)
        done.wait_recv()
        summed = jnp.sum(recv_obs[...], axis=0)
        return summed, summed[0:1, SCALAR_LANE : SCALAR_LANE + 1]

    def send_ord(packed):
        which = shares[0]
        shares[0] += 1
        send_buf, recv_buf = share_send[which], share_recv[which]
        send_buf[...] = packed
        recv_buf[ord_here] = packed
        return gather_ord(send_buf, recv_buf), recv_buf

    def take_ord(sent, index_ref):
        done, recv_buf = sent
        done.wait_recv()
        everyone = jnp.sum(recv_buf[...], axis=0)
        chosen = jnp.where(lane == SCALAR_LANE, everyone, 0.0)
        for slot in range(block):
            number = index_ref[slot]
            source = lax.div(number, block)
            place = number - source * block
            turn = lax.rem(2 * slot - 2 * place + LANES, LANES)
            lines = pltpu.roll(recv_buf[source], turn, 1)
            chosen = jnp.where(jnp.logical_and(inside, slot_lane == slot), lines, chosen)
        return chosen

    def send_obs(packed):
        which = alls[0]
        alls[0] += 1
        send_buf, recv_buf = all_send[which], all_recv[which]
        send_buf[...] = packed
        recv_buf[obs_here] = packed
        return gather_obs(send_buf, recv_buf), recv_buf

    def take_obs(sent):
        done, recv_buf = sent
        done.wait_recv()
        total = jnp.sum(recv_buf[...], axis=0)[0:1, SCALAR_LANE : SCALAR_LANE + 1]
        pieces = []
        for owner in range(obss):
            for piece in range(GROUPS):
                if owner * SHARE + piece * 8 < degrees:
                    lines = recv_buf[owner]
                    pieces.append(pltpu.roll(lines, LANES - GROUP * piece, 1) if piece else lines)
        return jnp.concatenate(pieces, axis=0), total

    def exchange_obs(packed):
        return take_obs(send_obs(packed))

    def precondition(packed, table_of, alive):
        lines, unused = exchange_obs(packed)
        column[pl.ds(0, degrees), :] = lines
        by_slot = jnp.transpose(column[...])
        result = jnp.zeros((8, LANES), jnp.float32)
        for slot in range(block):
            table = table_of(slot)
            for part in range(2):
                col = 2 * slot + part
                value = jnp.sum(table * by_slot[col : col + 1, : table.shape[1]], axis=1, keepdims=True)
                for piece in range(GROUPS):
                    result = jnp.where(lane == GROUP * piece + col, value[8 * piece : 8 * piece + 8], result)
        return jnp.where(alive, result, 0.0)

    share_start = pl.multiple_of(obs_here * SHARE, 8)

    def owner_table(slot):
        return inv[slot, pl.ds(share_start, SHARE), :]

    tiles_wide = inv_block.shape[2] // LANES
    spread_sems, inv_sems = next_round(), next_round()

    def build_spread():
        for slot in range(block):
            for wide in range(tiles_wide):
                width = min(LANES, degrees - wide * LANES)
                for piece in range(GROUPS):
                    lines = inv[slot, pl.ds(share_start + 8 * piece, 8), pl.ds(wide * LANES, width)]
                    if width < LANES:
                        lines = jnp.concatenate([lines, jnp.zeros((8, LANES - width), jnp.float32)], axis=1)
                    for half in range(2):
                        place = (wide * GROUPS + piece) * 2 + half
                        spread_send[place % ords, slot, place // ords] = lines[4 * half : 4 * half + 4]
        spread_recv[pl.ds(ord_here * block, block)] = spread_send[ord_here]

    def send_spread(first, last):
        def send(index, carry):
            peer = ord_peer(index)
            ord_copy(spread_send.at[peer], spread_recv.at[pl.ds(ord_here * block, block)], spread_sems, peer).start()
            return carry

        lax.fori_loop(first, last, send, 0)

    def build_inv():
        cut = spread_recv.at[pl.ds(0, (ords - 1) * block)]
        done = ord_copy(cut, cut, spread_sems, ord_peer(0))
        waits.append(done)
        done.wait_recv()

        def step(index, carry):
            for order in range(block):
                number = index * block + order
                inv_send[index, order] = spread_recv[slot_all[lax.div(number, LANES), lax.rem(number, LANES)]]
            return carry

        lax.fori_loop(0, ords, step, 0)
        inv_recv[ord_here] = inv_send[ord_here]

    def send_inv(first, last):
        def send(index, carry):
            peer = ord_peer(index)
            ord_copy(inv_send.at[peer], inv_recv.at[ord_here], inv_sems, peer).start()
            return carry

        lax.fori_loop(first, last, send, 0)

    def take_inv():
        done = whole(ord_copy, inv_recv, inv_sems, ords - 1, ord_peer(0))
        waits.append(done)
        done.wait_recv()
        for order in range(block):
            for wide in range(tiles_wide):
                for piece in range(GROUPS):
                    for half in range(2):
                        place = (wide * GROUPS + piece) * 2 + half
                        inv_block[order, pl.ds(8 * piece + 4 * half, 4), pl.ds(wide * LANES, LANES)] = inv_recv[
                            place % ords, order, place // ords
                        ]

    def find_slots():
        ids_done.wait_recv()
        ids_copy = pltpu.make_async_copy(ids_recv, ids_smem, local_sem.at[2])
        ids_copy.start()
        ids_copy.wait()
        position = sublane * LANES + lane

        def find(owner, found):
            for slot in range(block):
                found = jnp.where(position == ids_smem[owner, 0, slot], owner * block + slot, found)
            return found

        slot_vmem[...] = lax.fori_loop(0, ords, find, jnp.zeros((8, LANES), jnp.int32))
        slot_copy = pltpu.make_async_copy(slot_vmem, slot_all, local_sem.at[3])
        slot_copy.start()
        slot_copy.wait()
        for order in range(block):
            number = ord_here * block + order
            slot_smem[order] = slot_all[lax.div(number, LANES), lax.rem(number, LANES)]

    def with_energy(residual, precond):
        product = jnp.where(inside, residual * precond, 0.0)
        share = jnp.sum(jnp.sum(product, axis=1, keepdims=True), axis=0, keepdims=True)
        return jnp.where(lane == SCALAR_LANE, share, precond)

    def synthesize(coefficients, energy, rows, meanwhile):
        which = tiles[0]
        tiles[0] += 1
        sems = next_round()
        send_buf, recv_buf = tile_send[which], tile_recv[which]
        for order in range(block):
            table = leg[order]
            for part in range(2):
                col = 2 * order + part
                rows[pl.ds(col, 1), :] = jnp.sum(table * coefficients[:, col : col + 1], axis=0, keepdims=True)
        rows[pl.ds(CURVE_COLUMN, 1), :] = jnp.broadcast_to(energy, (1, cycles))
        turned = jnp.transpose(rows[...]).reshape(ords, CYCLES_HERE, 32)
        send_buf[:, :, pl.ds(0, 32)] = turned
        recv_buf[ord_here] = send_buf[ord_here]

        half = ord_z // 2
        sems = [sems] + [next_round() for unused in range(half)]

        def send_line(peer, sem):
            ord_copy(send_buf.at[peer], recv_buf.at[ord_here], sem, peer).start()

        for far in range(half, -1, -1):
            for step_z in ([far] if far in (0, half) else [far, ord_z - far]):
                for step_y in range(ord_y - 1, -1, -1):
                    if step_z or step_y:
                        send_line(ord_at(step_y, step_z), sems[far])

        meanwhile()
        sums = [jnp.zeros((CYCLES_HERE, SLOTS), jnp.float32) for unused in range(4)]
        energies = jnp.zeros((8, LANES), jnp.float32)
        for far in range(half + 1):
            steps = [far] if far in (0, half) else [far, ord_z - far]
            peers = len(steps) * ord_y - (far == 0)
            done = whole(ord_copy, recv_buf, sems[far], peers, ord_at(0, half))
            waits.append(done)
            done.wait_recv()
            for step_z in steps:
                for step_y in range(ord_y):
                    index = ord_at(step_y, step_z)
                    tile = recv_buf[index]
                    energies = energies + tile
                    for col in range(columns):
                        sums[col % 4] = sums[col % 4] + harm[index, col] * tile[:, col : col + 1]
        return (sums[0] + sums[1]) + (sums[2] + sums[3]), energies[0:1, CURVE_COLUMN : CURVE_COLUMN + 1]

    leg_copy.wait()
    done, recv_buf = per_cycle(windows_ref[pl.ds(2 * CYCLES_HERE, CYCLES_HERE), :], jnp.zeros((1, 1), jnp.float32))

    ids_done = gather_ord(ids_send, ids_recv)
    inv_copy.wait()
    build_spread()
    third = (ords - 1) // 3
    send_spread(0, third)
    done.wait_recv()
    summed, unused = adjoint(recv_buf, rows_ref[0])
    residual = jnp.where(inside, summed, 0.0)
    sent = send_ord(residual)
    send_spread(third, 2 * third)
    find_slots()
    owned = jnp.where(inside, take_ord(sent, own_ref), 0.0)
    precond = precondition(owned, owner_table, live)
    sent = send_ord(with_energy(owned, precond))
    send_spread(2 * third, ords - 1)
    chosen = take_ord(sent, slot_smem)
    lines, energy_now = exchange_obs(chosen)
    direction = jnp.where(inside, chosen, 0.0)
    solution = jnp.zeros((8, LANES), jnp.float32)
    gradient = None
    nothing = jnp.zeros((1, 1), jnp.float32)
    for iteration in range(ITERS):
        if iteration == 0:

            def prepare():
                build_inv()
                send_inv(0, third)

            gradient, unused = synthesize(lines, nothing, rows_ref[1], prepare)
        else:
            precond = precondition(residual, lambda slot: inv_block[slot], live_block)
            lines, energy_block = exchange_obs(with_energy(residual, precond))
            ahead, energy = synthesize(lines, energy_block, rows_ref[1], lambda: None)
            ratio = energy / energy_now
            gradient = ahead + ratio * gradient
            direction = precond + ratio * direction
            energy_now = energy
        weighted = windows_ref[pl.ds(CYCLES_HERE, CYCLES_HERE), :] * gradient
        curve = jnp.sum(jnp.sum(weighted * gradient, axis=1, keepdims=True), axis=0, keepdims=True)
        done, recv_buf = per_cycle(weighted, curve)
        if iteration == 0:
            send_inv(third, ords - 1)
        done.wait_recv()
        summed, curvature = adjoint(recv_buf, rows_ref[0])
        step_size = energy_now / curvature
        solution = solution + step_size * direction
        residual = residual - step_size * jnp.where(inside, summed, 0.0)
        if iteration == 0:
            take_inv()

    sent_solution, sent_residual = send_ord(solution), send_ord(residual)
    sent_solution = send_obs(take_ord(sent_solution, own_ref))
    sent_residual = send_obs(take_ord(sent_residual, own_ref))
    sent = [(sent_solution, solution_ref), (sent_residual, residual_ref)]
    for exchange, out in sent:
        lines, unused = take_obs(exchange)
        column[pl.ds(0, degrees), :] = lines
        by_slot = jnp.transpose(column[...])
        for slot in range(block):
            out[slot] = by_slot[2 * slot : 2 * slot + 2, :degrees]
    for done in waits:
        done.wait_send()


def buffers(rounds, *shape):
    return [pltpu.VMEM(shape, jnp.float32) for unused in range(rounds)]


def body(ord_y, ord_z, obs_x, longitude, cycle_of, obs_count, observed, obs_weight, legendre, precond_inv, order_of_slot):
    block, degrees, cycles = legendre.shape[1:]
    slab = longitude.shape[1]
    ords, obss = ord_y * ord_z, obs_x * 2
    vmem = pl.BlockSpec(memory_space=pltpu.VMEM)
    smem = pl.BlockSpec(memory_space=pltpu.SMEM)
    hbm = pl.BlockSpec(memory_space=pltpu.HBM)
    window = jax.ShapeDtypeStruct((3 * CYCLES_HERE, SLOTS), jnp.float32)
    lines = (slab // LANES, LANES)
    windows = pl.pallas_call(
        functools.partial(prologue_kernel, float(slab * obss)),
        out_shape=window,
        in_specs=[smem, vmem, vmem, vmem, vmem],
        out_specs=vmem,
        name="windows",
    )(obs_count, cycle_of.reshape(lines), longitude.reshape(lines), observed.reshape(lines), obs_weight.reshape(lines))
    result = jax.ShapeDtypeStruct((block, 2, degrees), jnp.float32)
    dims = (block, degrees, cycles, ord_y, ord_z, obs_x)
    column_rows = -(-max(degrees, 1) // LANES) * LANES
    tile_rounds = 1 + 2 * ITERS
    share_rounds = 4
    all_rounds = 2 * ITERS + 2
    deep = -(-(column_rows // LANES * GROUPS * 2) // ords)
    total_rounds = 1 + tile_rounds + (1 + ITERS) + share_rounds + all_rounds + ITERS * (ord_z // 2) + 2
    scratch = [
        pltpu.VMEM((ords, 2 * block, CYCLES_HERE, SLOTS), jnp.float32),
        pltpu.VMEM((block, degrees, cycles), jnp.float32),
        pltpu.VMEM((block, SHARE * obss, degrees), jnp.float32),
        pltpu.VMEM((column_rows, LANES), jnp.float32),
        [pltpu.VMEM((32, cycles), jnp.float32), pltpu.VMEM((32, cycles), jnp.float32)],
        buffers(tile_rounds, ords, CYCLES_HERE, LANES),
        buffers(tile_rounds, ords, CYCLES_HERE, LANES),
        buffers(1 + ITERS, obss, 8, LANES),
        buffers(1 + ITERS, obss, 8, LANES),
        buffers(share_rounds, 8, LANES),
        buffers(share_rounds, ords, 8, LANES),
        buffers(all_rounds, 8, LANES),
        buffers(all_rounds, obss, 8, LANES),
        pltpu.VMEM((1, LANES), jnp.int32),
        pltpu.VMEM((ords, 1, LANES), jnp.int32),
        pltpu.SMEM((ords, 1, LANES), jnp.int32),
        pltpu.VMEM((8, LANES), jnp.int32),
        pltpu.SMEM((8, LANES), jnp.int32),
        pltpu.SMEM((block,), jnp.int32),
        pltpu.VMEM((ords, block, deep, 4, LANES), jnp.float32),
        pltpu.VMEM((ords * block, deep, 4, LANES), jnp.float32),
        pltpu.VMEM((ords, block, deep, 4, LANES), jnp.float32),
        pltpu.VMEM((ords, block, deep, 4, LANES), jnp.float32),
        pltpu.VMEM((block, SHARE, column_rows), jnp.float32),
        pltpu.SemaphoreType.DMA((4,)),
        pltpu.SemaphoreType.DMA((total_rounds,)),
        pltpu.SemaphoreType.DMA((total_rounds,)),
    ]
    return pl.pallas_call(
        functools.partial(main_kernel, dims),
        out_shape=(result, result),
        in_specs=[smem, vmem, hbm, hbm],
        out_specs=(vmem, vmem),
        scratch_shapes=scratch,
        compiler_params=pltpu.CompilerParams(
            collective_id=0, has_side_effects=True
        ),
        name="solve",
    )(order_of_slot, windows, legendre[0], precond_inv)


def solution(mesh):
    placed = (
        P("obs", None),
        P("obs", None),
        P("obs"),
        P("obs", None),
        P("obs", None),
        P("obs", "ord", None, None),
        P("ord", None, None),
        P("ord"),
    )
    ords = mesh.shape["ord"]
    ord_y = 4 if ords == 32 else 2
    run = functools.partial(body, ord_y, ords // ord_y, mesh.shape["obs"] // 2)
    return jax.shard_map(
        run,
        mesh=mesh,
        in_specs=placed,
        out_specs=(P("ord", None, None), P("ord", None, None)),
        check_vma=False,
    )
```

```python
import functools

import jax
import jax.numpy as jnp
from jax import lax
from jax.experimental import pallas as pl
from jax.experimental.pallas import tpu as pltpu
from jax.sharding import PartitionSpec as P

ITERS = 2
MESH = pl.DeviceIdType.MESH
LANES = 128
SLOTS = 256
CYCLES_HERE = 8
GROUP = 20
GROUPS = 5
SHARE = 8 * GROUPS
SCALAR_LANE = 127
CURVE_COLUMN = 18
TWO_OVER_PI = 0.6366197723675814
PI_2_A = 1.5703125
PI_2_B = 0.00048351287841796875
PI_2_C = 3.13855707645416259765625e-07
PI_2_D = 6.077100628276710e-11


def sine_cosine(angle):
    turns = jnp.floor(angle * TWO_OVER_PI + 0.5)
    rest = angle - turns * PI_2_A
    rest = rest - turns * PI_2_B
    rest = rest - turns * PI_2_C
    rest = rest - turns * PI_2_D
    square = rest * rest
    sine = rest + rest * square * (-1.6666654611e-1 + square * (8.3321608736e-3 + square * -1.9515295891e-4))
    cosine = 1.0 - 0.5 * square + square * square * (
        4.166664568298827e-2 + square * (-1.388731625493765e-3 + square * 2.443315711809948e-5)
    )
    quadrant = turns.astype(jnp.int32)
    swap = (quadrant & 1) == 1
    sine_out = jnp.where(swap, cosine, sine)
    cosine_out = jnp.where(swap, sine, cosine)
    sine_out = jnp.where((quadrant & 2) == 2, -sine_out, sine_out)
    cosine_out = jnp.where(((quadrant + 1) & 2) == 2, -cosine_out, cosine_out)
    return sine_out, cosine_out


def prologue_kernel(total_obs, count_ref, cycle_ref, lon_ref, obs_ref, weight_ref, out_ref):
    first_cycle = lax.axis_index("ord") * CYCLES_HERE
    rows = cycle_ref.shape[0]
    ids = cycle_ref[...]
    starts = []
    for step in range(CYCLES_HERE + 1):
        below = jnp.where(ids < first_cycle + step, 1.0, 0.0)
        starts.append(jnp.sum(below).astype(jnp.int32))
    lane = lax.broadcasted_iota(jnp.int32, (1, LANES), 1)
    used = count_ref[0]
    for step in range(CYCLES_HERE):
        start = starts[step]
        count = starts[step + 1] - start
        row = start // LANES
        shift = start - row * LANES
        turn = lax.rem(LANES - shift, LANES)
        lines = [jnp.minimum(row + part, rows - 1) for part in range(3)]
        head = lane < LANES - shift
        windows = []
        for ref in (lon_ref, obs_ref, weight_ref):
            turned = [pltpu.roll(ref[pl.ds(line, 1), :], turn, 1) for line in lines]
            windows.append([jnp.where(head, turned[part], turned[part + 1]) for part in range(2)])
        for part in range(2):
            slot = lane + part * LANES
            valid = jnp.logical_and(slot < count, start + slot < used)
            scale = jnp.where(valid, windows[2][part] / total_obs, 0.0)
            cut = pl.ds(part * LANES, LANES)
            for which, value in enumerate((windows[0][part], scale, scale * windows[1][part])):
                out_ref[pl.ds(which * CYCLES_HERE + step, 1), cut] = value


def unpacked(shares, degrees):
    pieces = []
    for owner in range(shares.shape[0]):
        for piece in range(GROUPS):
            if owner * SHARE + piece * 8 < degrees:
                lines = shares[owner]
                pieces.append(pltpu.roll(lines, LANES - GROUP * piece, 1) if piece else lines)
    return jnp.concatenate(pieces, axis=0)


def finish_kernel(packed_ref, solution_ref, residual_ref, column):
    block, unused, degrees = solution_ref.shape
    column[...] = jnp.zeros(column.shape, jnp.float32)
    for which, out in enumerate((solution_ref, residual_ref)):
        column[pl.ds(0, degrees), :] = unpacked(packed_ref.at[which], degrees)
        by_slot = jnp.transpose(column[...])
        for slot in range(block):
            out[slot] = by_slot[2 * slot : 2 * slot + 2, :degrees]


def offset(index):
    return ((index + 1) // 2) * (1 - 2 * (index % 2))


def main_kernel(
    dims, own_ref, windows_ref, leg_hbm, inv_hbm, packed_ref,
    harm, leg, inv, column, rows_ref, tile_send, tile_recv, part_send, part_recv, share_send, share_recv,
    all_send, all_recv, ids_send, ids_recv, ids_smem, slot_vmem, slot_all, slot_smem, spread_send, spread_recv,
    inv_send, inv_recv, inv_block, local_sem, send_sem, recv_sem,
):
    block, degrees, cycles, ord_y, ord_z, obs_x = dims
    ords = ord_y * ord_z
    obss = obs_x * 2
    columns = 2 * block
    unroll = 2 * ord_y
    ord_here = lax.axis_index("ord")
    obs_here = lax.axis_index("obs")

    for slot in range(block):
        inv[slot, pl.ds(degrees, SHARE * obss - degrees), :] = jnp.zeros((SHARE * obss - degrees, degrees), jnp.float32)
    leg_copy = pltpu.make_async_copy(leg_hbm, leg, local_sem.at[0])
    inv_copy = pltpu.make_async_copy(inv_hbm, inv.at[:, pl.ds(0, degrees), :], local_sem.at[1])
    leg_copy.start()
    inv_copy.start()

    here_y, here_z = lax.div(ord_here, ord_z), lax.rem(ord_here, ord_z)
    here_x, here_core = lax.div(obs_here, 2), lax.rem(obs_here, 2)

    def ord_at(step_y, step_z):
        return lax.rem(here_y + step_y, ord_y) * ord_z + lax.rem(here_z + step_z, ord_z)

    def ord_peer(index):
        return ord_at(ord_y // 2 + offset(index % ord_y), ord_z // 2 + offset(index // ord_y))

    def bulk_peer(index):
        return ord_at(ord_y // 2 + offset(index // ord_z), ord_z // 2 + offset(index % ord_z))

    def obs_peer(index):
        step_x = obs_x // 2 + offset(index // 2)
        step_core = 1 - index % 2
        return lax.rem(here_x + step_x, obs_x) * 2 + lax.rem(here_core + step_core, 2)

    barrier = pltpu.get_barrier_semaphore()

    for index in range(ords - 1):
        pl.semaphore_signal(barrier, inc=1, device_id={"ord": ord_peer(index)}, device_id_type=MESH)
    for index in range(obss - 1):
        pl.semaphore_signal(barrier, inc=1, device_id={"obs": obs_peer(index)}, device_id_type=MESH)

    lane = lax.broadcasted_iota(jnp.int32, (8, LANES), 1)
    sublane = lax.broadcasted_iota(jnp.int32, (8, LANES), 0)
    group = lane // GROUP
    inner = lane % GROUP
    slot_lane = inner // 2
    degree_here = obs_here * SHARE + group * 8 + sublane
    inside = jnp.logical_and(jnp.logical_and(group < GROUPS, inner < columns), degree_here < degrees)
    order_lane = jnp.zeros((8, LANES), jnp.int32)
    for slot in range(block):
        order_lane = jnp.where(slot_lane == slot, own_ref[slot], order_lane)
    live = jnp.logical_and(inside, degree_here >= order_lane)
    live_block = jnp.logical_and(inside, degree_here >= ord_here * block + slot_lane)

    ids_row = jnp.zeros((1, LANES), jnp.int32)
    lane_row = lax.broadcasted_iota(jnp.int32, (1, LANES), 1)
    for slot in range(block):
        ids_row = jnp.where(lane_row == slot, own_ref[slot], ids_row)
    ids_send[...] = ids_row
    ids_recv[ord_here] = ids_row
    for which in range(len(rows_ref)):
        rows_ref[which][...] = jnp.zeros((32, cycles), jnp.float32)
    column[...] = jnp.zeros(column.shape, jnp.float32)

    longitude = windows_ref[pl.ds(0, CYCLES_HERE), :]

    def harmonic_block(index, carry):
        for order in range(block):
            number = (index * block + order).astype(jnp.float32)
            sine, cosine = sine_cosine(number * longitude)
            harm[index, 2 * order] = cosine
            harm[index, 2 * order + 1] = sine
        return carry

    lax.fori_loop(0, ords, harmonic_block, 0)
    pl.semaphore_wait(barrier, ords - 1 + obss - 1)

    rounds = [0]
    waits = []

    def next_round():
        rounds[0] += 1
        return rounds[0] - 1

    def ord_copy(source, target, sems, peer):
        return pltpu.make_async_remote_copy(
            src_ref=source, dst_ref=target, send_sem=send_sem.at[sems], recv_sem=recv_sem.at[sems],
            device_id={"ord": peer}, device_id_type=MESH,
        )

    def obs_copy(source, target, sems, peer):
        return pltpu.make_async_remote_copy(
            src_ref=source, dst_ref=target, send_sem=send_sem.at[sems], recv_sem=recv_sem.at[sems],
            device_id={"obs": peer}, device_id_type=MESH,
        )

    def whole(make, buffer, sems, peers, peer):
        cut = buffer.at[pl.ds(0, peers)]
        return make(cut, cut, sems, peer)

    def gather_ord(source, buffer):
        sems = next_round()

        def send(index, carry):
            ord_copy(source, buffer.at[ord_here], sems, ord_peer(index)).start()
            return carry

        lax.fori_loop(0, ords - 1, send, 0)
        done = whole(ord_copy, buffer, sems, ords - 1, ord_peer(0))
        waits.append(done)
        return done

    def gather_obs(source, buffer):
        sems = next_round()

        def send(index, carry):
            obs_copy(source, buffer.at[obs_here], sems, obs_peer(index)).start()
            return carry

        lax.fori_loop(0, obss - 1, send, 0)
        done = whole(obs_copy, buffer, sems, obss - 1, obs_peer(0))
        waits.append(done)
        return done

    tiles = [0]
    parts = [0]
    shares = [0]
    alls = [0]

    def per_cycle(weighted, curve):
        which = tiles[0]
        tiles[0] += 1
        sems = next_round()
        send_buf, recv_buf = tile_send[which], tile_recv[which]
        corner = jnp.logical_and(lane == CURVE_COLUMN, sublane == 0)
        empty = jnp.where(corner, curve, 0.0)

        def step(outer, carry):
            for inner_step in range(unroll):
                index = outer * unroll + inner_step
                peer = ord_at(
                    ord_y // 2 + offset(inner_step % ord_y), ord_z // 2 + offset(outer * (unroll // ord_y) + inner_step // ord_y)
                )
                tile = empty
                for col in range(columns):
                    total = jnp.sum(harm[peer, col] * weighted, axis=1, keepdims=True)
                    tile = jnp.where(lane == col, total, tile)
                send_buf[peer] = tile
                if inner_step < unroll - 1:
                    ord_copy(send_buf.at[peer], recv_buf.at[ord_here], sems, peer).start()
                else:
                    @pl.when(index < ords - 1)
                    def _():
                        ord_copy(send_buf.at[peer], recv_buf.at[ord_here], sems, peer).start()

                    @pl.when(index == ords - 1)
                    def _():
                        recv_buf[ord_here] = tile
            return carry

        lax.fori_loop(0, ords // unroll, step, 0)
        done = whole(ord_copy, recv_buf, sems, ords - 1, ord_peer(0))
        waits.append(done)
        return done, recv_buf

    def adjoint(recv_buf, rows, meanwhile):
        per_order = jnp.transpose(recv_buf[...].reshape(cycles, LANES)[:, :32])
        rows[...] = per_order
        curve = jnp.sum(rows[pl.ds(CURVE_COLUMN, 1), :], axis=1, keepdims=True)
        lane_all = lax.broadcasted_iota(jnp.int32, (degrees, LANES), 1)
        total = jnp.zeros((degrees, LANES), jnp.float32)
        for order in range(block):
            table = leg[order]
            for part in range(2):
                col = 2 * order + part
                value = jnp.sum(table * rows[pl.ds(col, 1), :], axis=1, keepdims=True)
                total = jnp.where(lane_all == col, value, total)
        column[pl.ds(0, degrees), :] = total
        which = parts[0]
        parts[0] += 1
        send_buf, recv_obs = part_send[which], part_recv[which]
        for owner in range(obss):
            packed = jnp.where(lane == SCALAR_LANE, curve, 0.0)
            for piece in range(GROUPS):
                start = owner * SHARE + piece * 8
                if start < degrees:
                    lines = column[pl.ds(start, 8), :]
                    packed = packed + (pltpu.roll(lines, GROUP * piece, 1) if piece else lines)
            send_buf[owner] = packed
        sems = next_round()

        def send(index, carry):
            peer = obs_peer(index)
            obs_copy(send_buf.at[peer], recv_obs.at[obs_here], sems, peer).start()
            return carry

        lax.fori_loop(0, obss - 1, send, 0)
        recv_obs[obs_here] = send_buf[obs_here]
        done = whole(obs_copy, recv_obs, sems, obss - 1, obs_peer(0))
        waits.append(done)
        meanwhile()
        done.wait_recv()
        summed = jnp.sum(recv_obs[...], axis=0)
        return summed, summed[0:1, SCALAR_LANE : SCALAR_LANE + 1]

    def send_ord(packed):
        which = shares[0]
        shares[0] += 1
        send_buf, recv_buf = share_send[which], share_recv[which]
        send_buf[...] = packed
        recv_buf[ord_here] = packed
        return gather_ord(send_buf, recv_buf), recv_buf

    def take_ord(sent, index_ref):
        done, recv_buf = sent
        done.wait_recv()
        everyone = jnp.sum(recv_buf[...], axis=0)
        chosen = jnp.where(lane == SCALAR_LANE, everyone, 0.0)
        for slot in range(block):
            number = index_ref[slot]
            source = lax.div(number, block)
            place = number - source * block
            turn = lax.rem(2 * slot - 2 * place + LANES, LANES)
            lines = pltpu.roll(recv_buf[source], turn, 1)
            chosen = jnp.where(jnp.logical_and(inside, slot_lane == slot), lines, chosen)
        return chosen

    def send_obs(packed):
        which = alls[0]
        alls[0] += 1
        send_buf, recv_buf = all_send[which], all_recv[which]
        send_buf[...] = packed
        recv_buf[obs_here] = packed
        return gather_obs(send_buf, recv_buf), recv_buf

    def take_obs(sent):
        done, recv_buf = sent
        done.wait_recv()
        total = jnp.sum(recv_buf[...], axis=0)[0:1, SCALAR_LANE : SCALAR_LANE + 1]
        return unpacked(recv_buf, degrees), total

    def exchange_obs(packed):
        return take_obs(send_obs(packed))

    def precondition(packed, table_of, alive, meanwhile):
        sent = send_obs(packed)
        meanwhile()
        lines, unused = take_obs(sent)
        column[pl.ds(0, degrees), :] = lines
        by_slot = jnp.transpose(column[...])
        result = jnp.zeros((8, LANES), jnp.float32)
        for slot in range(block):
            table = table_of(slot)
            for part in range(2):
                col = 2 * slot + part
                value = jnp.sum(table * by_slot[col : col + 1, : table.shape[1]], axis=1, keepdims=True)
                for piece in range(GROUPS):
                    result = jnp.where(lane == GROUP * piece + col, value[8 * piece : 8 * piece + 8], result)
        return jnp.where(alive, result, 0.0)

    share_start = pl.multiple_of(obs_here * SHARE, 8)

    def owner_table(slot):
        return inv[slot, pl.ds(share_start, SHARE), :]

    tiles_wide = inv_block.shape[2] // LANES
    spread_sems, inv_sems = next_round(), next_round()

    def build_spread():
        for slot in range(block):
            for wide in range(tiles_wide):
                width = min(LANES, degrees - wide * LANES)
                for piece in range(GROUPS):
                    lines = inv[slot, pl.ds(share_start + 8 * piece, 8), pl.ds(wide * LANES, width)]
                    if width < LANES:
                        lines = jnp.concatenate([lines, jnp.zeros((8, LANES - width), jnp.float32)], axis=1)
                    for half in range(2):
                        place = (wide * GROUPS + piece) * 2 + half
                        spread_send[place % ords, slot, place // ords] = lines[4 * half : 4 * half + 4]
        spread_recv[pl.ds(ord_here * block, block)] = spread_send[ord_here]

    def send_spread(first, last):
        def send(index, carry):
            peer = bulk_peer(index)
            ord_copy(spread_send.at[peer], spread_recv.at[pl.ds(ord_here * block, block)], spread_sems, peer).start()
            return carry

        lax.fori_loop(first, last, send, 0)

    def build_inv():
        cut = spread_recv.at[pl.ds(0, (ords - 1) * block)]
        done = ord_copy(cut, cut, spread_sems, ord_peer(0))
        waits.append(done)
        done.wait_recv()

        def step(index, carry):
            for order in range(block):
                number = index * block + order
                inv_send[index, order] = spread_recv[slot_all[lax.div(number, LANES), lax.rem(number, LANES)]]
            return carry

        lax.fori_loop(0, ords, step, 0)
        inv_recv[ord_here] = inv_send[ord_here]

    def send_inv(first, last):
        def send(index, carry):
            peer = bulk_peer(index)
            ord_copy(inv_send.at[peer], inv_recv.at[ord_here], inv_sems, peer).start()
            return carry

        lax.fori_loop(first, last, send, 0)

    def take_inv():
        done = whole(ord_copy, inv_recv, inv_sems, ords - 1, ord_peer(0))
        waits.append(done)
        done.wait_recv()
        for order in range(block):
            for wide in range(tiles_wide):
                for piece in range(GROUPS):
                    for half in range(2):
                        place = (wide * GROUPS + piece) * 2 + half
                        inv_block[order, pl.ds(8 * piece + 4 * half, 4), pl.ds(wide * LANES, LANES)] = inv_recv[
                            place % ords, order, place // ords
                        ]

    def find_slots():
        ids_done.wait_recv()
        ids_copy = pltpu.make_async_copy(ids_recv, ids_smem, local_sem.at[2])
        ids_copy.start()
        ids_copy.wait()
        position = sublane * LANES + lane

        def find(owner, found):
            for slot in range(block):
                found = jnp.where(position == ids_smem[owner, 0, slot], owner * block + slot, found)
            return found

        slot_vmem[...] = lax.fori_loop(0, ords, find, jnp.zeros((8, LANES), jnp.int32))
        slot_copy = pltpu.make_async_copy(slot_vmem, slot_all, local_sem.at[3])
        slot_copy.start()
        slot_copy.wait()
        for order in range(block):
            number = ord_here * block + order
            slot_smem[order] = slot_all[lax.div(number, LANES), lax.rem(number, LANES)]

    def with_energy(residual, precond):
        product = jnp.where(inside, residual * precond, 0.0)
        share = jnp.sum(jnp.sum(product, axis=1, keepdims=True), axis=0, keepdims=True)
        return jnp.where(lane == SCALAR_LANE, share, precond)

    def synthesize(coefficients, energy, rows, meanwhile):
        which = tiles[0]
        tiles[0] += 1
        sems = next_round()
        send_buf, recv_buf = tile_send[which], tile_recv[which]
        for order in range(block):
            table = leg[order]
            for part in range(2):
                col = 2 * order + part
                rows[pl.ds(col, 1), :] = jnp.sum(table * coefficients[:, col : col + 1], axis=0, keepdims=True)
        rows[pl.ds(CURVE_COLUMN, 1), :] = jnp.broadcast_to(energy, (1, cycles))
        turned = jnp.transpose(rows[...]).reshape(ords, CYCLES_HERE, 32)
        send_buf[:, :, pl.ds(0, 32)] = turned
        recv_buf[ord_here] = send_buf[ord_here]

        half = ord_z // 2
        sems = [sems] + [next_round() for unused in range(half)]

        def send_line(peer, sem):
            ord_copy(send_buf.at[peer], recv_buf.at[ord_here], sem, peer).start()

        for far in range(half, -1, -1):
            for step_z in ([far] if far in (0, half) else [far, ord_z - far]):
                for step_y in range(ord_y - 1, -1, -1):
                    if step_z or step_y:
                        send_line(ord_at(step_y, step_z), sems[far])

        meanwhile()
        sums = [jnp.zeros((CYCLES_HERE, SLOTS), jnp.float32) for unused in range(4)]
        energies = jnp.zeros((8, LANES), jnp.float32)
        for far in range(half + 1):
            steps = [far] if far in (0, half) else [far, ord_z - far]
            peers = len(steps) * ord_y - (far == 0)
            done = whole(ord_copy, recv_buf, sems[far], peers, ord_at(0, half))
            waits.append(done)
            done.wait_recv()
            for step_z in steps:
                for step_y in range(ord_y):
                    index = ord_at(step_y, step_z)
                    tile = recv_buf[index]
                    energies = energies + tile
                    for col in range(columns):
                        sums[col % 4] = sums[col % 4] + harm[index, col] * tile[:, col : col + 1]
        return (sums[0] + sums[1]) + (sums[2] + sums[3]), energies[0:1, CURVE_COLUMN : CURVE_COLUMN + 1]

    leg_copy.wait()
    done, recv_buf = per_cycle(windows_ref[pl.ds(2 * CYCLES_HERE, CYCLES_HERE), :], jnp.zeros((1, 1), jnp.float32))

    ids_done = gather_ord(ids_send, ids_recv)
    inv_copy.wait()
    build_spread()
    part = ords // 4
    last_bulk = 3 * part
    send_spread(0, part)
    done.wait_recv()
    summed, unused = adjoint(recv_buf, rows_ref[0], lambda: send_spread(part, 2 * part))
    residual = jnp.where(inside, summed, 0.0)
    sent = send_ord(residual)
    find_slots()
    owned = jnp.where(inside, take_ord(sent, own_ref), 0.0)
    precond = precondition(owned, owner_table, live, lambda: send_spread(2 * part, last_bulk))
    sent = send_ord(with_energy(owned, precond))
    chosen = take_ord(sent, slot_smem)
    sent = send_obs(chosen)
    send_spread(last_bulk, ords - 1)
    lines, energy_now = take_obs(sent)
    direction = jnp.where(inside, chosen, 0.0)
    solution = jnp.zeros((8, LANES), jnp.float32)
    gradient = None
    nothing = jnp.zeros((1, 1), jnp.float32)
    for iteration in range(ITERS):
        if iteration == 0:

            def prepare():
                build_inv()
                send_inv(0, part)

            gradient, unused = synthesize(lines, nothing, rows_ref[1], prepare)
        else:
            precond = precondition(residual, lambda slot: inv_block[slot], live_block, take_inv)
            lines, energy_block = exchange_obs(with_energy(residual, precond))
            ahead, energy = synthesize(lines, energy_block, rows_ref[1], lambda: None)
            ratio = energy / energy_now
            gradient = ahead + ratio * gradient
            direction = precond + ratio * direction
            energy_now = energy
        weighted = windows_ref[pl.ds(CYCLES_HERE, CYCLES_HERE), :] * gradient
        curve = jnp.sum(jnp.sum(weighted * gradient, axis=1, keepdims=True), axis=0, keepdims=True)
        done, recv_buf = per_cycle(weighted, curve)
        if iteration == 0:
            send_inv(part, last_bulk)
        done.wait_recv()
        summed, curvature = adjoint(
            recv_buf, rows_ref[0], (lambda: send_inv(last_bulk, ords - 1)) if iteration == 0 else (lambda: None)
        )
        step_size = energy_now / curvature
        solution = solution + step_size * direction
        residual = residual - step_size * jnp.where(inside, summed, 0.0)

    sent_solution, sent_residual = send_ord(solution), send_ord(residual)
    sent_solution = send_obs(take_ord(sent_solution, own_ref))
    sent_residual = send_obs(take_ord(sent_residual, own_ref))
    for which, (done, recv_buf) in enumerate((sent_solution, sent_residual)):
        done.wait_recv()
        packed_ref[which] = recv_buf[...]
    for done in waits:
        done.wait_send()


def buffers(rounds, *shape):
    return [pltpu.VMEM(shape, jnp.float32) for unused in range(rounds)]


def body(ord_y, ord_z, obs_x, longitude, cycle_of, obs_count, observed, obs_weight, legendre, precond_inv, order_of_slot):
    block, degrees, cycles = legendre.shape[1:]
    slab = longitude.shape[1]
    ords, obss = ord_y * ord_z, obs_x * 2
    vmem = pl.BlockSpec(memory_space=pltpu.VMEM)
    smem = pl.BlockSpec(memory_space=pltpu.SMEM)
    hbm = pl.BlockSpec(memory_space=pltpu.HBM)
    window = jax.ShapeDtypeStruct((3 * CYCLES_HERE, SLOTS), jnp.float32)
    lines = (slab // LANES, LANES)
    windows = pl.pallas_call(
        functools.partial(prologue_kernel, float(slab * obss)),
        out_shape=window,
        in_specs=[smem, vmem, vmem, vmem, vmem],
        out_specs=vmem,
        name="windows",
    )(obs_count, cycle_of.reshape(lines), longitude.reshape(lines), observed.reshape(lines), obs_weight.reshape(lines))
    result = jax.ShapeDtypeStruct((block, 2, degrees), jnp.float32)
    dims = (block, degrees, cycles, ord_y, ord_z, obs_x)
    column_rows = -(-max(degrees, 1) // LANES) * LANES
    tile_rounds = 1 + 2 * ITERS
    share_rounds = 4
    all_rounds = 2 * ITERS + 2
    deep = -(-(column_rows // LANES * GROUPS * 2) // ords)
    total_rounds = 1 + tile_rounds + (1 + ITERS) + share_rounds + all_rounds + ITERS * (ord_z // 2) + 2
    scratch = [
        pltpu.VMEM((ords, 2 * block, CYCLES_HERE, SLOTS), jnp.float32),
        pltpu.VMEM((block, degrees, cycles), jnp.float32),
        pltpu.VMEM((block, SHARE * obss, degrees), jnp.float32),
        pltpu.VMEM((column_rows, LANES), jnp.float32),
        [pltpu.VMEM((32, cycles), jnp.float32), pltpu.VMEM((32, cycles), jnp.float32)],
        buffers(tile_rounds, ords, CYCLES_HERE, LANES),
        buffers(tile_rounds, ords, CYCLES_HERE, LANES),
        buffers(1 + ITERS, obss, 8, LANES),
        buffers(1 + ITERS, obss, 8, LANES),
        buffers(share_rounds, 8, LANES),
        buffers(share_rounds, ords, 8, LANES),
        buffers(all_rounds, 8, LANES),
        buffers(all_rounds, obss, 8, LANES),
        pltpu.VMEM((1, LANES), jnp.int32),
        pltpu.VMEM((ords, 1, LANES), jnp.int32),
        pltpu.SMEM((ords, 1, LANES), jnp.int32),
        pltpu.VMEM((8, LANES), jnp.int32),
        pltpu.SMEM((8, LANES), jnp.int32),
        pltpu.SMEM((block,), jnp.int32),
        pltpu.VMEM((ords, block, deep, 4, LANES), jnp.float32),
        pltpu.VMEM((ords * block, deep, 4, LANES), jnp.float32),
        pltpu.VMEM((ords, block, deep, 4, LANES), jnp.float32),
        pltpu.VMEM((ords, block, deep, 4, LANES), jnp.float32),
        pltpu.VMEM((block, SHARE, column_rows), jnp.float32),
        pltpu.SemaphoreType.DMA((4,)),
        pltpu.SemaphoreType.DMA((total_rounds,)),
        pltpu.SemaphoreType.DMA((total_rounds,)),
    ]
    packed = pl.pallas_call(
        functools.partial(main_kernel, dims),
        out_shape=jax.ShapeDtypeStruct((2, obss, 8, LANES), jnp.float32),
        in_specs=[smem, vmem, hbm, hbm],
        out_specs=vmem,
        scratch_shapes=scratch,
        compiler_params=pltpu.CompilerParams(
            collective_id=0, has_side_effects=True
        ),
        name="solve",
    )(order_of_slot, windows, legendre[0], precond_inv)
    return pl.pallas_call(
        finish_kernel,
        out_shape=(result, result),
        in_specs=[vmem],
        out_specs=(vmem, vmem),
        scratch_shapes=[pltpu.VMEM((column_rows, LANES), jnp.float32)],
        name="unpack",
    )(packed)


def solution(mesh):
    placed = (
        P("obs", None),
        P("obs", None),
        P("obs"),
        P("obs", None),
        P("obs", None),
        P("obs", "ord", None, None),
        P("ord", None, None),
        P("ord"),
    )
    ords = mesh.shape["ord"]
    ord_y = 4 if ords == 32 else 2
    run = functools.partial(body, ord_y, ords // ord_y, mesh.shape["obs"] // 2)
    return jax.shard_map(
        run,
        mesh=mesh,
        in_specs=placed,
        out_specs=(P("ord", None, None), P("ord", None, None)),
        check_vma=False,
    )
```

```python
import functools

import jax
import jax.numpy as jnp
from jax import lax
from jax.experimental import pallas as pl
from jax.experimental.pallas import tpu as pltpu
from jax.sharding import PartitionSpec as P

ITERS = 2
MESH = pl.DeviceIdType.MESH
LANES = 128
SLOTS = 256
CYCLES_HERE = 8
GROUP = 20
GROUPS = 5
SHARE = 8 * GROUPS
SCALAR_LANE = 127
CURVE_COLUMN = 18
TWO_OVER_PI = 0.6366197723675814
PI_2_A = 1.5703125
PI_2_B = 0.00048351287841796875
PI_2_C = 3.13855707645416259765625e-07
PI_2_D = 6.077100628276710e-11


def sine_cosine(angle):
    turns = jnp.floor(angle * TWO_OVER_PI + 0.5)
    rest = angle - turns * PI_2_A
    rest = rest - turns * PI_2_B
    rest = rest - turns * PI_2_C
    rest = rest - turns * PI_2_D
    square = rest * rest
    sine = rest + rest * square * (-1.6666654611e-1 + square * (8.3321608736e-3 + square * -1.9515295891e-4))
    cosine = 1.0 - 0.5 * square + square * square * (
        4.166664568298827e-2 + square * (-1.388731625493765e-3 + square * 2.443315711809948e-5)
    )
    quadrant = turns.astype(jnp.int32)
    swap = (quadrant & 1) == 1
    sine_out = jnp.where(swap, cosine, sine)
    cosine_out = jnp.where(swap, sine, cosine)
    sine_out = jnp.where((quadrant & 2) == 2, -sine_out, sine_out)
    cosine_out = jnp.where(((quadrant + 1) & 2) == 2, -cosine_out, cosine_out)
    return sine_out, cosine_out


def prologue_kernel(total_obs, quarter, count_ref, cycle_ref, lon_ref, obs_ref, weight_ref, out_ref):
    first_cycle = lax.axis_index("ord") * 2
    rows = cycle_ref.shape[0]
    ids = cycle_ref[...]

    def before(cycle):
        return jnp.sum(jnp.where(ids < cycle, 1.0, 0.0)).astype(jnp.int32)

    starts = [[before(first_cycle + part * quarter + step) for step in range(3)] for part in range(4)]
    lane = lax.broadcasted_iota(jnp.int32, (1, LANES), 1)
    used = count_ref[0]
    for step in range(CYCLES_HERE):
        start = starts[step % 4][step // 4]
        count = starts[step % 4][step // 4 + 1] - start
        row = start // LANES
        shift = start - row * LANES
        turn = lax.rem(LANES - shift, LANES)
        lines = [jnp.minimum(row + part, rows - 1) for part in range(3)]
        head = lane < LANES - shift
        windows = []
        for ref in (lon_ref, obs_ref, weight_ref):
            turned = [pltpu.roll(ref[pl.ds(line, 1), :], turn, 1) for line in lines]
            windows.append([jnp.where(head, turned[part], turned[part + 1]) for part in range(2)])
        for part in range(2):
            slot = lane + part * LANES
            valid = jnp.logical_and(slot < count, start + slot < used)
            scale = jnp.where(valid, windows[2][part] / total_obs, 0.0)
            cut = pl.ds(part * LANES, LANES)
            for which, value in enumerate((windows[0][part], scale, scale * windows[1][part])):
                out_ref[pl.ds(which * CYCLES_HERE + step, 1), cut] = value


def unpacked(shares, degrees):
    pieces = []
    for owner in range(shares.shape[0]):
        for piece in range(GROUPS):
            if owner * SHARE + piece * 8 < degrees:
                lines = shares[owner]
                pieces.append(pltpu.roll(lines, LANES - GROUP * piece, 1) if piece else lines)
    return jnp.concatenate(pieces, axis=0)


def finish_kernel(packed_ref, solution_ref, residual_ref, column):
    block, unused, degrees = solution_ref.shape
    column[...] = jnp.zeros(column.shape, jnp.float32)
    for which, out in enumerate((solution_ref, residual_ref)):
        column[pl.ds(0, degrees), :] = unpacked(packed_ref.at[which], degrees)
        by_slot = jnp.transpose(column[...])
        for slot in range(block):
            out[slot] = by_slot[2 * slot : 2 * slot + 2, :degrees]


def offset(index):
    return ((index + 1) // 2) * (1 - 2 * (index % 2))


def main_kernel(
    dims, own_ref, windows_ref, leg_hbm, inv_hbm, packed_ref,
    harm, leg, inv, column, stage, rows_ref, tile_send, tile_recv, part_send, part_recv, share_send, share_recv,
    all_send, all_recv, ids_send, ids_recv, ids_smem, slot_vmem, slot_all, slot_smem, spread_send, spread_recv,
    inv_send, inv_recv, inv_block, last_send, last_recv, last_share, last_all, local_sem, send_sem, recv_sem,
):
    block, degrees, cycles, ord_y, ord_z, obs_x = dims
    ords = ord_y * ord_z
    obss = obs_x * 2
    columns = 2 * block
    unroll = 2 * ord_y
    ord_here = lax.axis_index("ord")
    obs_here = lax.axis_index("obs")

    for slot in range(block):
        inv[slot, pl.ds(degrees, SHARE * obss - degrees), :] = jnp.zeros((SHARE * obss - degrees, degrees), jnp.float32)
    leg_copy = pltpu.make_async_copy(leg_hbm, leg, local_sem.at[0])
    inv_copy = pltpu.make_async_copy(inv_hbm, inv.at[:, pl.ds(0, degrees), :], local_sem.at[1])
    leg_copy.start()
    inv_copy.start()

    here_y, here_z = lax.div(ord_here, ord_z), lax.rem(ord_here, ord_z)
    here_x, here_core = lax.div(obs_here, 2), lax.rem(obs_here, 2)

    def ord_at(step_y, step_z):
        return lax.rem(here_y + step_y, ord_y) * ord_z + lax.rem(here_z + step_z, ord_z)

    def ord_peer(index):
        return ord_at(ord_y // 2 + offset(index % ord_y), ord_z // 2 + offset(index // ord_y))

    def bulk_peer(index):
        return ord_at(ord_y // 2 + offset(index // ord_z), ord_z // 2 + offset(index % ord_z))

    def obs_peer(index):
        step_x = obs_x // 2 + offset(index // 2)
        step_core = 1 - index % 2
        return lax.rem(here_x + step_x, obs_x) * 2 + lax.rem(here_core + step_core, 2)

    barrier = pltpu.get_barrier_semaphore()

    for index in range(ords - 1):
        pl.semaphore_signal(barrier, inc=1, device_id={"ord": ord_peer(index)}, device_id_type=MESH)
    for index in range(obss - 1):
        pl.semaphore_signal(barrier, inc=1, device_id={"obs": obs_peer(index)}, device_id_type=MESH)

    lane = lax.broadcasted_iota(jnp.int32, (8, LANES), 1)
    sublane = lax.broadcasted_iota(jnp.int32, (8, LANES), 0)
    place = lane - 32 * (sublane % 4)
    group = lane // GROUP
    inner = lane % GROUP
    slot_lane = inner // 2
    degree_here = obs_here * SHARE + group * 8 + sublane
    inside = jnp.logical_and(jnp.logical_and(group < GROUPS, inner < columns), degree_here < degrees)
    order_lane = jnp.zeros((8, LANES), jnp.int32)
    for slot in range(block):
        order_lane = jnp.where(slot_lane == slot, own_ref[slot], order_lane)
    live = jnp.logical_and(inside, degree_here >= order_lane)
    live_block = jnp.logical_and(inside, degree_here >= ord_here * block + slot_lane)

    ids_row = jnp.zeros((1, LANES), jnp.int32)
    lane_row = lax.broadcasted_iota(jnp.int32, (1, LANES), 1)
    for slot in range(block):
        ids_row = jnp.where(lane_row == slot, own_ref[slot], ids_row)
    ids_send[...] = ids_row
    ids_recv[ord_here] = ids_row
    for which in range(len(rows_ref)):
        rows_ref[which][...] = jnp.zeros((32, cycles), jnp.float32)
    column[...] = jnp.zeros(column.shape, jnp.float32)

    longitude = windows_ref[pl.ds(0, CYCLES_HERE), :]

    def harmonic_block(index, carry):
        for order in range(block):
            number = (index * block + order).astype(jnp.float32)
            sine, cosine = sine_cosine(number * longitude)
            harm[index, 2 * order] = cosine
            harm[index, 2 * order + 1] = sine
        return carry

    lax.fori_loop(0, ords, harmonic_block, 0)
    pl.semaphore_wait(barrier, ords - 1 + obss - 1)

    rounds = [0]
    waits = []

    def next_round():
        rounds[0] += 1
        return rounds[0] - 1

    def ord_copy(source, target, sems, peer):
        return pltpu.make_async_remote_copy(
            src_ref=source, dst_ref=target, send_sem=send_sem.at[sems], recv_sem=recv_sem.at[sems],
            device_id={"ord": peer}, device_id_type=MESH,
        )

    def obs_copy(source, target, sems, peer):
        return pltpu.make_async_remote_copy(
            src_ref=source, dst_ref=target, send_sem=send_sem.at[sems], recv_sem=recv_sem.at[sems],
            device_id={"obs": peer}, device_id_type=MESH,
        )

    def whole(make, buffer, sems, peers, peer):
        cut = buffer.at[pl.ds(0, peers)]
        return make(cut, cut, sems, peer)

    def gather_ord(source, buffer):
        sems = next_round()

        def send(index, carry):
            ord_copy(source, buffer.at[ord_here], sems, ord_peer(index)).start()
            return carry

        lax.fori_loop(0, ords - 1, send, 0)
        done = whole(ord_copy, buffer, sems, ords - 1, ord_peer(0))
        waits.append(done)
        return done

    def gather_obs(source, buffer):
        sems = next_round()

        def send(index, carry):
            obs_copy(source, buffer.at[obs_here], sems, obs_peer(index)).start()
            return carry

        lax.fori_loop(0, obss - 1, send, 0)
        done = whole(obs_copy, buffer, sems, obss - 1, obs_peer(0))
        waits.append(done)
        return done

    tiles = [0]
    parts = [0]
    shares = [0]
    alls = [0]

    def per_cycle(weighted, curve):
        which = tiles[0]
        tiles[0] += 1
        sems = next_round()
        send_buf, recv_buf = tile_send[which], tile_recv[which]
        corner = jnp.logical_and(place == CURVE_COLUMN, sublane == 0)
        empty = jnp.where(corner, curve, 0.0)

        def step(outer, carry):
            for inner_step in range(unroll):
                index = outer * unroll + inner_step
                peer = ord_at(
                    ord_y // 2 + offset(inner_step % ord_y), ord_z // 2 + offset(outer * (unroll // ord_y) + inner_step // ord_y)
                )
                tile = empty
                for col in range(columns):
                    total = jnp.sum(harm[peer, col] * weighted, axis=1, keepdims=True)
                    tile = jnp.where(place == col, total, tile)
                tile = jnp.concatenate(
                    [jnp.sum(tile[4 * half : 4 * half + 4], axis=0, keepdims=True) for half in range(2)], axis=0
                )
                send_buf[peer] = tile
                if inner_step < unroll - 1:
                    ord_copy(send_buf.at[peer], recv_buf.at[ord_here], sems, peer).start()
                else:
                    @pl.when(index < ords - 1)
                    def _():
                        ord_copy(send_buf.at[peer], recv_buf.at[ord_here], sems, peer).start()

                    @pl.when(index == ords - 1)
                    def _():
                        recv_buf[ord_here] = tile
            return carry

        lax.fori_loop(0, ords // unroll, step, 0)
        done = whole(ord_copy, recv_buf, sems, ords - 1, ord_peer(0))
        waits.append(done)
        return done, recv_buf

    def adjoint(recv_buf, rows, meanwhile):
        for source in range(ords):
            stage[pl.ds(2 * source, 2), :] = recv_buf[source]
        turned = jnp.transpose(stage[...])
        rows[...] = jnp.concatenate([turned[32 * part : 32 * part + 32] for part in range(4)], axis=1)
        curve = jnp.sum(rows[pl.ds(CURVE_COLUMN, 1), :], axis=1, keepdims=True)
        lane_all = lax.broadcasted_iota(jnp.int32, (degrees, LANES), 1)
        total = jnp.zeros((degrees, LANES), jnp.float32)
        for order in range(block):
            table = leg[order]
            for part in range(2):
                col = 2 * order + part
                value = jnp.sum(table * rows[pl.ds(col, 1), :], axis=1, keepdims=True)
                total = jnp.where(lane_all == col, value, total)
        column[pl.ds(0, degrees), :] = total
        which = parts[0]
        parts[0] += 1
        send_buf, recv_obs = part_send[which], part_recv[which]
        for owner in range(obss):
            packed = jnp.where(lane == SCALAR_LANE, curve, 0.0)
            for piece in range(GROUPS):
                start = owner * SHARE + piece * 8
                if start < degrees:
                    lines = column[pl.ds(start, 8), :]
                    packed = packed + (pltpu.roll(lines, GROUP * piece, 1) if piece else lines)
            send_buf[owner] = packed
        sems = next_round()

        def send(index, carry):
            peer = obs_peer(index)
            obs_copy(send_buf.at[peer], recv_obs.at[obs_here], sems, peer).start()
            return carry

        lax.fori_loop(0, obss - 1, send, 0)
        recv_obs[obs_here] = send_buf[obs_here]
        done = whole(obs_copy, recv_obs, sems, obss - 1, obs_peer(0))
        waits.append(done)
        meanwhile()
        done.wait_recv()
        summed = jnp.sum(recv_obs[...], axis=0)
        return summed, summed[0:1, SCALAR_LANE : SCALAR_LANE + 1]

    def send_ord(packed):
        which = shares[0]
        shares[0] += 1
        send_buf, recv_buf = share_send[which], share_recv[which]
        send_buf[...] = packed
        recv_buf[ord_here] = packed
        return gather_ord(send_buf, recv_buf), recv_buf

    def choose(block_line, index_ref, chosen):
        for slot in range(block):
            number = index_ref[slot]
            source = lax.div(number, block)
            shift = lax.rem(2 * slot - 2 * (number - source * block) + LANES, LANES)
            lines = pltpu.roll(block_line(source), shift, 1)
            chosen = jnp.where(jnp.logical_and(inside, slot_lane == slot), lines, chosen)
        return chosen

    def take_ord(sent, index_ref):
        done, recv_buf = sent
        done.wait_recv()
        everyone = jnp.sum(recv_buf[...], axis=0)
        return choose(lambda source: recv_buf[source], index_ref, jnp.where(lane == SCALAR_LANE, everyone, 0.0))

    def send_obs(packed):
        which = alls[0]
        alls[0] += 1
        send_buf, recv_buf = all_send[which], all_recv[which]
        send_buf[...] = packed
        recv_buf[obs_here] = packed
        return gather_obs(send_buf, recv_buf), recv_buf

    def take_obs(sent):
        done, recv_buf = sent
        done.wait_recv()
        total = jnp.sum(recv_buf[...], axis=0)[0:1, SCALAR_LANE : SCALAR_LANE + 1]
        return unpacked(recv_buf, degrees), total

    def exchange_obs(packed):
        return take_obs(send_obs(packed))

    def precondition(packed, table_of, alive, meanwhile):
        sent = send_obs(packed)
        meanwhile()
        lines, unused = take_obs(sent)
        column[pl.ds(0, degrees), :] = lines
        by_slot = jnp.transpose(column[...])
        result = jnp.zeros((8, LANES), jnp.float32)
        for slot in range(block):
            table = table_of(slot)
            for part in range(2):
                col = 2 * slot + part
                value = jnp.sum(table * by_slot[col : col + 1, : table.shape[1]], axis=1, keepdims=True)
                for piece in range(GROUPS):
                    result = jnp.where(lane == GROUP * piece + col, value[8 * piece : 8 * piece + 8], result)
        return jnp.where(alive, result, 0.0)

    share_start = pl.multiple_of(obs_here * SHARE, 8)

    def owner_table(slot):
        return inv[slot, pl.ds(share_start, SHARE), :]

    tiles_wide = inv_block.shape[2] // LANES
    spread_sems, inv_sems = next_round(), next_round()

    def build_spread():
        for slot in range(block):
            for wide in range(tiles_wide):
                width = min(LANES, degrees - wide * LANES)
                for piece in range(GROUPS):
                    lines = inv[slot, pl.ds(share_start + 8 * piece, 8), pl.ds(wide * LANES, width)]
                    if width < LANES:
                        lines = jnp.concatenate([lines, jnp.zeros((8, LANES - width), jnp.float32)], axis=1)
                    for half in range(2):
                        place = (wide * GROUPS + piece) * 2 + half
                        spread_send[place % ords, slot, place // ords] = lines[4 * half : 4 * half + 4]
        spread_recv[pl.ds(ord_here * block, block)] = spread_send[ord_here]

    def send_spread(first, last):
        def send(index, carry):
            peer = bulk_peer(index)
            ord_copy(spread_send.at[peer], spread_recv.at[pl.ds(ord_here * block, block)], spread_sems, peer).start()
            return carry

        lax.fori_loop(first, last, send, 0)

    def build_inv():
        cut = spread_recv.at[pl.ds(0, (ords - 1) * block)]
        done = ord_copy(cut, cut, spread_sems, ord_peer(0))
        waits.append(done)
        done.wait_recv()

        def step(index, carry):
            for order in range(block):
                number = index * block + order
                inv_send[index, order] = spread_recv[slot_all[lax.div(number, LANES), lax.rem(number, LANES)]]
            return carry

        lax.fori_loop(0, ords, step, 0)
        inv_recv[ord_here] = inv_send[ord_here]

    def send_inv(first, last):
        def send(index, carry):
            peer = bulk_peer(index)
            ord_copy(inv_send.at[peer], inv_recv.at[ord_here], inv_sems, peer).start()
            return carry

        lax.fori_loop(first, last, send, 0)

    def take_inv():
        done = whole(ord_copy, inv_recv, inv_sems, ords - 1, ord_peer(0))
        waits.append(done)
        done.wait_recv()
        for order in range(block):
            for wide in range(tiles_wide):
                for piece in range(GROUPS):
                    for half in range(2):
                        place = (wide * GROUPS + piece) * 2 + half
                        inv_block[order, pl.ds(8 * piece + 4 * half, 4), pl.ds(wide * LANES, LANES)] = inv_recv[
                            place % ords, order, place // ords
                        ]

    def find_slots():
        ids_done.wait_recv()
        ids_copy = pltpu.make_async_copy(ids_recv, ids_smem, local_sem.at[2])
        ids_copy.start()
        ids_copy.wait()
        position = sublane * LANES + lane

        def find(owner, found):
            for slot in range(block):
                found = jnp.where(position == ids_smem[owner, 0, slot], owner * block + slot, found)
            return found

        slot_vmem[...] = lax.fori_loop(0, ords, find, jnp.zeros((8, LANES), jnp.int32))
        slot_copy = pltpu.make_async_copy(slot_vmem, slot_all, local_sem.at[3])
        slot_copy.start()
        slot_copy.wait()
        for order in range(block):
            number = ord_here * block + order
            slot_smem[order] = slot_all[lax.div(number, LANES), lax.rem(number, LANES)]

    def with_energy(residual, precond):
        product = jnp.where(inside, residual * precond, 0.0)
        share = jnp.sum(jnp.sum(product, axis=1, keepdims=True), axis=0, keepdims=True)
        return jnp.where(lane == SCALAR_LANE, share, precond)

    def synthesize(coefficients, energy, rows, meanwhile):
        which = tiles[0]
        tiles[0] += 1
        sems = next_round()
        send_buf, recv_buf = tile_send[which], tile_recv[which]
        for order in range(block):
            table = leg[order]
            for part in range(2):
                col = 2 * order + part
                rows[pl.ds(col, 1), :] = jnp.sum(table * coefficients[:, col : col + 1], axis=0, keepdims=True)
        rows[pl.ds(CURVE_COLUMN, 1), :] = jnp.broadcast_to(energy, (1, cycles))
        quarter = cycles // 4
        lines = rows[...]
        turned = jnp.transpose(
            jnp.concatenate([lines[:, part * quarter : part * quarter + quarter] for part in range(4)], axis=0)
        )
        for target in range(ords):
            send_buf[target] = turned[2 * target : 2 * target + 2]
        recv_buf[ord_here] = send_buf[ord_here]

        half = ord_z // 2
        sems = [sems] + [next_round() for unused in range(half)]

        def send_line(peer, sem):
            ord_copy(send_buf.at[peer], recv_buf.at[ord_here], sem, peer).start()

        for far in range(half, -1, -1):
            for step_z in ([far] if far in (0, half) else [far, ord_z - far]):
                for step_y in range(ord_y - 1, -1, -1):
                    if step_z or step_y:
                        send_line(ord_at(step_y, step_z), sems[far])

        meanwhile()
        sums = [jnp.zeros((CYCLES_HERE, SLOTS), jnp.float32) for unused in range(4)]
        energies = jnp.zeros((8, LANES), jnp.float32)
        for far in range(half + 1):
            steps = [far] if far in (0, half) else [far, ord_z - far]
            peers = len(steps) * ord_y - (far == 0)
            done = whole(ord_copy, recv_buf, sems[far], peers, ord_at(0, half))
            waits.append(done)
            done.wait_recv()
            for step_z in steps:
                for step_y in range(ord_y):
                    index = ord_at(step_y, step_z)
                    pair = recv_buf[index]
                    tile = jnp.concatenate(
                        [jnp.broadcast_to(pair[half : half + 1], (4, LANES)) for half in range(2)], axis=0
                    )
                    spread = tile
                    for part in range(1, 4):
                        tile = jnp.where(sublane % 4 == part, pltpu.roll(spread, LANES - 32 * part, 1), tile)
                    energies = energies + tile
                    for col in range(columns):
                        sums[col % 4] = sums[col % 4] + harm[index, col] * tile[:, col : col + 1]
        return (sums[0] + sums[1]) + (sums[2] + sums[3]), energies[0:1, CURVE_COLUMN : CURVE_COLUMN + 1]

    leg_copy.wait()
    done, recv_buf = per_cycle(windows_ref[pl.ds(2 * CYCLES_HERE, CYCLES_HERE), :], jnp.zeros((1, 1), jnp.float32))

    ids_done = gather_ord(ids_send, ids_recv)
    inv_copy.wait()
    build_spread()
    part = ords // 4
    last_bulk = 3 * part
    send_spread(0, part)
    done.wait_recv()
    summed, unused = adjoint(recv_buf, rows_ref[0], lambda: send_spread(part, 2 * part))
    residual = jnp.where(inside, summed, 0.0)
    sent = send_ord(residual)
    find_slots()
    owned = jnp.where(inside, take_ord(sent, own_ref), 0.0)
    precond = precondition(owned, owner_table, live, lambda: send_spread(2 * part, last_bulk))
    sent = send_ord(with_energy(owned, precond))
    chosen = take_ord(sent, slot_smem)
    sent = send_obs(chosen)
    send_spread(last_bulk, ords - 1)
    lines, energy_now = take_obs(sent)
    direction = jnp.where(inside, chosen, 0.0)
    solution = jnp.zeros((8, LANES), jnp.float32)
    gradient = None
    nothing = jnp.zeros((1, 1), jnp.float32)
    for iteration in range(ITERS):
        if iteration == 0:

            def prepare():
                build_inv()
                send_inv(0, part)

            gradient, unused = synthesize(lines, nothing, rows_ref[1], prepare)
        else:
            precond = precondition(residual, lambda slot: inv_block[slot], live_block, take_inv)
            lines, energy_block = exchange_obs(with_energy(residual, precond))
            ahead, energy = synthesize(lines, energy_block, rows_ref[1], lambda: None)
            ratio = energy / energy_now
            gradient = ahead + ratio * gradient
            direction = precond + ratio * direction
            energy_now = energy
        weighted = windows_ref[pl.ds(CYCLES_HERE, CYCLES_HERE), :] * gradient
        curve = jnp.sum(jnp.sum(weighted * gradient, axis=1, keepdims=True), axis=0, keepdims=True)
        done, recv_buf = per_cycle(weighted, curve)
        if iteration == 0:
            send_inv(part, last_bulk)
        done.wait_recv()
        summed, curvature = adjoint(
            recv_buf, rows_ref[0], (lambda: send_inv(last_bulk, ords - 1)) if iteration == 0 else (lambda: None)
        )
        step_size = energy_now / curvature
        solution = solution + step_size * direction
        residual = residual - step_size * jnp.where(inside, summed, 0.0)

    for which, value in enumerate((solution, residual)):
        last_send[which] = value
        last_recv[ord_here, which] = value
    gather_ord(last_send, last_recv).wait_recv()
    for which in range(2):
        value = choose(lambda source, which=which: last_recv[source, which], own_ref, jnp.zeros((8, LANES), jnp.float32))
        last_share[which] = value
        last_all[obs_here, which] = value
    gather_obs(last_share, last_all).wait_recv()
    for which in range(2):
        packed_ref[which] = last_all[:, which]
    for done in waits:
        done.wait_send()


def buffers(rounds, *shape):
    return [pltpu.VMEM(shape, jnp.float32) for unused in range(rounds)]


def body(ord_y, ord_z, obs_x, longitude, cycle_of, obs_count, observed, obs_weight, legendre, precond_inv, order_of_slot):
    block, degrees, cycles = legendre.shape[1:]
    slab = longitude.shape[1]
    ords, obss = ord_y * ord_z, obs_x * 2
    vmem = pl.BlockSpec(memory_space=pltpu.VMEM)
    smem = pl.BlockSpec(memory_space=pltpu.SMEM)
    hbm = pl.BlockSpec(memory_space=pltpu.HBM)
    window = jax.ShapeDtypeStruct((3 * CYCLES_HERE, SLOTS), jnp.float32)
    lines = (slab // LANES, LANES)
    windows = pl.pallas_call(
        functools.partial(prologue_kernel, float(slab * obss), cycles // 4),
        out_shape=window,
        in_specs=[smem, vmem, vmem, vmem, vmem],
        out_specs=vmem,
        name="windows",
    )(obs_count, cycle_of.reshape(lines), longitude.reshape(lines), observed.reshape(lines), obs_weight.reshape(lines))
    result = jax.ShapeDtypeStruct((block, 2, degrees), jnp.float32)
    dims = (block, degrees, cycles, ord_y, ord_z, obs_x)
    column_rows = -(-max(degrees, 1) // LANES) * LANES
    tile_rounds = 1 + 2 * ITERS
    share_rounds = 2
    all_rounds = 2 * ITERS
    deep = -(-(column_rows // LANES * GROUPS * 2) // ords)
    total_rounds = 1 + tile_rounds + (1 + ITERS) + share_rounds + all_rounds + ITERS * (ord_z // 2) + 4
    scratch = [
        pltpu.VMEM((ords, 2 * block, CYCLES_HERE, SLOTS), jnp.float32),
        pltpu.VMEM((block, degrees, cycles), jnp.float32),
        pltpu.VMEM((block, SHARE * obss, degrees), jnp.float32),
        pltpu.VMEM((column_rows, LANES), jnp.float32),
        pltpu.VMEM((2 * ords, LANES), jnp.float32),
        [pltpu.VMEM((32, cycles), jnp.float32), pltpu.VMEM((32, cycles), jnp.float32)],
        buffers(tile_rounds, ords, 2, LANES),
        buffers(tile_rounds, ords, 2, LANES),
        buffers(1 + ITERS, obss, 8, LANES),
        buffers(1 + ITERS, obss, 8, LANES),
        buffers(share_rounds, 8, LANES),
        buffers(share_rounds, ords, 8, LANES),
        buffers(all_rounds, 8, LANES),
        buffers(all_rounds, obss, 8, LANES),
        pltpu.VMEM((1, LANES), jnp.int32),
        pltpu.VMEM((ords, 1, LANES), jnp.int32),
        pltpu.SMEM((ords, 1, LANES), jnp.int32),
        pltpu.VMEM((8, LANES), jnp.int32),
        pltpu.SMEM((8, LANES), jnp.int32),
        pltpu.SMEM((block,), jnp.int32),
        pltpu.VMEM((ords, block, deep, 4, LANES), jnp.float32),
        pltpu.VMEM((ords * block, deep, 4, LANES), jnp.float32),
        pltpu.VMEM((ords, block, deep, 4, LANES), jnp.float32),
        pltpu.VMEM((ords, block, deep, 4, LANES), jnp.float32),
        pltpu.VMEM((block, SHARE, column_rows), jnp.float32),
        pltpu.VMEM((2, 8, LANES), jnp.float32),
        pltpu.VMEM((ords, 2, 8, LANES), jnp.float32),
        pltpu.VMEM((2, 8, LANES), jnp.float32),
        pltpu.VMEM((obss, 2, 8, LANES), jnp.float32),
        pltpu.SemaphoreType.DMA((4,)),
        pltpu.SemaphoreType.DMA((total_rounds,)),
        pltpu.SemaphoreType.DMA((total_rounds,)),
    ]
    packed = pl.pallas_call(
        functools.partial(main_kernel, dims),
        out_shape=jax.ShapeDtypeStruct((2, obss, 8, LANES), jnp.float32),
        in_specs=[smem, vmem, hbm, hbm],
        out_specs=vmem,
        scratch_shapes=scratch,
        compiler_params=pltpu.CompilerParams(
            collective_id=0, has_side_effects=True
        ),
        name="solve",
    )(order_of_slot, windows, legendre[0], precond_inv)
    return pl.pallas_call(
        finish_kernel,
        out_shape=(result, result),
        in_specs=[vmem],
        out_specs=(vmem, vmem),
        scratch_shapes=[pltpu.VMEM((column_rows, LANES), jnp.float32)],
        name="unpack",
    )(packed)


def solution(mesh):
    placed = (
        P("obs", None),
        P("obs", None),
        P("obs"),
        P("obs", None),
        P("obs", None),
        P("obs", "ord", None, None),
        P("ord", None, None),
        P("ord"),
    )
    ords = mesh.shape["ord"]
    ord_y = 4 if ords == 32 else 2
    run = functools.partial(body, ord_y, ords // ord_y, mesh.shape["obs"] // 2)
    return jax.shard_map(
        run,
        mesh=mesh,
        in_specs=placed,
        out_specs=(P("ord", None, None), P("ord", None, None)),
        check_vma=False,
    )
```

```python
import functools

import jax
import jax.numpy as jnp
from jax import lax
from jax.experimental import pallas as pl
from jax.experimental.pallas import tpu as pltpu
from jax.sharding import PartitionSpec as P

ITERS = 2
MESH = pl.DeviceIdType.MESH
LANES = 128
SLOTS = 256
CYCLES_HERE = 8
GROUP = 20
GROUPS = 5
SHARE = 8 * GROUPS
SCALAR_LANE = 127
CURVE_COLUMN = 18
TWO_OVER_PI = 0.6366197723675814
PI_2_A = 1.5703125
PI_2_B = 0.00048351287841796875
PI_2_C = 3.13855707645416259765625e-07
PI_2_D = 6.077100628276710e-11


def sine_cosine(angle):
    turns = jnp.floor(angle * TWO_OVER_PI + 0.5)
    rest = angle - turns * PI_2_A
    rest = rest - turns * PI_2_B
    rest = rest - turns * PI_2_C
    rest = rest - turns * PI_2_D
    square = rest * rest
    sine = rest + rest * square * (-1.6666654611e-1 + square * (8.3321608736e-3 + square * -1.9515295891e-4))
    cosine = 1.0 - 0.5 * square + square * square * (
        4.166664568298827e-2 + square * (-1.388731625493765e-3 + square * 2.443315711809948e-5)
    )
    quadrant = turns.astype(jnp.int32)
    swap = (quadrant & 1) == 1
    sine_out = jnp.where(swap, cosine, sine)
    cosine_out = jnp.where(swap, sine, cosine)
    sine_out = jnp.where((quadrant & 2) == 2, -sine_out, sine_out)
    cosine_out = jnp.where(((quadrant + 1) & 2) == 2, -cosine_out, cosine_out)
    return sine_out, cosine_out


def fill_windows(total_obs, quarter, count_ref, cycle_ref, lon_ref, obs_ref, weight_ref, out_ref):
    first_cycle = lax.axis_index("ord") * 2
    rows = cycle_ref.shape[0]
    ids = cycle_ref[...]

    def before(cycle):
        return jnp.sum(jnp.where(ids < cycle, 1, 0))

    starts = [[before(first_cycle + part * quarter + step) for step in range(3)] for part in range(4)]
    lane = lax.broadcasted_iota(jnp.int32, (1, LANES), 1)
    used = count_ref[0]
    for step in range(CYCLES_HERE):
        start = starts[step % 4][step // 4]
        count = starts[step % 4][step // 4 + 1] - start
        row = start // LANES
        shift = start - row * LANES
        turn = lax.rem(LANES - shift, LANES)
        lines = [jnp.minimum(row + part, rows - 1) for part in range(3)]
        head = lane < LANES - shift
        windows = []
        for ref in (lon_ref, obs_ref, weight_ref):
            turned = [pltpu.roll(ref[pl.ds(line, 1), :], turn, 1) for line in lines]
            windows.append([jnp.where(head, turned[part], turned[part + 1]) for part in range(2)])
        for part in range(2):
            slot = lane + part * LANES
            valid = jnp.logical_and(slot < count, start + slot < used)
            scale = jnp.where(valid, windows[2][part] / total_obs, 0.0)
            cut = pl.ds(part * LANES, LANES)
            for which, value in enumerate((windows[0][part], scale, scale * windows[1][part])):
                out_ref[pl.ds(which * CYCLES_HERE + step, 1), cut] = value


def unpacked(shares, degrees):
    pieces = []
    for owner in range(shares.shape[0]):
        for piece in range(GROUPS):
            if owner * SHARE + piece * 8 < degrees:
                lines = shares[owner]
                pieces.append(pltpu.roll(lines, LANES - GROUP * piece, 1) if piece else lines)
    return jnp.concatenate(pieces, axis=0)


def finish_kernel(packed_ref, solution_ref, residual_ref, column):
    block, unused, degrees = solution_ref.shape
    column[...] = jnp.zeros(column.shape, jnp.float32)
    for which, out in enumerate((solution_ref, residual_ref)):
        column[pl.ds(0, degrees), :] = unpacked(packed_ref.at[which], degrees)
        by_slot = jnp.transpose(column[...])
        for slot in range(block):
            out[slot] = by_slot[2 * slot : 2 * slot + 2, :degrees]


def offset(index):
    return ((index + 1) // 2) * (1 - 2 * (index % 2))


def main_kernel(
    dims, total_obs, own_ref, count_ref, cycle_ref, lon_ref, obs_ref, weight_ref, leg_hbm, inv_hbm, packed_ref, windows_ref,
    harm, leg, inv, column, stage, rows_ref, tile_send, tile_recv, part_send, part_recv, share_send, share_recv,
    all_send, all_recv, ids_send, ids_recv, ids_smem, slot_vmem, slot_all, slot_smem, spread_send, spread_recv,
    inv_send, inv_recv, inv_block, last_send, last_recv, last_share, last_all, local_sem, send_sem, recv_sem,
):
    block, degrees, cycles, ord_y, ord_z, obs_x = dims
    ords = ord_y * ord_z
    obss = obs_x * 2
    columns = 2 * block
    unroll = 2 * ord_y
    ord_here = lax.axis_index("ord")
    obs_here = lax.axis_index("obs")

    for slot in range(block):
        inv[slot, pl.ds(degrees, SHARE * obss - degrees), :] = jnp.zeros((SHARE * obss - degrees, degrees), jnp.float32)
    leg_copy = pltpu.make_async_copy(leg_hbm, leg, local_sem.at[0])
    inv_copy = pltpu.make_async_copy(inv_hbm, inv.at[:, pl.ds(0, degrees), :], local_sem.at[1])
    leg_copy.start()
    inv_copy.start()

    here_y, here_z = lax.div(ord_here, ord_z), lax.rem(ord_here, ord_z)
    here_x, here_core = lax.div(obs_here, 2), lax.rem(obs_here, 2)

    def ord_at(step_y, step_z):
        return lax.rem(here_y + step_y, ord_y) * ord_z + lax.rem(here_z + step_z, ord_z)

    def ord_peer(index):
        return ord_at(ord_y // 2 + offset(index % ord_y), ord_z // 2 + offset(index // ord_y))

    def bulk_peer(index):
        return ord_at(ord_y // 2 + offset(index // ord_z), ord_z // 2 + offset(index % ord_z))

    def obs_peer(index):
        step_x = obs_x // 2 + offset(index // 2)
        step_core = 1 - index % 2
        return lax.rem(here_x + step_x, obs_x) * 2 + lax.rem(here_core + step_core, 2)

    barrier = pltpu.get_barrier_semaphore()

    for index in range(ords - 1):
        pl.semaphore_signal(barrier, inc=1, device_id={"ord": ord_peer(index)}, device_id_type=MESH)
    for index in range(obss - 1):
        pl.semaphore_signal(barrier, inc=1, device_id={"obs": obs_peer(index)}, device_id_type=MESH)

    lane = lax.broadcasted_iota(jnp.int32, (8, LANES), 1)
    sublane = lax.broadcasted_iota(jnp.int32, (8, LANES), 0)
    place = lane - 32 * (sublane % 4)
    group = lane // GROUP
    inner = lane % GROUP
    slot_lane = inner // 2
    degree_here = obs_here * SHARE + group * 8 + sublane
    inside = jnp.logical_and(jnp.logical_and(group < GROUPS, inner < columns), degree_here < degrees)
    order_lane = jnp.zeros((8, LANES), jnp.int32)
    for slot in range(block):
        order_lane = jnp.where(slot_lane == slot, own_ref[slot], order_lane)
    live = jnp.logical_and(inside, degree_here >= order_lane)
    live_block = jnp.logical_and(inside, degree_here >= ord_here * block + slot_lane)

    ids_row = jnp.zeros((1, LANES), jnp.int32)
    lane_row = lax.broadcasted_iota(jnp.int32, (1, LANES), 1)
    for slot in range(block):
        ids_row = jnp.where(lane_row == slot, own_ref[slot], ids_row)
    ids_send[...] = ids_row
    ids_recv[ord_here] = ids_row
    for which in range(len(rows_ref)):
        rows_ref[which][...] = jnp.zeros((32, cycles), jnp.float32)
    column[...] = jnp.zeros(column.shape, jnp.float32)

    fill_windows(total_obs, cycles // 4, count_ref, cycle_ref, lon_ref, obs_ref, weight_ref, windows_ref)
    longitude = windows_ref[pl.ds(0, CYCLES_HERE), :]

    def harmonic_block(index, carry):
        for order in range(block):
            number = (index * block + order).astype(jnp.float32)
            sine, cosine = sine_cosine(number * longitude)
            harm[index, 2 * order] = cosine
            harm[index, 2 * order + 1] = sine
        return carry

    lax.fori_loop(0, ords, harmonic_block, 0)
    pl.semaphore_wait(barrier, ords - 1 + obss - 1)

    rounds = [0]
    waits = []

    def next_round():
        rounds[0] += 1
        return rounds[0] - 1

    def ord_copy(source, target, sems, peer):
        return pltpu.make_async_remote_copy(
            src_ref=source, dst_ref=target, send_sem=send_sem.at[sems], recv_sem=recv_sem.at[sems],
            device_id={"ord": peer}, device_id_type=MESH,
        )

    def obs_copy(source, target, sems, peer):
        return pltpu.make_async_remote_copy(
            src_ref=source, dst_ref=target, send_sem=send_sem.at[sems], recv_sem=recv_sem.at[sems],
            device_id={"obs": peer}, device_id_type=MESH,
        )

    def whole(make, buffer, sems, peers, peer):
        cut = buffer.at[pl.ds(0, peers)]
        return make(cut, cut, sems, peer)

    def gather_ord(source, buffer):
        sems = next_round()

        def send(index, carry):
            ord_copy(source, buffer.at[ord_here], sems, ord_peer(index)).start()
            return carry

        lax.fori_loop(0, ords - 1, send, 0)
        done = whole(ord_copy, buffer, sems, ords - 1, ord_peer(0))
        waits.append(done)
        return done

    def gather_obs(source, buffer):
        sems = next_round()

        def send(index, carry):
            obs_copy(source, buffer.at[obs_here], sems, obs_peer(index)).start()
            return carry

        lax.fori_loop(0, obss - 1, send, 0)
        done = whole(obs_copy, buffer, sems, obss - 1, obs_peer(0))
        waits.append(done)
        return done

    tiles = [0]
    parts = [0]
    shares = [0]
    alls = [0]

    def per_cycle(weighted, curve):
        which = tiles[0]
        tiles[0] += 1
        sems = next_round()
        send_buf, recv_buf = tile_send[which], tile_recv[which]
        corner = jnp.logical_and(place == CURVE_COLUMN, sublane == 0)
        empty = jnp.where(corner, curve, 0.0)

        def step(outer, carry):
            for inner_step in range(unroll):
                index = outer * unroll + inner_step
                peer = ord_at(
                    ord_y // 2 + offset(inner_step % ord_y), ord_z // 2 + offset(outer * (unroll // ord_y) + inner_step // ord_y)
                )
                tile = empty
                for col in range(columns):
                    total = jnp.sum(harm[peer, col] * weighted, axis=1, keepdims=True)
                    tile = jnp.where(place == col, total, tile)
                tile = jnp.concatenate(
                    [jnp.sum(tile[4 * half : 4 * half + 4], axis=0, keepdims=True) for half in range(2)], axis=0
                )
                send_buf[peer] = tile
                if inner_step < unroll - 1:
                    ord_copy(send_buf.at[peer], recv_buf.at[ord_here], sems, peer).start()
                else:
                    @pl.when(index < ords - 1)
                    def _():
                        ord_copy(send_buf.at[peer], recv_buf.at[ord_here], sems, peer).start()

                    @pl.when(index == ords - 1)
                    def _():
                        recv_buf[ord_here] = tile
            return carry

        lax.fori_loop(0, ords // unroll, step, 0)
        done = whole(ord_copy, recv_buf, sems, ords - 1, ord_peer(0))
        waits.append(done)
        return done, recv_buf

    def adjoint(recv_buf, rows, meanwhile):
        for source in range(ords):
            stage[pl.ds(2 * source, 2), :] = recv_buf[source]
        turned = jnp.transpose(stage[...])
        rows[...] = jnp.concatenate([turned[32 * part : 32 * part + 32] for part in range(4)], axis=1)
        curve = jnp.sum(rows[pl.ds(CURVE_COLUMN, 1), :], axis=1, keepdims=True)
        lane_all = lax.broadcasted_iota(jnp.int32, (degrees, LANES), 1)
        total = jnp.zeros((degrees, LANES), jnp.float32)
        for order in range(block):
            table = leg[order]
            for part in range(2):
                col = 2 * order + part
                value = jnp.sum(table * rows[pl.ds(col, 1), :], axis=1, keepdims=True)
                total = jnp.where(lane_all == col, value, total)
        column[pl.ds(0, degrees), :] = total
        which = parts[0]
        parts[0] += 1
        send_buf, recv_obs = part_send[which], part_recv[which]
        for owner in range(obss):
            packed = jnp.where(lane == SCALAR_LANE, curve, 0.0)
            for piece in range(GROUPS):
                start = owner * SHARE + piece * 8
                if start < degrees:
                    lines = column[pl.ds(start, 8), :]
                    packed = packed + (pltpu.roll(lines, GROUP * piece, 1) if piece else lines)
            send_buf[owner] = packed
        sems = next_round()

        def send(index, carry):
            peer = obs_peer(index)
            obs_copy(send_buf.at[peer], recv_obs.at[obs_here], sems, peer).start()
            return carry

        lax.fori_loop(0, obss - 1, send, 0)
        recv_obs[obs_here] = send_buf[obs_here]
        done = whole(obs_copy, recv_obs, sems, obss - 1, obs_peer(0))
        waits.append(done)
        meanwhile()
        done.wait_recv()
        summed = jnp.sum(recv_obs[...], axis=0)
        return summed, summed[0:1, SCALAR_LANE : SCALAR_LANE + 1]

    def send_ord(packed):
        which = shares[0]
        shares[0] += 1
        send_buf, recv_buf = share_send[which], share_recv[which]
        send_buf[...] = packed
        recv_buf[ord_here] = packed
        return gather_ord(send_buf, recv_buf), recv_buf

    def choose(block_line, index_ref, chosen):
        for slot in range(block):
            number = index_ref[slot]
            source = lax.div(number, block)
            shift = lax.rem(2 * slot - 2 * (number - source * block) + LANES, LANES)
            lines = pltpu.roll(block_line(source), shift, 1)
            chosen = jnp.where(jnp.logical_and(inside, slot_lane == slot), lines, chosen)
        return chosen

    def take_ord(sent, index_ref):
        done, recv_buf = sent
        done.wait_recv()
        everyone = jnp.sum(recv_buf[...], axis=0)
        return choose(lambda source: recv_buf[source], index_ref, jnp.where(lane == SCALAR_LANE, everyone, 0.0))

    def send_obs(packed):
        which = alls[0]
        alls[0] += 1
        send_buf, recv_buf = all_send[which], all_recv[which]
        send_buf[...] = packed
        recv_buf[obs_here] = packed
        return gather_obs(send_buf, recv_buf), recv_buf

    def take_obs(sent):
        done, recv_buf = sent
        done.wait_recv()
        total = jnp.sum(recv_buf[...], axis=0)[0:1, SCALAR_LANE : SCALAR_LANE + 1]
        return unpacked(recv_buf, degrees), total

    def exchange_obs(packed):
        return take_obs(send_obs(packed))

    def precondition(packed, table_of, alive, meanwhile):
        sent = send_obs(packed)
        meanwhile()
        lines, unused = take_obs(sent)
        column[pl.ds(0, degrees), :] = lines
        by_slot = jnp.transpose(column[...])
        result = jnp.zeros((8, LANES), jnp.float32)
        for slot in range(block):
            table = table_of(slot)
            for part in range(2):
                col = 2 * slot + part
                value = jnp.sum(table * by_slot[col : col + 1, : table.shape[1]], axis=1, keepdims=True)
                for piece in range(GROUPS):
                    result = jnp.where(lane == GROUP * piece + col, value[8 * piece : 8 * piece + 8], result)
        return jnp.where(alive, result, 0.0)

    share_start = pl.multiple_of(obs_here * SHARE, 8)

    def owner_table(slot):
        return inv[slot, pl.ds(share_start, SHARE), :]

    tiles_wide = inv_block.shape[2] // LANES
    spread_sems, inv_sems = next_round(), next_round()

    def build_spread():
        for slot in range(block):
            for wide in range(tiles_wide):
                width = min(LANES, degrees - wide * LANES)
                for piece in range(GROUPS):
                    lines = inv[slot, pl.ds(share_start + 8 * piece, 8), pl.ds(wide * LANES, width)]
                    if width < LANES:
                        lines = jnp.concatenate([lines, jnp.zeros((8, LANES - width), jnp.float32)], axis=1)
                    for half in range(2):
                        place = (wide * GROUPS + piece) * 2 + half
                        spread_send[place % ords, slot, place // ords] = lines[4 * half : 4 * half + 4]
        spread_recv[pl.ds(ord_here * block, block)] = spread_send[ord_here]

    def send_spread(first, last):
        def send(index, carry):
            peer = bulk_peer(index)
            ord_copy(spread_send.at[peer], spread_recv.at[pl.ds(ord_here * block, block)], spread_sems, peer).start()
            return carry

        lax.fori_loop(first, last, send, 0)

    def build_inv():
        cut = spread_recv.at[pl.ds(0, (ords - 1) * block)]
        done = ord_copy(cut, cut, spread_sems, ord_peer(0))
        waits.append(done)
        done.wait_recv()

        def step(index, carry):
            for order in range(block):
                number = index * block + order
                inv_send[index, order] = spread_recv[slot_all[lax.div(number, LANES), lax.rem(number, LANES)]]
            return carry

        lax.fori_loop(0, ords, step, 0)
        inv_recv[ord_here] = inv_send[ord_here]

    def send_inv(first, last):
        def send(index, carry):
            peer = bulk_peer(index)
            ord_copy(inv_send.at[peer], inv_recv.at[ord_here], inv_sems, peer).start()
            return carry

        lax.fori_loop(first, last, send, 0)

    def take_inv():
        done = whole(ord_copy, inv_recv, inv_sems, ords - 1, ord_peer(0))
        waits.append(done)
        done.wait_recv()
        for order in range(block):
            for wide in range(tiles_wide):
                for piece in range(GROUPS):
                    for half in range(2):
                        place = (wide * GROUPS + piece) * 2 + half
                        inv_block[order, pl.ds(8 * piece + 4 * half, 4), pl.ds(wide * LANES, LANES)] = inv_recv[
                            place % ords, order, place // ords
                        ]

    def find_slots():
        ids_done.wait_recv()
        ids_copy = pltpu.make_async_copy(ids_recv, ids_smem, local_sem.at[2])
        ids_copy.start()
        ids_copy.wait()
        position = sublane * LANES + lane

        def find(owner, found):
            for slot in range(block):
                found = jnp.where(position == ids_smem[owner, 0, slot], owner * block + slot, found)
            return found

        slot_vmem[...] = lax.fori_loop(0, ords, find, jnp.zeros((8, LANES), jnp.int32))
        slot_copy = pltpu.make_async_copy(slot_vmem, slot_all, local_sem.at[3])
        slot_copy.start()
        slot_copy.wait()
        for order in range(block):
            number = ord_here * block + order
            slot_smem[order] = slot_all[lax.div(number, LANES), lax.rem(number, LANES)]

    def with_energy(residual, precond):
        product = jnp.where(inside, residual * precond, 0.0)
        share = jnp.sum(jnp.sum(product, axis=1, keepdims=True), axis=0, keepdims=True)
        return jnp.where(lane == SCALAR_LANE, share, precond)

    def synthesize(coefficients, energy, rows, meanwhile):
        which = tiles[0]
        tiles[0] += 1
        sems = next_round()
        send_buf, recv_buf = tile_send[which], tile_recv[which]
        for order in range(block):
            table = leg[order]
            for part in range(2):
                col = 2 * order + part
                rows[pl.ds(col, 1), :] = jnp.sum(table * coefficients[:, col : col + 1], axis=0, keepdims=True)
        rows[pl.ds(CURVE_COLUMN, 1), :] = jnp.broadcast_to(energy, (1, cycles))
        quarter = cycles // 4
        lines = rows[...]
        turned = jnp.transpose(
            jnp.concatenate([lines[:, part * quarter : part * quarter + quarter] for part in range(4)], axis=0)
        )
        for target in range(ords):
            send_buf[target] = turned[2 * target : 2 * target + 2]
        recv_buf[ord_here] = send_buf[ord_here]

        half = ord_z // 2
        sems = [sems] + [next_round() for unused in range(half)]

        def send_line(peer, sem):
            ord_copy(send_buf.at[peer], recv_buf.at[ord_here], sem, peer).start()

        for far in range(half, -1, -1):
            for step_z in ([far] if far in (0, half) else [far, ord_z - far]):
                for step_y in range(ord_y - 1, -1, -1):
                    if step_z or step_y:
                        send_line(ord_at(step_y, step_z), sems[far])

        meanwhile()
        sums = [jnp.zeros((CYCLES_HERE, SLOTS), jnp.float32) for unused in range(4)]
        energies = jnp.zeros((8, LANES), jnp.float32)
        for far in range(half + 1):
            steps = [far] if far in (0, half) else [far, ord_z - far]
            peers = len(steps) * ord_y - (far == 0)
            done = whole(ord_copy, recv_buf, sems[far], peers, ord_at(0, half))
            waits.append(done)
            done.wait_recv()
            for step_z in steps:
                for step_y in range(ord_y):
                    index = ord_at(step_y, step_z)
                    pair = recv_buf[index]
                    tile = jnp.concatenate(
                        [jnp.broadcast_to(pair[half : half + 1], (4, LANES)) for half in range(2)], axis=0
                    )
                    spread = tile
                    for part in range(1, 4):
                        tile = jnp.where(sublane % 4 == part, pltpu.roll(spread, LANES - 32 * part, 1), tile)
                    energies = energies + tile
                    for col in range(columns):
                        sums[col % 4] = sums[col % 4] + harm[index, col] * tile[:, col : col + 1]
        return (sums[0] + sums[1]) + (sums[2] + sums[3]), energies[0:1, CURVE_COLUMN : CURVE_COLUMN + 1]

    leg_copy.wait()
    done, recv_buf = per_cycle(windows_ref[pl.ds(2 * CYCLES_HERE, CYCLES_HERE), :], jnp.zeros((1, 1), jnp.float32))

    ids_done = gather_ord(ids_send, ids_recv)
    inv_copy.wait()
    build_spread()
    part = ords // 4
    last_bulk = 3 * part
    send_spread(0, part)
    done.wait_recv()
    summed, unused = adjoint(recv_buf, rows_ref[0], lambda: send_spread(part, 2 * part))
    residual = jnp.where(inside, summed, 0.0)
    sent = send_ord(residual)
    find_slots()
    owned = jnp.where(inside, take_ord(sent, own_ref), 0.0)
    precond = precondition(owned, owner_table, live, lambda: send_spread(2 * part, last_bulk))
    sent = send_ord(with_energy(owned, precond))
    chosen = take_ord(sent, slot_smem)
    sent = send_obs(chosen)
    send_spread(last_bulk, ords - 1)
    lines, energy_now = take_obs(sent)
    direction = jnp.where(inside, chosen, 0.0)
    solution = jnp.zeros((8, LANES), jnp.float32)
    gradient = None
    nothing = jnp.zeros((1, 1), jnp.float32)
    for iteration in range(ITERS):
        if iteration == 0:

            def prepare():
                build_inv()
                send_inv(0, part)

            gradient, unused = synthesize(lines, nothing, rows_ref[1], prepare)
        else:
            precond = precondition(residual, lambda slot: inv_block[slot], live_block, take_inv)
            lines, energy_block = exchange_obs(with_energy(residual, precond))
            ahead, energy = synthesize(lines, energy_block, rows_ref[1], lambda: None)
            ratio = energy / energy_now
            gradient = ahead + ratio * gradient
            direction = precond + ratio * direction
            energy_now = energy
        weighted = windows_ref[pl.ds(CYCLES_HERE, CYCLES_HERE), :] * gradient
        curve = jnp.sum(jnp.sum(weighted * gradient, axis=1, keepdims=True), axis=0, keepdims=True)
        done, recv_buf = per_cycle(weighted, curve)
        if iteration == 0:
            send_inv(part, last_bulk)
        done.wait_recv()
        summed, curvature = adjoint(
            recv_buf, rows_ref[0], (lambda: send_inv(last_bulk, ords - 1)) if iteration == 0 else (lambda: None)
        )
        step_size = energy_now / curvature
        solution = solution + step_size * direction
        residual = residual - step_size * jnp.where(inside, summed, 0.0)

    for which, value in enumerate((solution, residual)):
        last_send[which] = value
        last_recv[ord_here, which] = value
    gather_ord(last_send, last_recv).wait_recv()
    for which in range(2):
        value = choose(lambda source, which=which: last_recv[source, which], own_ref, jnp.zeros((8, LANES), jnp.float32))
        last_share[which] = value
        last_all[obs_here, which] = value
    gather_obs(last_share, last_all).wait_recv()
    for which in range(2):
        packed_ref[which] = last_all[:, which]
    for done in waits:
        done.wait_send()


def buffers(rounds, *shape):
    return [pltpu.VMEM(shape, jnp.float32) for unused in range(rounds)]


def body(ord_y, ord_z, obs_x, longitude, cycle_of, obs_count, observed, obs_weight, legendre, precond_inv, order_of_slot):
    block, degrees, cycles = legendre.shape[1:]
    slab = longitude.shape[1]
    ords, obss = ord_y * ord_z, obs_x * 2
    vmem = pl.BlockSpec(memory_space=pltpu.VMEM)
    smem = pl.BlockSpec(memory_space=pltpu.SMEM)
    hbm = pl.BlockSpec(memory_space=pltpu.HBM)
    lines = (slab // LANES, LANES)
    result = jax.ShapeDtypeStruct((block, 2, degrees), jnp.float32)
    dims = (block, degrees, cycles, ord_y, ord_z, obs_x)
    column_rows = -(-max(degrees, 1) // LANES) * LANES
    tile_rounds = 1 + 2 * ITERS
    share_rounds = 2
    all_rounds = 2 * ITERS
    deep = -(-(column_rows // LANES * GROUPS * 2) // ords)
    total_rounds = 1 + tile_rounds + (1 + ITERS) + share_rounds + all_rounds + ITERS * (ord_z // 2) + 4
    scratch = [
        pltpu.VMEM((3 * CYCLES_HERE, SLOTS), jnp.float32),
        pltpu.VMEM((ords, 2 * block, CYCLES_HERE, SLOTS), jnp.float32),
        pltpu.VMEM((block, degrees, cycles), jnp.float32),
        pltpu.VMEM((block, SHARE * obss, degrees), jnp.float32),
        pltpu.VMEM((column_rows, LANES), jnp.float32),
        pltpu.VMEM((2 * ords, LANES), jnp.float32),
        [pltpu.VMEM((32, cycles), jnp.float32), pltpu.VMEM((32, cycles), jnp.float32)],
        buffers(tile_rounds, ords, 2, LANES),
        buffers(tile_rounds, ords, 2, LANES),
        buffers(1 + ITERS, obss, 8, LANES),
        buffers(1 + ITERS, obss, 8, LANES),
        buffers(share_rounds, 8, LANES),
        buffers(share_rounds, ords, 8, LANES),
        buffers(all_rounds, 8, LANES),
        buffers(all_rounds, obss, 8, LANES),
        pltpu.VMEM((1, LANES), jnp.int32),
        pltpu.VMEM((ords, 1, LANES), jnp.int32),
        pltpu.SMEM((ords, 1, LANES), jnp.int32),
        pltpu.VMEM((8, LANES), jnp.int32),
        pltpu.SMEM((8, LANES), jnp.int32),
        pltpu.SMEM((block,), jnp.int32),
        pltpu.VMEM((ords, block, deep, 4, LANES), jnp.float32),
        pltpu.VMEM((ords * block, deep, 4, LANES), jnp.float32),
        pltpu.VMEM((ords, block, deep, 4, LANES), jnp.float32),
        pltpu.VMEM((ords, block, deep, 4, LANES), jnp.float32),
        pltpu.VMEM((block, SHARE, column_rows), jnp.float32),
        pltpu.VMEM((2, 8, LANES), jnp.float32),
        pltpu.VMEM((ords, 2, 8, LANES), jnp.float32),
        pltpu.VMEM((2, 8, LANES), jnp.float32),
        pltpu.VMEM((obss, 2, 8, LANES), jnp.float32),
        pltpu.SemaphoreType.DMA((4,)),
        pltpu.SemaphoreType.DMA((total_rounds,)),
        pltpu.SemaphoreType.DMA((total_rounds,)),
    ]
    packed = pl.pallas_call(
        functools.partial(main_kernel, dims, float(slab * obss)),
        out_shape=jax.ShapeDtypeStruct((2, obss, 8, LANES), jnp.float32),
        in_specs=[smem, smem, vmem, vmem, vmem, vmem, hbm, hbm],
        out_specs=vmem,
        scratch_shapes=scratch,
        compiler_params=pltpu.CompilerParams(
            collective_id=0, has_side_effects=True
        ),
        name="solve",
    )(
        order_of_slot, obs_count, cycle_of.reshape(lines), longitude.reshape(lines), observed.reshape(lines),
        obs_weight.reshape(lines), legendre[0], precond_inv,
    )
    return pl.pallas_call(
        finish_kernel,
        out_shape=(result, result),
        in_specs=[vmem],
        out_specs=(vmem, vmem),
        scratch_shapes=[pltpu.VMEM((column_rows, LANES), jnp.float32)],
        name="unpack",
    )(packed)


def solution(mesh):
    placed = (
        P("obs", None),
        P("obs", None),
        P("obs"),
        P("obs", None),
        P("obs", None),
        P("obs", "ord", None, None),
        P("ord", None, None),
        P("ord"),
    )
    ords = mesh.shape["ord"]
    ord_y = 4 if ords == 32 else 2
    run = functools.partial(body, ord_y, ords // ord_y, mesh.shape["obs"] // 2)
    return jax.shard_map(
        run,
        mesh=mesh,
        in_specs=placed,
        out_specs=(P("ord", None, None), P("ord", None, None)),
        check_vma=False,
    )
```

```python
import functools

import jax
import jax.numpy as jnp
from jax import lax
from jax.experimental import pallas as pl
from jax.experimental.pallas import tpu as pltpu
from jax.sharding import PartitionSpec as P

ITERS = 2
MESH = pl.DeviceIdType.MESH
LANES = 128
SLOTS = 256
CYCLES_HERE = 8
GROUP = 20
GROUPS = 5
SHARE = 8 * GROUPS
SCALAR_LANE = 127
CURVE_COLUMN = 18
TWO_OVER_PI = 0.6366197723675814
PI_2_A = 1.5703125
PI_2_B = 0.00048351287841796875
PI_2_C = 3.13855707645416259765625e-07
PI_2_D = 6.077100628276710e-11


def sine_cosine(angle):
    turns = jnp.floor(angle * TWO_OVER_PI + 0.5)
    rest = angle - turns * PI_2_A
    rest = rest - turns * PI_2_B
    rest = rest - turns * PI_2_C
    rest = rest - turns * PI_2_D
    square = rest * rest
    sine = rest + rest * square * (-1.6666654611e-1 + square * (8.3321608736e-3 + square * -1.9515295891e-4))
    cosine = 1.0 - 0.5 * square + square * square * (
        4.166664568298827e-2 + square * (-1.388731625493765e-3 + square * 2.443315711809948e-5)
    )
    quadrant = turns.astype(jnp.int32)
    swap = (quadrant & 1) == 1
    sine_out = jnp.where(swap, cosine, sine)
    cosine_out = jnp.where(swap, sine, cosine)
    sine_out = jnp.where((quadrant & 2) == 2, -sine_out, sine_out)
    cosine_out = jnp.where(((quadrant + 1) & 2) == 2, -cosine_out, cosine_out)
    return sine_out, cosine_out


def fill_windows(total_obs, quarter, count_ref, cycle_ref, lon_ref, obs_ref, weight_ref, out_ref):
    first_cycle = lax.axis_index("ord") * 2
    rows = cycle_ref.shape[0]
    ids = cycle_ref[...]

    def before(cycle):
        return jnp.sum(jnp.where(ids < cycle, 1, 0))

    starts = [[before(first_cycle + part * quarter + step) for step in range(3)] for part in range(4)]
    lane = lax.broadcasted_iota(jnp.int32, (1, LANES), 1)
    used = count_ref[0]
    for step in range(CYCLES_HERE):
        start = starts[step % 4][step // 4]
        count = starts[step % 4][step // 4 + 1] - start
        row = start // LANES
        shift = start - row * LANES
        turn = lax.rem(LANES - shift, LANES)
        lines = [jnp.minimum(row + part, rows - 1) for part in range(3)]
        head = lane < LANES - shift
        windows = []
        for ref in (lon_ref, obs_ref, weight_ref):
            turned = [pltpu.roll(ref[pl.ds(line, 1), :], turn, 1) for line in lines]
            windows.append([jnp.where(head, turned[part], turned[part + 1]) for part in range(2)])
        for part in range(2):
            slot = lane + part * LANES
            valid = jnp.logical_and(slot < count, start + slot < used)
            scale = jnp.where(valid, windows[2][part] / total_obs, 0.0)
            cut = pl.ds(part * LANES, LANES)
            for which, value in enumerate((windows[0][part], scale, scale * windows[1][part])):
                out_ref[pl.ds(which * CYCLES_HERE + step, 1), cut] = value


def unpacked(shares, degrees):
    pieces = []
    for owner in range(shares.shape[0]):
        for piece in range(GROUPS):
            if owner * SHARE + piece * 8 < degrees:
                lines = shares[owner]
                pieces.append(pltpu.roll(lines, LANES - GROUP * piece, 1) if piece else lines)
    return jnp.concatenate(pieces, axis=0)


def finish_kernel(packed_ref, solution_ref, residual_ref, column):
    block, unused, degrees = solution_ref.shape
    column[...] = jnp.zeros(column.shape, jnp.float32)
    for which, out in enumerate((solution_ref, residual_ref)):
        column[pl.ds(0, degrees), :] = unpacked(packed_ref.at[which], degrees)
        by_slot = jnp.transpose(column[...])
        for slot in range(block):
            out[slot] = by_slot[2 * slot : 2 * slot + 2, :degrees]


def offset(index):
    return ((index + 1) // 2) * (1 - 2 * (index % 2))


def main_kernel(
    dims, total_obs, own_ref, count_ref, cycle_ref, lon_ref, obs_ref, weight_ref, leg_hbm, inv_hbm, packed_ref, windows_ref,
    harm, leg, inv, column, stage, rows_ref, tile_send, tile_recv, part_send, part_recv, share_send, share_recv,
    all_send, all_recv, ids_send, ids_recv, ids_smem, slot_vmem, slot_all, slot_smem, spread_send, spread_recv,
    inv_send, inv_recv, inv_block, last_send, last_recv, last_share, last_all, local_sem, send_sem, recv_sem,
):
    block, degrees, cycles, ord_y, ord_z, obs_x = dims
    ords = ord_y * ord_z
    obss = obs_x * 2
    columns = 2 * block
    unroll = 4 * ord_y
    ord_here = lax.axis_index("ord")
    obs_here = lax.axis_index("obs")

    for slot in range(block):
        inv[slot, pl.ds(degrees, SHARE * obss - degrees), :] = jnp.zeros((SHARE * obss - degrees, degrees), jnp.float32)
    leg_copy = pltpu.make_async_copy(leg_hbm, leg, local_sem.at[0])
    inv_copy = pltpu.make_async_copy(inv_hbm, inv.at[:, pl.ds(0, degrees), :], local_sem.at[1])
    leg_copy.start()
    inv_copy.start()

    here_y, here_z = lax.div(ord_here, ord_z), lax.rem(ord_here, ord_z)
    here_x, here_core = lax.div(obs_here, 2), lax.rem(obs_here, 2)

    def ord_at(step_y, step_z):
        return lax.rem(here_y + step_y, ord_y) * ord_z + lax.rem(here_z + step_z, ord_z)

    def ord_peer(index):
        return ord_at(ord_y // 2 + offset(index % ord_y), ord_z // 2 + offset(index // ord_y))

    def bulk_peer(index):
        return ord_at(ord_y // 2 + offset(index // ord_z), ord_z // 2 + offset(index % ord_z))

    def obs_peer(index):
        step_x = obs_x // 2 + offset(index // 2)
        step_core = 1 - index % 2
        return lax.rem(here_x + step_x, obs_x) * 2 + lax.rem(here_core + step_core, 2)

    barrier = pltpu.get_barrier_semaphore()

    for index in range(ords - 1):
        pl.semaphore_signal(barrier, inc=1, device_id={"ord": ord_peer(index)}, device_id_type=MESH)
    for index in range(obss - 1):
        pl.semaphore_signal(barrier, inc=1, device_id={"obs": obs_peer(index)}, device_id_type=MESH)

    lane = lax.broadcasted_iota(jnp.int32, (8, LANES), 1)
    sublane = lax.broadcasted_iota(jnp.int32, (8, LANES), 0)
    place = lane - 32 * (sublane % 4)
    group = lane // GROUP
    inner = lane % GROUP
    slot_lane = inner // 2
    degree_here = obs_here * SHARE + group * 8 + sublane
    inside = jnp.logical_and(jnp.logical_and(group < GROUPS, inner < columns), degree_here < degrees)
    order_lane = jnp.zeros((8, LANES), jnp.int32)
    for slot in range(block):
        order_lane = jnp.where(slot_lane == slot, own_ref[slot], order_lane)
    live = jnp.logical_and(inside, degree_here >= order_lane)
    live_block = jnp.logical_and(inside, degree_here >= ord_here * block + slot_lane)

    ids_row = jnp.zeros((1, LANES), jnp.int32)
    lane_row = lax.broadcasted_iota(jnp.int32, (1, LANES), 1)
    for slot in range(block):
        ids_row = jnp.where(lane_row == slot, own_ref[slot], ids_row)
    ids_send[...] = ids_row
    ids_recv[ord_here] = ids_row
    for which in range(len(rows_ref)):
        rows_ref[which][...] = jnp.zeros((32, cycles), jnp.float32)
    column[...] = jnp.zeros(column.shape, jnp.float32)

    fill_windows(total_obs, cycles // 4, count_ref, cycle_ref, lon_ref, obs_ref, weight_ref, windows_ref)
    longitude = windows_ref[pl.ds(0, CYCLES_HERE), :]

    def harmonic_block(index, carry):
        for order in range(block):
            number = (index * block + order).astype(jnp.float32)
            sine, cosine = sine_cosine(number * longitude)
            harm[index, 2 * order] = cosine
            harm[index, 2 * order + 1] = sine
        return carry

    lax.fori_loop(0, ords, harmonic_block, 0)
    pl.semaphore_wait(barrier, ords - 1 + obss - 1)

    rounds = [0]
    waits = []

    def next_round():
        rounds[0] += 1
        return rounds[0] - 1

    def ord_copy(source, target, sems, peer):
        return pltpu.make_async_remote_copy(
            src_ref=source, dst_ref=target, send_sem=send_sem.at[sems], recv_sem=recv_sem.at[sems],
            device_id={"ord": peer}, device_id_type=MESH,
        )

    def obs_copy(source, target, sems, peer):
        return pltpu.make_async_remote_copy(
            src_ref=source, dst_ref=target, send_sem=send_sem.at[sems], recv_sem=recv_sem.at[sems],
            device_id={"obs": peer}, device_id_type=MESH,
        )

    def whole(make, buffer, sems, peers, peer):
        cut = buffer.at[pl.ds(0, peers)]
        return make(cut, cut, sems, peer)

    def gather_ord(source, buffer):
        sems = next_round()

        def send(index, carry):
            ord_copy(source, buffer.at[ord_here], sems, ord_peer(index)).start()
            return carry

        lax.fori_loop(0, ords - 1, send, 0)
        done = whole(ord_copy, buffer, sems, ords - 1, ord_peer(0))
        waits.append(done)
        return done

    def gather_obs(source, buffer):
        sems = next_round()

        def send(index, carry):
            obs_copy(source, buffer.at[obs_here], sems, obs_peer(index)).start()
            return carry

        lax.fori_loop(0, obss - 1, send, 0)
        done = whole(obs_copy, buffer, sems, obss - 1, obs_peer(0))
        waits.append(done)
        return done

    tiles = [0]
    parts = [0]
    shares = [0]
    alls = [0]

    def per_cycle(weighted, curve):
        which = tiles[0]
        tiles[0] += 1
        sems = next_round()
        send_buf, recv_buf = tile_send[which], tile_recv[which]
        corner = jnp.logical_and(place == CURVE_COLUMN, sublane == 0)
        empty = jnp.where(corner, curve, 0.0)

        def step(outer, carry):
            for inner_step in range(unroll):
                index = outer * unroll + inner_step
                peer = ord_at(
                    ord_y // 2 + offset(inner_step % ord_y), ord_z // 2 + offset(outer * (unroll // ord_y) + inner_step // ord_y)
                )
                tile = empty
                for col in range(columns):
                    total = jnp.sum(harm[peer, col] * weighted, axis=1, keepdims=True)
                    tile = jnp.where(place == col, total, tile)
                tile = jnp.concatenate(
                    [jnp.sum(tile[4 * half : 4 * half + 4], axis=0, keepdims=True) for half in range(2)], axis=0
                )
                send_buf[peer] = tile
                if inner_step < unroll - 1:
                    ord_copy(send_buf.at[peer], recv_buf.at[ord_here], sems, peer).start()
                else:
                    @pl.when(index < ords - 1)
                    def _():
                        ord_copy(send_buf.at[peer], recv_buf.at[ord_here], sems, peer).start()

                    @pl.when(index == ords - 1)
                    def _():
                        recv_buf[ord_here] = tile
            return carry

        lax.fori_loop(0, ords // unroll, step, 0)
        done = whole(ord_copy, recv_buf, sems, ords - 1, ord_peer(0))
        waits.append(done)
        return done, recv_buf

    def adjoint(recv_buf, rows, meanwhile):
        for source in range(ords):
            stage[pl.ds(2 * source, 2), :] = recv_buf[source]
        turned = jnp.transpose(stage[...])
        rows[...] = jnp.concatenate([turned[32 * part : 32 * part + 32] for part in range(4)], axis=1)
        curve = jnp.sum(rows[pl.ds(CURVE_COLUMN, 1), :], axis=1, keepdims=True)
        lane_all = lax.broadcasted_iota(jnp.int32, (degrees, LANES), 1)
        total = jnp.zeros((degrees, LANES), jnp.float32)
        for order in range(block):
            table = leg[order]
            for part in range(2):
                col = 2 * order + part
                value = jnp.sum(table * rows[pl.ds(col, 1), :], axis=1, keepdims=True)
                total = jnp.where(lane_all == col, value, total)
        column[pl.ds(0, degrees), :] = total
        which = parts[0]
        parts[0] += 1
        send_buf, recv_obs = part_send[which], part_recv[which]
        for owner in range(obss):
            packed = jnp.where(lane == SCALAR_LANE, curve, 0.0)
            for piece in range(GROUPS):
                start = owner * SHARE + piece * 8
                if start < degrees:
                    lines = column[pl.ds(start, 8), :]
                    packed = packed + (pltpu.roll(lines, GROUP * piece, 1) if piece else lines)
            send_buf[owner] = packed
        sems = next_round()

        def send(index, carry):
            peer = obs_peer(index)
            obs_copy(send_buf.at[peer], recv_obs.at[obs_here], sems, peer).start()
            return carry

        lax.fori_loop(0, obss - 1, send, 0)
        recv_obs[obs_here] = send_buf[obs_here]
        done = whole(obs_copy, recv_obs, sems, obss - 1, obs_peer(0))
        waits.append(done)
        meanwhile()
        done.wait_recv()
        summed = jnp.sum(recv_obs[...], axis=0)
        return summed, summed[0:1, SCALAR_LANE : SCALAR_LANE + 1]

    def send_ord(packed):
        which = shares[0]
        shares[0] += 1
        send_buf, recv_buf = share_send[which], share_recv[which]
        send_buf[...] = packed
        recv_buf[ord_here] = packed
        return gather_ord(send_buf, recv_buf), recv_buf

    def choose(block_line, index_ref, chosen):
        for slot in range(block):
            number = index_ref[slot]
            source = lax.div(number, block)
            shift = lax.rem(2 * slot - 2 * (number - source * block) + LANES, LANES)
            lines = pltpu.roll(block_line(source), shift, 1)
            chosen = jnp.where(jnp.logical_and(inside, slot_lane == slot), lines, chosen)
        return chosen

    def take_ord(sent, index_ref):
        done, recv_buf = sent
        done.wait_recv()
        everyone = jnp.sum(recv_buf[...], axis=0)
        return choose(lambda source: recv_buf[source], index_ref, jnp.where(lane == SCALAR_LANE, everyone, 0.0))

    def send_obs(packed):
        which = alls[0]
        alls[0] += 1
        send_buf, recv_buf = all_send[which], all_recv[which]
        send_buf[...] = packed
        recv_buf[obs_here] = packed
        return gather_obs(send_buf, recv_buf), recv_buf

    def take_obs(sent):
        done, recv_buf = sent
        done.wait_recv()
        total = jnp.sum(recv_buf[...], axis=0)[0:1, SCALAR_LANE : SCALAR_LANE + 1]
        return unpacked(recv_buf, degrees), total

    def exchange_obs(packed):
        return take_obs(send_obs(packed))

    def precondition(packed, table_of, alive, meanwhile):
        sent = send_obs(packed)
        meanwhile()
        lines, unused = take_obs(sent)
        column[pl.ds(0, degrees), :] = lines
        by_slot = jnp.transpose(column[...])
        result = jnp.zeros((8, LANES), jnp.float32)
        for slot in range(block):
            table = table_of(slot)
            for part in range(2):
                col = 2 * slot + part
                value = jnp.sum(table * by_slot[col : col + 1, : table.shape[1]], axis=1, keepdims=True)
                for piece in range(GROUPS):
                    result = jnp.where(lane == GROUP * piece + col, value[8 * piece : 8 * piece + 8], result)
        return jnp.where(alive, result, 0.0)

    share_start = pl.multiple_of(obs_here * SHARE, 8)

    def owner_table(slot):
        return inv[slot, pl.ds(share_start, SHARE), :]

    tiles_wide = inv_block.shape[2] // LANES
    spread_sems, inv_sems = next_round(), next_round()

    def build_spread():
        for slot in range(block):
            for wide in range(tiles_wide):
                width = min(LANES, degrees - wide * LANES)
                for piece in range(GROUPS):
                    lines = inv[slot, pl.ds(share_start + 8 * piece, 8), pl.ds(wide * LANES, width)]
                    if width < LANES:
                        lines = jnp.concatenate([lines, jnp.zeros((8, LANES - width), jnp.float32)], axis=1)
                    for half in range(2):
                        place = (wide * GROUPS + piece) * 2 + half
                        spread_send[place % ords, slot, place // ords] = lines[4 * half : 4 * half + 4]
        spread_recv[pl.ds(ord_here * block, block)] = spread_send[ord_here]

    def send_spread(first, last):
        def send(index, carry):
            peer = bulk_peer(index)
            ord_copy(spread_send.at[peer], spread_recv.at[pl.ds(ord_here * block, block)], spread_sems, peer).start()
            return carry

        lax.fori_loop(first, last, send, 0)

    def build_inv():
        cut = spread_recv.at[pl.ds(0, (ords - 1) * block)]
        done = ord_copy(cut, cut, spread_sems, ord_peer(0))
        waits.append(done)
        done.wait_recv()

        def step(index, carry):
            for order in range(block):
                number = index * block + order
                inv_send[index, order] = spread_recv[slot_all[lax.div(number, LANES), lax.rem(number, LANES)]]
            return carry

        lax.fori_loop(0, ords, step, 0)
        inv_recv[ord_here] = inv_send[ord_here]

    def send_inv(first, last):
        def send(index, carry):
            peer = bulk_peer(index)
            ord_copy(inv_send.at[peer], inv_recv.at[ord_here], inv_sems, peer).start()
            return carry

        lax.fori_loop(first, last, send, 0)

    def take_inv():
        done = whole(ord_copy, inv_recv, inv_sems, ords - 1, ord_peer(0))
        waits.append(done)
        done.wait_recv()
        for order in range(block):
            for wide in range(tiles_wide):
                for piece in range(GROUPS):
                    for half in range(2):
                        place = (wide * GROUPS + piece) * 2 + half
                        inv_block[order, pl.ds(8 * piece + 4 * half, 4), pl.ds(wide * LANES, LANES)] = inv_recv[
                            place % ords, order, place // ords
                        ]

    def find_slots():
        ids_done.wait_recv()
        ids_copy = pltpu.make_async_copy(ids_recv, ids_smem, local_sem.at[2])
        ids_copy.start()
        ids_copy.wait()
        position = sublane * LANES + lane

        def find(owner, found):
            for slot in range(block):
                found = jnp.where(position == ids_smem[owner, 0, slot], owner * block + slot, found)
            return found

        slot_vmem[...] = lax.fori_loop(0, ords, find, jnp.zeros((8, LANES), jnp.int32))
        slot_copy = pltpu.make_async_copy(slot_vmem, slot_all, local_sem.at[3])
        slot_copy.start()
        slot_copy.wait()
        for order in range(block):
            number = ord_here * block + order
            slot_smem[order] = slot_all[lax.div(number, LANES), lax.rem(number, LANES)]

    def with_energy(residual, precond):
        product = jnp.where(inside, residual * precond, 0.0)
        share = jnp.sum(jnp.sum(product, axis=1, keepdims=True), axis=0, keepdims=True)
        return jnp.where(lane == SCALAR_LANE, share, precond)

    def synthesize(coefficients, energy, rows, meanwhile):
        which = tiles[0]
        tiles[0] += 1
        sems = next_round()
        send_buf, recv_buf = tile_send[which], tile_recv[which]
        for order in range(block):
            table = leg[order]
            for part in range(2):
                col = 2 * order + part
                rows[pl.ds(col, 1), :] = jnp.sum(table * coefficients[:, col : col + 1], axis=0, keepdims=True)
        rows[pl.ds(CURVE_COLUMN, 1), :] = jnp.broadcast_to(energy, (1, cycles))
        quarter = cycles // 4
        lines = rows[...]
        turned = jnp.transpose(
            jnp.concatenate([lines[:, part * quarter : part * quarter + quarter] for part in range(4)], axis=0)
        )
        for target in range(ords):
            send_buf[target] = turned[2 * target : 2 * target + 2]
        recv_buf[ord_here] = send_buf[ord_here]

        half = ord_z // 2
        sems = [sems] + [next_round() for unused in range(half)]

        def send_line(peer, sem):
            ord_copy(send_buf.at[peer], recv_buf.at[ord_here], sem, peer).start()

        for far in range(half, -1, -1):
            for step_z in ([far] if far in (0, half) else [far, ord_z - far]):
                for step_y in range(ord_y - 1, -1, -1):
                    if step_z or step_y:
                        send_line(ord_at(step_y, step_z), sems[far])

        meanwhile()
        sums = [jnp.zeros((CYCLES_HERE, SLOTS), jnp.float32) for unused in range(4)]
        energies = jnp.zeros((8, LANES), jnp.float32)
        for far in range(half + 1):
            steps = [far] if far in (0, half) else [far, ord_z - far]
            peers = len(steps) * ord_y - (far == 0)
            done = whole(ord_copy, recv_buf, sems[far], peers, ord_at(0, half))
            waits.append(done)
            done.wait_recv()
            for step_z in steps:
                for step_y in range(ord_y):
                    index = ord_at(step_y, step_z)
                    pair = recv_buf[index]
                    tile = jnp.concatenate(
                        [jnp.broadcast_to(pair[half : half + 1], (4, LANES)) for half in range(2)], axis=0
                    )
                    spread = tile
                    for part in range(1, 4):
                        tile = jnp.where(sublane % 4 == part, pltpu.roll(spread, LANES - 32 * part, 1), tile)
                    energies = energies + tile
                    for col in range(columns):
                        sums[col % 4] = sums[col % 4] + harm[index, col] * tile[:, col : col + 1]
        return (sums[0] + sums[1]) + (sums[2] + sums[3]), energies[0:1, CURVE_COLUMN : CURVE_COLUMN + 1]

    leg_copy.wait()
    done, recv_buf = per_cycle(windows_ref[pl.ds(2 * CYCLES_HERE, CYCLES_HERE), :], jnp.zeros((1, 1), jnp.float32))

    ids_done = gather_ord(ids_send, ids_recv)
    inv_copy.wait()
    build_spread()
    part = ords // 4
    last_bulk = 3 * part
    send_spread(0, part)
    done.wait_recv()
    summed, unused = adjoint(recv_buf, rows_ref[0], lambda: send_spread(part, 2 * part))
    residual = jnp.where(inside, summed, 0.0)
    sent = send_ord(residual)
    find_slots()
    owned = jnp.where(inside, take_ord(sent, own_ref), 0.0)
    precond = precondition(owned, owner_table, live, lambda: send_spread(2 * part, last_bulk))
    sent = send_ord(with_energy(owned, precond))
    chosen = take_ord(sent, slot_smem)
    sent = send_obs(chosen)
    send_spread(last_bulk, ords - 1)
    lines, energy_now = take_obs(sent)
    direction = jnp.where(inside, chosen, 0.0)
    solution = jnp.zeros((8, LANES), jnp.float32)
    gradient = None
    nothing = jnp.zeros((1, 1), jnp.float32)
    for iteration in range(ITERS):
        if iteration == 0:

            def prepare():
                build_inv()
                send_inv(0, part)

            gradient, unused = synthesize(lines, nothing, rows_ref[1], prepare)
        else:
            precond = precondition(residual, lambda slot: inv_block[slot], live_block, take_inv)
            lines, energy_block = exchange_obs(with_energy(residual, precond))
            ahead, energy = synthesize(lines, energy_block, rows_ref[1], lambda: None)
            ratio = energy / energy_now
            gradient = ahead + ratio * gradient
            direction = precond + ratio * direction
            energy_now = energy
        weighted = windows_ref[pl.ds(CYCLES_HERE, CYCLES_HERE), :] * gradient
        curve = jnp.sum(jnp.sum(weighted * gradient, axis=1, keepdims=True), axis=0, keepdims=True)
        done, recv_buf = per_cycle(weighted, curve)
        if iteration == 0:
            send_inv(part, last_bulk)
        done.wait_recv()
        summed, curvature = adjoint(
            recv_buf, rows_ref[0], (lambda: send_inv(last_bulk, ords - 1)) if iteration == 0 else (lambda: None)
        )
        step_size = energy_now / curvature
        solution = solution + step_size * direction
        residual = residual - step_size * jnp.where(inside, summed, 0.0)

    for which, value in enumerate((solution, residual)):
        last_send[which] = value
        last_recv[ord_here, which] = value
    gather_ord(last_send, last_recv).wait_recv()
    for which in range(2):
        value = choose(lambda source, which=which: last_recv[source, which], own_ref, jnp.zeros((8, LANES), jnp.float32))
        last_share[which] = value
        last_all[obs_here, which] = value
    gather_obs(last_share, last_all).wait_recv()
    for which in range(2):
        packed_ref[which] = last_all[:, which]
    for done in waits:
        done.wait_send()


def buffers(rounds, *shape):
    return [pltpu.VMEM(shape, jnp.float32) for unused in range(rounds)]


def body(ord_y, ord_z, obs_x, longitude, cycle_of, obs_count, observed, obs_weight, legendre, precond_inv, order_of_slot):
    block, degrees, cycles = legendre.shape[1:]
    slab = longitude.shape[1]
    ords, obss = ord_y * ord_z, obs_x * 2
    vmem = pl.BlockSpec(memory_space=pltpu.VMEM)
    smem = pl.BlockSpec(memory_space=pltpu.SMEM)
    hbm = pl.BlockSpec(memory_space=pltpu.HBM)
    lines = (slab // LANES, LANES)
    result = jax.ShapeDtypeStruct((block, 2, degrees), jnp.float32)
    dims = (block, degrees, cycles, ord_y, ord_z, obs_x)
    column_rows = -(-max(degrees, 1) // LANES) * LANES
    tile_rounds = 1 + 2 * ITERS
    share_rounds = 2
    all_rounds = 2 * ITERS
    deep = -(-(column_rows // LANES * GROUPS * 2) // ords)
    total_rounds = 1 + tile_rounds + (1 + ITERS) + share_rounds + all_rounds + ITERS * (ord_z // 2) + 4
    scratch = [
        pltpu.VMEM((3 * CYCLES_HERE, SLOTS), jnp.float32),
        pltpu.VMEM((ords, 2 * block, CYCLES_HERE, SLOTS), jnp.float32),
        pltpu.VMEM((block, degrees, cycles), jnp.float32),
        pltpu.VMEM((block, SHARE * obss, degrees), jnp.float32),
        pltpu.VMEM((column_rows, LANES), jnp.float32),
        pltpu.VMEM((2 * ords, LANES), jnp.float32),
        [pltpu.VMEM((32, cycles), jnp.float32), pltpu.VMEM((32, cycles), jnp.float32)],
        buffers(tile_rounds, ords, 2, LANES),
        buffers(tile_rounds, ords, 2, LANES),
        buffers(1 + ITERS, obss, 8, LANES),
        buffers(1 + ITERS, obss, 8, LANES),
        buffers(share_rounds, 8, LANES),
        buffers(share_rounds, ords, 8, LANES),
        buffers(all_rounds, 8, LANES),
        buffers(all_rounds, obss, 8, LANES),
        pltpu.VMEM((1, LANES), jnp.int32),
        pltpu.VMEM((ords, 1, LANES), jnp.int32),
        pltpu.SMEM((ords, 1, LANES), jnp.int32),
        pltpu.VMEM((8, LANES), jnp.int32),
        pltpu.SMEM((8, LANES), jnp.int32),
        pltpu.SMEM((block,), jnp.int32),
        pltpu.VMEM((ords, block, deep, 4, LANES), jnp.float32),
        pltpu.VMEM((ords * block, deep, 4, LANES), jnp.float32),
        pltpu.VMEM((ords, block, deep, 4, LANES), jnp.float32),
        pltpu.VMEM((ords, block, deep, 4, LANES), jnp.float32),
        pltpu.VMEM((block, SHARE, column_rows), jnp.float32),
        pltpu.VMEM((2, 8, LANES), jnp.float32),
        pltpu.VMEM((ords, 2, 8, LANES), jnp.float32),
        pltpu.VMEM((2, 8, LANES), jnp.float32),
        pltpu.VMEM((obss, 2, 8, LANES), jnp.float32),
        pltpu.SemaphoreType.DMA((4,)),
        pltpu.SemaphoreType.DMA((total_rounds,)),
        pltpu.SemaphoreType.DMA((total_rounds,)),
    ]
    packed = pl.pallas_call(
        functools.partial(main_kernel, dims, float(slab * obss)),
        out_shape=jax.ShapeDtypeStruct((2, obss, 8, LANES), jnp.float32),
        in_specs=[smem, smem, vmem, vmem, vmem, vmem, hbm, hbm],
        out_specs=vmem,
        scratch_shapes=scratch,
        compiler_params=pltpu.CompilerParams(
            collective_id=0, has_side_effects=True
        ),
        name="solve",
    )(
        order_of_slot, obs_count, cycle_of.reshape(lines), longitude.reshape(lines), observed.reshape(lines),
        obs_weight.reshape(lines), legendre[0], precond_inv,
    )
    return pl.pallas_call(
        finish_kernel,
        out_shape=(result, result),
        in_specs=[vmem],
        out_specs=(vmem, vmem),
        scratch_shapes=[pltpu.VMEM((column_rows, LANES), jnp.float32)],
        name="unpack",
    )(packed)


def solution(mesh):
    placed = (
        P("obs", None),
        P("obs", None),
        P("obs"),
        P("obs", None),
        P("obs", None),
        P("obs", "ord", None, None),
        P("ord", None, None),
        P("ord"),
    )
    ords = mesh.shape["ord"]
    ord_y = 4 if ords == 32 else 2
    run = functools.partial(body, ord_y, ords // ord_y, mesh.shape["obs"] // 2)
    return jax.shard_map(
        run,
        mesh=mesh,
        in_specs=placed,
        out_specs=(P("ord", None, None), P("ord", None, None)),
        check_vma=False,
    )
```
